16 devices in a mesh: dp: 2 (over y, z), kv: 8 (over x, core).
Axes of the slice: x: 4, y: 2, z: 1, core: 2. Of those that a mesh axis runs over, the one named last changes fastest.
The devices are a block of a 4x4x8 slice.
Arguments:
- x_first: bfloat16 [32, 1536], P('dp'), parts along dimension 0
- next_emb: bfloat16 [2, 32, 1536], P(None, 'dp'), parts along dimension 1
- k_cache: bfloat16 [32, 4096, 8, 64], P('dp', 'kv'), parts along dimension 0
- v_cache: bfloat16 [32, 4096, 8, 64], P('dp', 'kv'), parts along dimension 0
- seq_len: int32 [32], P('dp'), parts along dimension 0
- ln1_gain: float32 [1536], replicated
- ln1_bias: float32 [1536], replicated
- w_q: bfloat16 [1536, 1536], replicated
- b_q: float32 [1536], replicated
- w_k: bfloat16 [1536, 512], replicated
- b_k: float32 [512], replicated
- w_v: bfloat16 [1536, 512], replicated
- b_v: float32 [512], replicated
- w_o: bfloat16 [1536, 1536], replicated
- b_o: float32 [1536], replicated
- ln2_gain: float32 [1536], replicated
- ln2_bias: float32 [1536], replicated
- w_router: bfloat16 [1536, 40], replicated
- w_gate: bfloat16 [40, 1536, 512], P(None, None, 'kv')
- w_up: bfloat16 [40, 1536, 512], P(None, None, 'kv')
- w_down: bfloat16 [40, 512, 1536], P(None, 'kv')
- long_factor: float32 [32], replicated
- expert_idx: int32 [3, 32, 8], P(None, 'dp'), parts along dimension 1
- route_mask: int32 [3, 32, 8, 40], P(None, 'dp'), parts along dimension 1
Outputs:
- output 1: bfloat16 [3, 32, 1536], P(None, 'dp'), parts along dimension 1
- output 2: bfloat16 [32, 3, 8, 64], P('dp'), parts along dimension 0
- output 3: bfloat16 [32, 3, 8, 64], P('dp'), parts along dimension 0
There are 2 independent parts. The reference program is written for one: setup_inputs(seed, part) draws one part's arguments, and reference() takes and returns one part's arrays. A program takes and returns all parts, laid end to end along the dimension named above; an argument that names none is the same for every part.
All inputs are finite; a program needn't handle non-finite values.
Results may differ from the reference program's by a relative error of at most 0.0119208.
Values sent between devices are 32-bit elements.
A program may use at most 768 MiB of HBM per device.

```python
import math
import jax
import jax.numpy as jnp
from jax import lax

BATCH_SIZE = 16
SHARD_LEN = 512
KV_GROUP = 8
CACHE_LEN = 4096
D_MODEL = 1536
Q_HEADS = 24
KV_HEADS = 8
HEAD_DIM = 64
NUM_EXPERTS = 40
TOP_K = 8
FF_DIM = 512
NUM_STEPS = 3
SEG_COUNT = 64

HALF_DIM = HEAD_DIM // 2
Q_GROUP = Q_HEADS // KV_HEADS
FF_SHARD = FF_DIM // KV_GROUP
ROPE_BASE = 10000.0
ROPE_MSCALE = math.sqrt(1.0 + math.log(32.0) / math.log(4096.0))
NORM_EPS = 1e-5
NEG_FILL = -1e30


def setup_inputs(seed: int = 0, part: int = 0) -> dict:
    base_key = jax.random.key(seed)
    shared_keys = jax.random.split(base_key, 17)
    part_keys = jax.random.split(jax.random.fold_in(base_key, part), 9)
    q_width = Q_HEADS * HEAD_DIM
    kv_width = KV_HEADS * HEAD_DIM
    d_scale = D_MODEL ** -0.5

    def normal(rand_key, arr_dims, factor):
        return jax.random.normal(rand_key, arr_dims, jnp.float32) * factor

    x_first = normal(part_keys[0], (BATCH_SIZE, D_MODEL), 1.0).astype(jnp.bfloat16)
    next_emb = normal(part_keys[1], (NUM_STEPS - 1, BATCH_SIZE, D_MODEL), 1.0).astype(jnp.bfloat16)
    seg_index = (jnp.arange(CACHE_LEN) * SEG_COUNT) // CACHE_LEN
    key_segs = normal(part_keys[2], (BATCH_SIZE, SEG_COUNT, KV_HEADS, HEAD_DIM), 1.0)
    value_segs = normal(part_keys[3], (BATCH_SIZE, SEG_COUNT, KV_HEADS, HEAD_DIM), 4.0)
    cache_dims = (BATCH_SIZE, CACHE_LEN, KV_HEADS, HEAD_DIM)
    k_cache = (normal(part_keys[4], cache_dims, 1.0) + key_segs[:, seg_index]).astype(jnp.bfloat16)
    v_cache = (normal(part_keys[5], cache_dims, 1.0) + value_segs[:, seg_index]).astype(jnp.bfloat16)
    drawn_lens = jax.random.randint(part_keys[6], (BATCH_SIZE,), CACHE_LEN // 4, CACHE_LEN + 1)
    seq_len = jnp.where(jnp.arange(BATCH_SIZE) == 0, CACHE_LEN, drawn_lens).astype(jnp.int32)
    rank_scores = jax.random.randint(part_keys[7], (NUM_STEPS, BATCH_SIZE, NUM_EXPERTS), 0, 1 << 20)
    expert_order = jnp.argsort(rank_scores * NUM_EXPERTS + jnp.arange(NUM_EXPERTS), axis=-1)
    expert_idx = expert_order[..., :TOP_K].astype(jnp.int32)
    chosen = (expert_idx[..., None] == jnp.arange(NUM_EXPERTS)).astype(jnp.int32)
    earlier = jnp.cumsum(chosen, axis=2) - chosen
    coin_flip = jax.random.randint(part_keys[8], (NUM_STEPS, BATCH_SIZE, TOP_K, NUM_EXPERTS), 0, 2)
    route_mask = jnp.where(chosen == 1, 1, jnp.where(earlier > 0, 0, coin_flip)).astype(jnp.int32)
    return {
        'x_first': x_first,
        'next_emb': next_emb,
        'k_cache': k_cache,
        'v_cache': v_cache,
        'seq_len': seq_len,
        'ln1_gain': 1.0 + normal(shared_keys[0], (D_MODEL,), 0.3),
        'ln1_bias': normal(shared_keys[1], (D_MODEL,), 0.3),
        'w_q': normal(shared_keys[2], (D_MODEL, q_width), d_scale).astype(jnp.bfloat16),
        'b_q': normal(shared_keys[3], (q_width,), 0.5),
        'w_k': normal(shared_keys[4], (D_MODEL, kv_width), d_scale).astype(jnp.bfloat16),
        'b_k': normal(shared_keys[5], (kv_width,), 0.5),
        'w_v': normal(shared_keys[6], (D_MODEL, kv_width), d_scale).astype(jnp.bfloat16),
        'b_v': normal(shared_keys[7], (kv_width,), 0.5),
        'w_o': normal(shared_keys[8], (q_width, D_MODEL), q_width ** -0.5).astype(jnp.bfloat16),
        'b_o': normal(shared_keys[9], (D_MODEL,), 0.3),
        'ln2_gain': 1.0 + normal(shared_keys[10], (D_MODEL,), 0.3),
        'ln2_bias': normal(shared_keys[11], (D_MODEL,), 0.3),
        'w_router': normal(shared_keys[12], (D_MODEL, NUM_EXPERTS), 1.5 * d_scale).astype(jnp.bfloat16),
        'w_gate': normal(shared_keys[13], (NUM_EXPERTS, D_MODEL, FF_DIM), d_scale).astype(jnp.bfloat16),
        'w_up': normal(shared_keys[14], (NUM_EXPERTS, D_MODEL, FF_DIM), d_scale).astype(jnp.bfloat16),
        'w_down': normal(shared_keys[15], (NUM_EXPERTS, FF_DIM, D_MODEL), FF_DIM ** -0.5).astype(jnp.bfloat16),
        'long_factor': jnp.exp(jax.random.uniform(shared_keys[16], (HALF_DIM,), jnp.float32, 0.0, 3.5)),
        'expert_idx': expert_idx,
        'route_mask': route_mask,
    }


def layer_norm(x_in, gain_vec, bias_vec):
    x_f32 = x_in.astype(jnp.float32)
    mean_val = jnp.mean(x_f32, axis=-1, keepdims=True)
    centered = x_f32 - mean_val
    var_val = jnp.mean(centered * centered, axis=-1, keepdims=True)
    return (centered * lax.rsqrt(var_val + NORM_EPS) * gain_vec + bias_vec).astype(jnp.bfloat16)


def rotate_heads(x_in, angles):
    cos_half = jnp.cos(angles) * ROPE_MSCALE
    sin_half = jnp.sin(angles) * ROPE_MSCALE
    cos_full = jnp.concatenate([cos_half, cos_half], axis=-1)[:, None, :]
    sin_full = jnp.concatenate([sin_half, sin_half], axis=-1)[:, None, :]
    x_f32 = x_in.astype(jnp.float32)
    rotated = jnp.concatenate([-x_f32[..., HALF_DIM:], x_f32[..., :HALF_DIM]], axis=-1)
    return (x_f32 * cos_full + rotated * sin_full).astype(jnp.bfloat16)


def partial_stats(q_grp, keys, values, keep_mask):
    scores = jnp.einsum('bkgd,btkd->bkgt', q_grp.astype(jnp.float32), keys.astype(jnp.float32)) * (HEAD_DIM ** -0.5)
    keep_full = keep_mask[:, None, None, :]
    scores = jnp.where(keep_full, scores, NEG_FILL)
    run_max = jnp.max(scores, axis=-1)
    weights = jnp.where(keep_full, jnp.exp(scores - run_max[..., None]), 0.0)
    run_sum = jnp.sum(weights, axis=-1)
    out_part = jnp.einsum('bkgt,btkd->bkgd', weights.astype(jnp.bfloat16).astype(jnp.float32), values.astype(jnp.float32))
    return run_max, run_sum, out_part


def reference(x_first, next_emb, k_cache, v_cache, seq_len, ln1_gain, ln1_bias, w_q, b_q, w_k, b_k, w_v, b_v, w_o, b_o, ln2_gain, ln2_bias, w_router, w_gate, w_up, w_down, long_factor, expert_idx, route_mask):
    inv_freq = 1.0 / (long_factor * ROPE_BASE ** (jnp.arange(HALF_DIM, dtype=jnp.float32) * 2.0 / HEAD_DIM))
    step_inputs = jnp.concatenate([x_first[None], next_emb], axis=0)
    shard_ids = jnp.arange(KV_GROUP)
    tail_slots = jnp.arange(NUM_STEPS)

    def decode_step(step_carry, step_in):
        tail_k, tail_v = step_carry
        x_in, idx_step, mask_step, step_idx = step_in
        h_norm = layer_norm(x_in, ln1_gain, ln1_bias)
        q_new = (jnp.dot(h_norm, w_q, preferred_element_type=jnp.float32) + b_q).astype(jnp.bfloat16).reshape(BATCH_SIZE, Q_HEADS, HEAD_DIM)
        k_new = (jnp.dot(h_norm, w_k, preferred_element_type=jnp.float32) + b_k).astype(jnp.bfloat16).reshape(BATCH_SIZE, KV_HEADS, HEAD_DIM)
        v_new = (jnp.dot(h_norm, w_v, preferred_element_type=jnp.float32) + b_v).astype(jnp.bfloat16).reshape(BATCH_SIZE, KV_HEADS, HEAD_DIM)
        angles = (seq_len + step_idx).astype(jnp.float32)[:, None] * inv_freq[None, :]
        q_grp = rotate_heads(q_new, angles).reshape(BATCH_SIZE, KV_HEADS, Q_GROUP, HEAD_DIM)
        k_rot = rotate_heads(k_new, angles)
        tail_k = lax.dynamic_update_slice_in_dim(tail_k, k_rot[:, None], step_idx, axis=1)
        tail_v = lax.dynamic_update_slice_in_dim(tail_v, v_new[:, None], step_idx, axis=1)

        def one_shard(shard_id):
            k_blk = lax.dynamic_slice_in_dim(k_cache, shard_id * SHARD_LEN, SHARD_LEN, axis=1)
            v_blk = lax.dynamic_slice_in_dim(v_cache, shard_id * SHARD_LEN, SHARD_LEN, axis=1)
            positions = shard_id * SHARD_LEN + jnp.arange(SHARD_LEN)
            keep_mask = positions[None, :] < seq_len[:, None]
            return partial_stats(q_grp, k_blk, v_blk, keep_mask)

        cache_max, cache_sum, cache_out = lax.map(one_shard, shard_ids)
        tail_keep = jnp.broadcast_to(tail_slots[None, :] <= step_idx, (BATCH_SIZE, NUM_STEPS))
        tail_max, tail_sum, tail_out = partial_stats(q_grp, tail_k, tail_v, tail_keep)
        max_all = jnp.concatenate([cache_max, tail_max[None]], axis=0)
        sum_all = jnp.concatenate([cache_sum, tail_sum[None]], axis=0)
        out_all = jnp.concatenate([cache_out, tail_out[None]], axis=0)
        top_max = jnp.max(max_all, axis=0, keepdims=True)
        factor = jnp.exp(max_all - top_max)
        total_sum = jnp.sum(sum_all * factor, axis=0)
        merged = jnp.sum(out_all * factor[..., None], axis=0) / total_sum[..., None]
        attn_out = merged.reshape(BATCH_SIZE, Q_HEADS * HEAD_DIM).astype(jnp.bfloat16)
        x_mid = (x_in.astype(jnp.float32) + jnp.dot(attn_out, w_o, preferred_element_type=jnp.float32) + b_o).astype(jnp.bfloat16)
        h_moe = layer_norm(x_mid, ln2_gain, ln2_bias)
        logits = jnp.dot(h_moe, w_router, preferred_element_type=jnp.float32)
        masked = jnp.where(mask_step == 1, logits[:, None, :], NEG_FILL)
        gate_probs = jax.nn.softmax(masked, axis=-1)
        chosen = idx_step[..., None] == jnp.arange(NUM_EXPERTS)[None, None, :]
        gate_mat = jnp.sum(jnp.where(chosen, gate_probs, 0.0), axis=1)

        def expert_body(part_acc, expert_in):
            gate_w, up_w, down_w, gate_col = expert_in
            act_gate = jnp.dot(h_moe, gate_w, preferred_element_type=jnp.float32)
            act_up = jnp.dot(h_moe, up_w, preferred_element_type=jnp.float32)
            mixed_act = (gate_col[:, None] * jax.nn.silu(act_gate) * act_up).astype(jnp.bfloat16)
            blocks = mixed_act.reshape(BATCH_SIZE, KV_GROUP, FF_SHARD).astype(jnp.float32)
            down_blocks = down_w.reshape(KV_GROUP, FF_SHARD, D_MODEL).astype(jnp.float32)
            return part_acc + jnp.einsum('bjf,jfd->bjd', blocks, down_blocks), None

        part_init = jnp.zeros((BATCH_SIZE, KV_GROUP, D_MODEL), jnp.float32)
        part_acc = lax.scan(expert_body, part_init, (w_gate, w_up, w_down, gate_mat.T))[0]
        moe_out = jnp.sum(part_acc.astype(jnp.bfloat16).astype(jnp.float32), axis=1)
        x_out = (x_mid.astype(jnp.float32) + moe_out).astype(jnp.bfloat16)
        return (tail_k, tail_v), x_out

    tail_init = jnp.zeros((BATCH_SIZE, NUM_STEPS, KV_HEADS, HEAD_DIM), jnp.bfloat16)
    final_carry, hidden = lax.scan(decode_step, (tail_init, tail_init), (step_inputs, expert_idx, route_mask, jnp.arange(NUM_STEPS)))
    return hidden, final_carry[0], final_carry[1]
```

```python
import functools
import math

import jax
import jax.numpy as jnp
from jax import lax
from jax.experimental import pallas as pl
from jax.experimental.pallas import tpu as pltpu
from jax.sharding import PartitionSpec as P

ROPE_BASE = 10000.0
ROPE_MSCALE = math.sqrt(1.0 + math.log(32.0) / math.log(4096.0))
NORM_EPS = 1e-5
NEG_FILL = -1e30
LANES = 128
SUBL = 8
F32 = jnp.float32
BF16 = jnp.bfloat16
NT = (((1,), (1,)), ((), ()))


def norm_rows(x, gain, bias):
    mean = jnp.mean(x, axis=-1, keepdims=True)
    cent = x - mean
    var = jnp.mean(cent * cent, axis=-1, keepdims=True)
    return (cent * lax.rsqrt(var + NORM_EPS) * gain + bias).astype(BF16)


def layer_kernel(dims, x_first, next_emb, k_hbm, v_hbm, len_hbm, g1_hbm, b1_hbm, wq_hbm, bq_hbm, wk_hbm, bk_hbm, wv_hbm, bv_hbm, wo_hbm, bo_hbm, g2_hbm, b2_hbm, wr_hbm, wg_hbm, wu_hbm, wd_hbm, lf_hbm, idx_hbm, mask_hbm,
                 hid_out, tk_out, tv_out,
                 x_s, len_s, lf_s, vec_s, bk_s, bv_s, wr_s, idx_s, mask_s,
                 wq_s, wk_s, wv_s, wo_s, k_s, v_s, wg_s, wu_s, wd_s,
                 q_s, kt_s, vt_s, hs_s, p_s, msg_s, recv_s, obuf_s, xm_s, gex_s, u_s, pbuf_s, rbuf_s, ybuf_s,
                 small_sem, wq_sem, wkv_sem, wo_sem, k_sem, v_sem, exp_sem, wd_sem,
                 a_send, a_recv, o_send, o_recv, p_send, p_recv, y_send, y_recv):
    n, steps, batch, heads_kv, hd, group, shard, n_exp, ff, dm = dims
    rows = steps * batch
    gs_n = group * steps
    qrows = (gs_n + 1) * heads_kv
    hdk = heads_kv * hd
    n_hp = hdk // LANES
    half_b = batch // 2
    me = lax.axis_index('kv')
    chip = me // 2
    core = lax.rem(me, 2)

    barrier = pltpu.get_barrier_semaphore()
    for d in range(1, n):
        pl.semaphore_signal(barrier, inc=1, device_id={'kv': lax.rem(me + d, n)}, device_id_type=pl.DeviceIdType.MESH)

    smalls = [(x_first, x_s.at[0])] + [(next_emb.at[i], x_s.at[i + 1]) for i in range(steps - 1)]
    smalls += [(len_hbm, len_s), (lf_hbm, lf_s)]
    smalls += [(src, vec_s.at[i]) for i, src in enumerate((g1_hbm, b1_hbm, bq_hbm, bo_hbm, g2_hbm, b2_hbm))]
    smalls += [(bk_hbm, bk_s), (bv_hbm, bv_s), (wr_hbm, wr_s), (idx_hbm, idx_s), (mask_hbm, mask_s)]
    small_copies = [pltpu.make_async_copy(src, dst, small_sem.at[i]) for i, (src, dst) in enumerate(smalls)]
    qw = wq_s.shape[2]
    wq_copies = [pltpu.make_async_copy(wq_hbm.at[:, pl.ds(i * qw, qw)], wq_s.at[i], wq_sem.at[i]) for i in range(n_hp)]
    wkv_copies = [pltpu.make_async_copy(wk_hbm, wk_s, wkv_sem.at[0]), pltpu.make_async_copy(wv_hbm, wv_s, wkv_sem.at[1])]
    for cp in small_copies + wq_copies + wkv_copies:
        cp.start()

    def seq_of(it):
        return lax.rem(core * half_b + it, batch)

    def k_copy(b):
        return pltpu.make_async_copy(k_hbm.at[b], k_s.at[b], k_sem.at[b])

    def v_copy(b):
        return pltpu.make_async_copy(v_hbm.at[b], v_s.at[b], v_sem.at[b])

    for it in range(batch):
        k_copy(seq_of(it)).start()
    for it in range(batch):
        v_copy(seq_of(it)).start()
    wo_copies = [pltpu.make_async_copy(wo_hbm.at[:, g], wo_s.at[g], wo_sem.at[g]) for g in range(group)]
    n_ec = wg_s.shape[0] // LANES
    ec_part = 4
    ec_rows = wg_s.shape[0] // ec_part
    exp_copies = []
    for i in range(ec_part):
        sl = pl.ds(i * ec_rows, ec_rows)
        exp_copies.append(pltpu.make_async_copy(wg_hbm.at[sl], wg_s.at[sl], exp_sem.at[0, i]))
        exp_copies.append(pltpu.make_async_copy(wu_hbm.at[sl], wu_s.at[sl], exp_sem.at[1, i]))
    wd_copies = [pltpu.make_async_copy(wd_hbm.at[pl.ds(i * ec_rows, ec_rows)], wd_s.at[pl.ds(i * ec_rows, ec_rows)], wd_sem.at[i]) for i in range(ec_part)]

    for cp in small_copies:
        cp.wait()

    g1, b1, bq, bo, g2, b2 = [vec_s[i].reshape(1, dm) for i in range(6)]
    x = x_s[...].reshape(rows, dm).astype(F32)
    h = norm_rows(x, g1, b1)

    lane1 = lax.broadcasted_iota(jnp.int32, (1, LANES), 1)
    half_dim = hd // 2
    jlane = lax.rem(lane1, half_dim)
    lfv = jnp.zeros((1, LANES), F32)
    for j in range(half_dim):
        lfv = jnp.where(jlane == j, lf_s[j], lfv)
    inv = 1.0 / (lfv * jnp.exp(jlane.astype(F32) * (2.0 * math.log(ROPE_BASE) / hd)))
    subb = lax.broadcasted_iota(jnp.int32, (batch, LANES), 0)
    pos = jnp.zeros((batch, LANES), jnp.int32)
    for b in range(batch):
        pos = jnp.where(subb == b, len_s[b], pos)
    ang = jnp.concatenate([(pos + s).astype(F32) * inv for s in range(steps)], axis=0)
    cos = jnp.cos(ang) * ROPE_MSCALE
    sin = jnp.sin(ang) * ROPE_MSCALE
    lane_r = lax.broadcasted_iota(jnp.int32, (rows, LANES), 1)
    sin = jnp.where(lax.rem(lane_r, hd) < half_dim, -sin, sin)
    low_half = lax.rem(lane_r, hd) < half_dim
    low_head = lane_r < hd

    def rope(t):
        t = t.astype(BF16).astype(F32)
        rot = jnp.where(low_half, pltpu.roll(t, LANES - half_dim, 1), pltpu.roll(t, half_dim, 1))
        return (t * cos + rot * sin).astype(BF16).astype(F32)

    for hp in range(n_hp):
        wq_copies[hp].wait()
        t = jnp.dot(h, wq_s[hp], preferred_element_type=F32) + bq[:, hp * qw:(hp + 1) * qw]
        parts = [rope(t[:, c * LANES:(c + 1) * LANES]) for c in range(qw // LANES)]
        for g in range(group):
            first, second = g, group + g
            a, a_hi = parts[first // 2], first % 2
            c, c_hi = parts[second // 2], second % 2
            a = pltpu.roll(a, hd, 1) if a_hi else a
            c = c if c_hi else pltpu.roll(c, hd, 1)
            q_s[hp, g * steps:(g + 1) * steps] = jnp.where(low_head, a, c).reshape(steps, batch, LANES)
    for cp in wkv_copies:
        cp.wait()
    t = jnp.dot(h, wk_s[...], preferred_element_type=F32) + bk_s[...].reshape(1, hdk)
    for hp in range(n_hp):
        kt_s[hp] = rope(t[:, hp * LANES:(hp + 1) * LANES]).reshape(steps, batch, LANES)
    t = (jnp.dot(h, wv_s[...], preferred_element_type=F32) + bv_s[...].reshape(1, hdk)).astype(BF16).astype(F32)
    for hp in range(n_hp):
        vt_s[hp] = t[:, hp * LANES:(hp + 1) * LANES].reshape(steps, batch, LANES)

    for cp in wo_copies + exp_copies + wd_copies:
        cp.start()

    tpos = me * shard + lax.broadcasted_iota(jnp.int32, (1, shard), 1)
    diag = lax.broadcasted_iota(jnp.int32, (heads_kv, hdk), 0) == lax.broadcasted_iota(jnp.int32, (heads_kv, hdk), 1) // hd
    ident = lax.broadcasted_iota(jnp.int32, (qrows, LANES), 0) == lax.broadcasted_iota(jnp.int32, (qrows, LANES), 1)

    def to_row(col):
        return jnp.sum(jnp.where(ident, col, 0.0), axis=0, keepdims=True)

    def scores(it, _):
        b = seq_of(it)
        k_copy(b).wait()
        blocks = []
        for gs in range(gs_n):
            qrow = jnp.concatenate([q_s[hp, gs, pl.ds(b, 1), :] for hp in range(n_hp)], axis=1)
            blocks.append(jnp.where(diag, qrow, 0.0))
        blocks.append(jnp.zeros((heads_kv, hdk), F32))
        qbd = jnp.concatenate(blocks, axis=0).astype(BF16)
        keep = tpos < len_s[b]
        sc = jnp.dot(qbd, k_s[b], preferred_element_type=F32) * (hd ** -0.5)
        sc = jnp.where(keep, sc, NEG_FILL)
        m = jnp.max(sc, axis=1, keepdims=True)
        w = jnp.where(keep, jnp.exp(sc - m), 0.0)
        p_s[b] = w.astype(BF16)
        half, b8 = b // half_b, lax.rem(b, half_b)
        msg_s[half, 0, gs_n, pl.ds(b8, 1), :] = to_row(m)
        msg_s[half, 0, gs_n + 1, pl.ds(b8, 1), :] = to_row(jnp.sum(w, axis=1, keepdims=True))
        return 0

    def outputs(it, _):
        b = seq_of(it)
        v_copy(b).wait()
        o = lax.dot_general(p_s[b], v_s[b], NT, preferred_element_type=F32)
        half, b8 = b // half_b, lax.rem(b, half_b)
        for gs in range(gs_n):
            row = jnp.sum(jnp.where(diag, o[gs * heads_kv:(gs + 1) * heads_kv], 0.0), axis=0, keepdims=True)
            for hp in range(n_hp):
                msg_s[half, hp, gs, pl.ds(b8, 1), :] = row[:, hp * LANES:(hp + 1) * LANES]
        return 0

    def a_copy(half, hp, slot):
        return pltpu.make_async_remote_copy(
            src_ref=msg_s.at[half, hp], dst_ref=recv_s.at[me], send_sem=a_send.at[slot], recv_sem=a_recv.at[me],
            device_id={'kv': hp * 2 + half}, device_id_type=pl.DeviceIdType.MESH)

    sends = []
    for turn in range(2):
        lax.fori_loop(turn * half_b, (turn + 1) * half_b, scores, 0, unroll=4)
        lax.fori_loop(turn * half_b, (turn + 1) * half_b, outputs, 0, unroll=4)
        half = lax.rem(core + turn, 2)
        mt, lt = msg_s[half, 0, gs_n], msg_s[half, 0, gs_n + 1]
        for hp in range(1, n_hp):
            msg_s[half, hp, gs_n] = pltpu.roll(mt, LANES - 2 * hp, 1)
            msg_s[half, hp, gs_n + 1] = pltpu.roll(lt, LANES - 2 * hp, 1)
        if turn == 0:
            pl.semaphore_wait(barrier, n - 1)
        for dx in (2, 1, 3, 0):
            hp = lax.rem(chip + dx, n_hp)
            if turn == 0 and dx == 0:
                recv_s[me] = msg_s[half, hp]
            else:
                cp = a_copy(half, hp, len(sends))
                cp.start()
                sends.append(cp)

    lane8 = lax.broadcasted_iota(jnp.int32, (half_b, LANES), 1)
    low8 = lane8 < hd
    brow = pl.ds(pl.multiple_of(core * half_b, half_b), half_b)
    m_tail = jnp.full((half_b, LANES), NEG_FILL, F32)
    l_tail = jnp.zeros((half_b, LANES), F32)
    for gs in range(gs_n):
        s = gs % steps
        qt = q_s[chip, gs, brow, :]
        cols = []
        for slot in range(s + 1):
            prod = qt * kt_s[chip, slot, brow, :]
            lo = jnp.sum(jnp.where(low8, prod, 0.0), axis=1, keepdims=True)
            hi = jnp.sum(jnp.where(low8, 0.0, prod), axis=1, keepdims=True)
            cols.append(jnp.where(low8, lo, hi) * (hd ** -0.5))
        mx = functools.reduce(jnp.maximum, cols)
        ws = [jnp.exp(c - mx) for c in cols]
        lsum = functools.reduce(jnp.add, ws)
        acc = functools.reduce(jnp.add, [w.astype(BF16).astype(F32) * vt_s[chip, slot, brow, :] for slot, w in enumerate(ws)])
        recv_s[n, gs] = acc
        for j in range(2):
            sel = lane8 == gs * heads_kv + j
            m_tail = jnp.where(sel, mx[:, j * hd:j * hd + 1], m_tail)
            l_tail = jnp.where(sel, lsum[:, j * hd:j * hd + 1], l_tail)


    def a_wait(src):
        pltpu.make_async_remote_copy(
            src_ref=msg_s.at[0, 0], dst_ref=recv_s.at[src], send_sem=a_send.at[0], recv_sem=a_recv.at[src],
            device_id={'kv': me}, device_id_type=pl.DeviceIdType.MESH).wait_recv()

    for d in range(1, n):
        a_wait(lax.rem(me + d, n))
    ms = [recv_s[src, gs_n] for src in range(n)] + [m_tail]
    ls = [recv_s[src, gs_n + 1] for src in range(n)] + [l_tail]
    mx = functools.reduce(jnp.maximum, ms)
    al = [jnp.exp(m - mx) for m in ms]
    tot = functools.reduce(jnp.add, [a * l for a, l in zip(al, ls)])
    for gs in range(gs_n):
        def spread(t):
            lane = gs * heads_kv
            return jnp.where(low8, t[:, lane:lane + 1], t[:, lane + 1:lane + 2])
        acc = functools.reduce(jnp.add, [spread(a) * recv_s[src, gs] for src, a in enumerate(al)])
        obuf_s[me, gs] = (acc / spread(tot)).astype(BF16).astype(F32)

    def bcast(buf, send, recv):
        out = []
        for i, d in enumerate((4, 5, 2, 6, 3, 7, 1)):
            cp = pltpu.make_async_remote_copy(
                src_ref=buf.at[me], dst_ref=buf.at[me], send_sem=send.at[i], recv_sem=recv.at[me],
                device_id={'kv': lax.rem(me + d, n)}, device_id_type=pl.DeviceIdType.MESH)
            cp.start()
            out.append(cp)
        return out

    def wait_all(buf, send, recv):
        for d in range(1, n):
            src = lax.rem(me + d, n)
            pltpu.make_async_remote_copy(
                src_ref=buf.at[src], dst_ref=buf.at[src], send_sem=send.at[0], recv_sem=recv.at[src],
                device_id={'kv': me}, device_id_type=pl.DeviceIdType.MESH).wait_recv()

    sends += bcast(obuf_s, o_send, o_recv)

    for src_s, dst in ((kt_s, tk_out), (vt_s, tv_out)):
        for hp in range(n_hp):
            t = src_s[hp].reshape(rows, LANES)
            hs_s[:, 2 * hp, :] = t[:, :hd]
            hs_s[:, 2 * hp + 1, :] = pltpu.roll(t, hd, 1)[:, :hd]
        for s in range(steps):
            dst[:, s] = hs_s[s * batch:(s + 1) * batch].astype(BF16)

    for cp in wo_copies:
        cp.wait()
    wait_all(obuf_s, o_send, o_recv)
    pieces = []
    for g in range(group):
        for hp in range(n_hp):
            pieces.append(jnp.concatenate([obuf_s[hp * 2 + half, g * steps + s] for s in range(steps) for half in range(2)], axis=0))
    o_all = jnp.concatenate(pieces, axis=1).astype(BF16)
    x = x_s[...].reshape(rows, dm).astype(F32)
    xm = (x + jnp.dot(o_all, wo_s[...].reshape(dm, dm), preferred_element_type=F32) + bo).astype(BF16).astype(F32)
    xm_s[...] = xm.reshape(2, rows // 2, dm)
    h2 = norm_rows(xm, g2, b2)

    logits = lax.dot_general(h2, wr_s[...], NT, preferred_element_type=F32)
    topk = mask_s.shape[1]
    e_iota = lax.broadcasted_iota(jnp.int32, (topk, n_exp), 1)
    grows = []
    for s in range(steps):
        ids = idx_s[s]
        for b in range(batch):
            r = s * batch + b
            lg = jnp.where(mask_s[r] == 1, logits[r:r + 1, :], NEG_FILL)
            ex = jnp.exp(lg - jnp.max(lg, axis=1, keepdims=True))
            pr = ex / jnp.sum(ex, axis=1, keepdims=True)
            grows.append(jnp.sum(jnp.where(ids[:, b:b + 1] == e_iota, pr, 0.0), axis=0, keepdims=True))
    gates = jnp.concatenate(grows, axis=0)
    per = LANES // ff
    for c in range(n_ec):
        gex_s[c] = jnp.where(low_head, gates[:, per * c:per * c + 1], gates[:, per * c + 1:per * c + 2])

    for cp in exp_copies:
        cp.wait()

    def expert(c, _):
        rs = pl.ds(pl.multiple_of(c * LANES, LANES), LANES)
        ag = lax.dot_general(h2, wg_s[rs, :], NT, preferred_element_type=F32)
        au = lax.dot_general(h2, wu_s[rs, :], NT, preferred_element_type=F32)
        u_s[c] = (gex_s[c] * (ag * (1.0 / (1.0 + jnp.exp(-ag)))) * au).astype(BF16)
        return 0

    lax.fori_loop(0, n_ec, expert, 0, unroll=2)

    for cp in wd_copies:
        cp.wait()
    cw = dm // n_hp
    hr = rows // 2
    u = jnp.concatenate([u_s[c] for c in range(n_ec)], axis=1)
    k = 0
    for dx in (2, 1, 3, 0):
        cq = lax.rem(chip + dx, n_hp)
        part = jnp.dot(u, wd_s[:, pl.ds(pl.multiple_of(cq * cw, LANES), cw)], preferred_element_type=F32)
        part = part.astype(BF16).astype(F32)
        for half in range(2):
            pbuf_s[cq * 2 + half] = part[half * hr:(half + 1) * hr]
        for dc in range(2):
            half = lax.rem(core + 1 + dc, 2)
            owner = cq * 2 + half
            if dx == 0 and dc == 1:
                rbuf_s[me] = pbuf_s[me]
            else:
                cp = pltpu.make_async_remote_copy(
                    src_ref=pbuf_s.at[owner], dst_ref=rbuf_s.at[me], send_sem=p_send.at[k], recv_sem=p_recv.at[me],
                    device_id={'kv': owner}, device_id_type=pl.DeviceIdType.MESH)
                cp.start()
                sends.append(cp)
                k += 1
    wait_all(rbuf_s, p_send, p_recv)
    tot = functools.reduce(jnp.add, [rbuf_s[src] for src in range(n)])
    y = xm_s[core, :, pl.ds(pl.multiple_of(chip * cw, LANES), cw)] + tot
    ybuf_s[me] = y.astype(BF16).astype(F32)
    sends += bcast(ybuf_s, y_send, y_recv)
    wait_all(ybuf_s, y_send, y_recv)
    for cq in range(n_hp):
        blk = jnp.concatenate([ybuf_s[cq * 2], ybuf_s[cq * 2 + 1]], axis=0)
        hid_out[:, :, cq * cw:(cq + 1) * cw] = blk.astype(BF16).reshape(steps, batch, cw)
    for cp in sends:
        cp.wait_send()


def solution(mesh):
    n = mesh.shape['kv']

    def layer_steps(x_first, next_emb, k_cache, v_cache, seq_len, ln1_gain, ln1_bias, w_q, b_q, w_k, b_k, w_v, b_v, w_o, b_o, ln2_gain, ln2_bias, w_router, w_gate, w_up, w_down, long_factor, expert_idx, route_mask):
        batch, shard, heads_kv, hd = k_cache.shape
        dm = x_first.shape[1]
        q_heads = w_q.shape[1] // hd
        group = q_heads // heads_kv
        steps = next_emb.shape[0] + 1
        n_exp, _, ff = w_gate.shape
        topk = expert_idx.shape[-1]
        rows = steps * batch
        hdk = heads_kv * hd
        n_hp = hdk // LANES
        gs_n = group * steps
        qrows = (gs_n + 1) * heads_kv
        fe = n_exp * ff
        dims = (n, steps, batch, heads_kv, hd, group, shard, n_exp, ff, dm)
        args = (
            x_first, next_emb,
            jnp.transpose(k_cache, (0, 2, 3, 1)).reshape(batch, hdk, shard),
            jnp.transpose(v_cache, (0, 2, 3, 1)).reshape(batch, hdk, shard),
            seq_len, ln1_gain, ln1_bias, w_q, b_q, w_k, b_k, w_v, b_v,
            w_o.reshape(heads_kv, group, hd, dm), b_o, ln2_gain, ln2_bias,
            jnp.transpose(w_router),
            jnp.transpose(w_gate, (0, 2, 1)).reshape(fe, dm),
            jnp.transpose(w_up, (0, 2, 1)).reshape(fe, dm),
            w_down.reshape(fe, dm), long_factor,
            jnp.transpose(expert_idx, (0, 2, 1)),
            route_mask.reshape(rows, topk, n_exp),
        )
        any_spec = pl.BlockSpec(memory_space=pl.ANY)
        vmem_spec = pl.BlockSpec(memory_space=pltpu.VMEM)
        dma = pltpu.SemaphoreType.DMA
        vm = pltpu.VMEM
        scratch = [
            vm((steps, batch, dm), BF16), pltpu.SMEM((batch,), jnp.int32), pltpu.SMEM((hd // 2,), F32),
            vm((6, dm), F32), vm((hdk,), F32), vm((hdk,), F32), vm((n_exp, dm), BF16),
            vm((steps, topk, batch), jnp.int32), vm((rows, topk, n_exp), jnp.int32),
            vm((n_hp, dm, dm // n_hp), BF16), vm((dm, hdk), BF16), vm((dm, hdk), BF16),
            vm((group, heads_kv, hd, dm), BF16), vm((batch, hdk, shard), BF16), vm((batch, hdk, shard), BF16),
            vm((fe, dm), BF16), vm((fe, dm), BF16), vm((fe, dm), BF16),
            vm((n_hp, gs_n, batch, LANES), F32), vm((n_hp, steps, batch, LANES), F32), vm((n_hp, steps, batch, LANES), F32),
            vm((rows, heads_kv, hd), F32), vm((batch, qrows, shard), BF16),
            vm((2, n_hp, gs_n + 2, SUBL, LANES), F32), vm((n + 1, gs_n + 2, SUBL, LANES), F32),
            vm((n, gs_n, SUBL, LANES), F32), vm((2, rows // 2, dm), F32),
            vm((fe // LANES, rows, LANES), F32), vm((fe // LANES, rows, LANES), BF16),
            vm((n, rows // 2, dm // n_hp), F32), vm((n, rows // 2, dm // n_hp), F32), vm((n, rows // 2, dm // n_hp), F32),
            dma((steps + 13,)), dma((n_hp,)), dma((2,)), dma((group,)), dma((batch,)), dma((batch,)), dma((2, 4)), dma((4,)),
            dma((n,)), dma((n,)), dma((n,)), dma((n,)), dma((n,)), dma((n,)), dma((n,)), dma((n,)),
        ]
        return pl.pallas_call(
            functools.partial(layer_kernel, dims),
            out_shape=(
                jax.ShapeDtypeStruct((steps, batch, dm), BF16),
                jax.ShapeDtypeStruct((batch, steps, heads_kv, hd), BF16),
                jax.ShapeDtypeStruct((batch, steps, heads_kv, hd), BF16),
            ),
            in_specs=[any_spec] * len(args),
            out_specs=(vmem_spec,) * 3,
            scratch_shapes=scratch,
            compiler_params=pltpu.CompilerParams(collective_id=0, has_side_effects=True, vmem_limit_bytes=66 * 1024 * 1024 - 2 * 1024 * 1024),
        )(*args)

    replicated = P()
    in_specs = (P('dp'), P(None, 'dp'), P('dp', 'kv'), P('dp', 'kv'), P('dp')) + (replicated,) * 13 + (P(None, None, 'kv'), P(None, None, 'kv'), P(None, 'kv'), replicated, P(None, 'dp'), P(None, 'dp'))
    out_specs = (P(None, 'dp'), P('dp'), P('dp'))
    return jax.shard_map(layer_steps, mesh=mesh, in_specs=in_specs, out_specs=out_specs, check_vma=False)
```

```python
import functools
import math

import jax
import jax.numpy as jnp
from jax import lax
from jax.experimental import pallas as pl
from jax.experimental.pallas import tpu as pltpu
from jax.sharding import PartitionSpec as P

ROPE_BASE = 10000.0
ROPE_MSCALE = math.sqrt(1.0 + math.log(32.0) / math.log(4096.0))
NORM_EPS = 1e-5
NEG_FILL = -1e30
LANES = 128
SUBL = 8
F32 = jnp.float32
BF16 = jnp.bfloat16
NT = (((1,), (1,)), ((), ()))


def norm_rows(x, gain, bias):
    mean = jnp.mean(x, axis=-1, keepdims=True)
    cent = x - mean
    var = jnp.mean(cent * cent, axis=-1, keepdims=True)
    return (cent * lax.rsqrt(var + NORM_EPS) * gain + bias).astype(BF16)


def layer_kernel(dims, x_first, next_emb, k_hbm, v_hbm, len_hbm, g1_hbm, b1_hbm, wq_hbm, bq_hbm, wk_hbm, bk_hbm, wv_hbm, bv_hbm, wo_hbm, bo_hbm, g2_hbm, b2_hbm, wr_hbm, wg_hbm, wu_hbm, wd_hbm, lf_hbm, idx_hbm, mask_hbm,
                 hid_out, tk_out, tv_out,
                 x_s, len_s, lf_s, vec_s, bk_s, bv_s, wr_s, idx_s, mask_s,
                 wq_s, wk_s, wv_s, wo_s, k_s, v_s, wg_s, wu_s, wd_s,
                 q_s, kt_s, vt_s, hs_s, p_s, msg_s, pair_s, amsg_s, recv_s, obuf_s, xm_s, gex_s, u_s, pbuf_s, ppair_s, psum_s, rbuf_s, ybuf_s,
                 hid_s, tk_s, tv_s,
                 small_sem, wq_sem, wkv_sem, wo_sem, k_sem, v_sem, exp_sem, wd_sem, out_sem,
                 pair_sem, a_send, a_recv, o_send, o_recv, d_send, d_recv, p_send, p_recv, y_send, y_recv):
    n, steps, batch, heads_kv, hd, group, shard, n_exp, ff, dm = dims
    rows = steps * batch
    gs_n = group * steps
    qrows = (gs_n + 1) * heads_kv
    hdk = heads_kv * hd
    n_hp = hdk // LANES
    half_b = batch // 2
    me = lax.axis_index('kv')
    chip = me // 2
    core = lax.rem(me, 2)
    other = 1 - core
    partner = chip * 2 + other
    mesh_id = pl.DeviceIdType.MESH

    def remote(src, dst, send, recv, dev):
        return pltpu.make_async_remote_copy(src_ref=src, dst_ref=dst, send_sem=send, recv_sem=recv, device_id={'kv': dev}, device_id_type=mesh_id)

    vecs = (g1_hbm, b1_hbm, bq_hbm, bo_hbm, g2_hbm, b2_hbm)
    smalls = [(x_first, x_s.at[0], 0), (next_emb, x_s.at[pl.ds(1, steps - 1)], 0)]
    smalls += [(len_hbm, len_s, 1), (lf_hbm, lf_s, 2), (bk_hbm, bk_s, 3), (bv_hbm, bv_s, 4), (wr_hbm, wr_s, 5), (idx_hbm, idx_s, 6), (mask_hbm, mask_s, 7)]
    smalls += [(src, vec_s.at[i], 8 + i) for i, src in enumerate(vecs)]
    small_copies = [pltpu.make_async_copy(src, dst, small_sem.at[i]) for src, dst, i in smalls]
    small_waits = [pltpu.make_async_copy(x_s, x_s, small_sem.at[0])] + small_copies[2:]
    qw = wq_s.shape[2]
    wq_copies = [pltpu.make_async_copy(wq_hbm.at[:, pl.ds(i * qw, qw)], wq_s.at[i], wq_sem.at[i]) for i in range(n_hp)]
    wkv_copies = [pltpu.make_async_copy(wk_hbm, wk_s, wkv_sem.at[0]), pltpu.make_async_copy(wv_hbm, wv_s, wkv_sem.at[1])]
    for cp in small_copies + wq_copies + wkv_copies:
        cp.start()

    barrier = pltpu.get_barrier_semaphore()
    for d in range(1, n):
        pl.semaphore_signal(barrier, inc=1, device_id={'kv': lax.rem(me + d, n)}, device_id_type=mesh_id)

    quad = half_b // 2
    n_quad = batch // quad

    def quad_base(i):
        return pl.multiple_of((other if i < n_quad // 2 else core) * half_b + (i % 2) * quad, quad)

    def cache_copy(src, dst, sem, i):
        sl = pl.ds(quad_base(i), quad)
        return pltpu.make_async_copy(src.at[sl], dst.at[sl], sem.at[i])

    k_copies = [cache_copy(k_hbm, k_s, k_sem, i) for i in range(n_quad)]
    v_copies = [cache_copy(v_hbm, v_s, v_sem, i) for i in range(n_quad)]
    n_ec = wg_s.shape[0] // LANES

    def weight_start(src, dst, sem, parts=4):
        ec = src.shape[0] // parts
        for i in range(parts):
            pltpu.make_async_copy(src.at[pl.ds(i * ec, ec)], dst.at[pl.ds(i * ec, ec)], sem).start()

    def weight_wait(dst, sem):
        pltpu.make_async_copy(dst, dst, sem).wait()

    for cp in small_waits:
        cp.wait()

    g1, b1, bq, bo, g2, b2 = [vec_s[i].reshape(1, dm) for i in range(6)]
    x = x_s[...].reshape(rows, dm).astype(F32)
    h = norm_rows(x, g1, b1)

    lane1 = lax.broadcasted_iota(jnp.int32, (1, LANES), 1)
    half_dim = hd // 2
    jlane = lax.rem(lane1, half_dim)
    lfv = jnp.zeros((1, LANES), F32)
    for j in range(half_dim):
        lfv = jnp.where(jlane == j, lf_s[j], lfv)
    inv = 1.0 / (lfv * jnp.exp(jlane.astype(F32) * (2.0 * math.log(ROPE_BASE) / hd)))
    subb = lax.broadcasted_iota(jnp.int32, (batch, LANES), 0)
    pos = jnp.zeros((batch, LANES), jnp.int32)
    for b in range(batch):
        pos = jnp.where(subb == b, len_s[b], pos)
    ang = jnp.concatenate([(pos + s).astype(F32) * inv for s in range(steps)], axis=0)
    cos = jnp.cos(ang) * ROPE_MSCALE
    sin = jnp.sin(ang) * ROPE_MSCALE
    lane_r = lax.broadcasted_iota(jnp.int32, (rows, LANES), 1)
    sin = jnp.where(lax.rem(lane_r, hd) < half_dim, -sin, sin)
    low_half = lax.rem(lane_r, hd) < half_dim
    low_head = lane_r < hd

    def rope(t):
        t = t.astype(BF16).astype(F32)
        rot = jnp.where(low_half, pltpu.roll(t, LANES - half_dim, 1), pltpu.roll(t, half_dim, 1))
        return (t * cos + rot * sin).astype(BF16).astype(F32)

    def q_block(hp):
        t = jnp.dot(h, wq_s[hp], preferred_element_type=F32) + bq[:, hp * qw:(hp + 1) * qw]
        parts = [rope(t[:, c * LANES:(c + 1) * LANES]) for c in range(qw // LANES)]
        for g in range(group):
            first, second = g, group + g
            a, a_hi = parts[first // 2], first % 2
            c, c_hi = parts[second // 2], second % 2
            a = pltpu.roll(a, hd, 1) if a_hi else a
            c = c if c_hi else pltpu.roll(c, hd, 1)
            q_s[hp, g * steps:(g + 1) * steps] = jnp.where(low_head, a, c).reshape(steps, batch, LANES)

    wq_copies[0].wait()
    for cp in (k_copies[0], k_copies[1], v_copies[0], k_copies[2]):
        cp.start()
    wq_copies[1].wait()
    for hp in range(2):
        q_block(hp)
    for cp in wq_copies[2:] + wkv_copies:
        cp.wait()
    for cp in (v_copies[1], k_copies[3], v_copies[2], v_copies[3]):
        cp.start()
    for hp in range(2, n_hp):
        q_block(hp)
    t = jnp.dot(h, wk_s[...], preferred_element_type=F32) + bk_s[...].reshape(1, hdk)
    for hp in range(n_hp):
        kt_s[hp] = rope(t[:, hp * LANES:(hp + 1) * LANES]).reshape(steps, batch, LANES)
    t = (jnp.dot(h, wv_s[...], preferred_element_type=F32) + bv_s[...].reshape(1, hdk)).astype(BF16).astype(F32)
    for hp in range(n_hp):
        vt_s[hp] = t[:, hp * LANES:(hp + 1) * LANES].reshape(steps, batch, LANES)

    tpos = me * shard + lax.broadcasted_iota(jnp.int32, (1, shard), 1)
    diag = lax.broadcasted_iota(jnp.int32, (heads_kv, hdk), 0) == lax.broadcasted_iota(jnp.int32, (heads_kv, hdk), 1) // hd
    ident = lax.broadcasted_iota(jnp.int32, (qrows, LANES), 0) == lax.broadcasted_iota(jnp.int32, (qrows, LANES), 1)
    m_slot = n_hp * gs_n

    def to_row(col):
        return jnp.sum(jnp.where(ident, col, 0.0), axis=0, keepdims=True)

    def scores(i):
        base = quad_base(i)
        half = other if i < n_quad // 2 else core
        for j in range(quad):
            b = base + j
            blocks = []
            for gs in range(gs_n):
                qrow = jnp.concatenate([q_s[hp, gs, pl.ds(b, 1), :] for hp in range(n_hp)], axis=1)
                blocks.append(jnp.where(diag, qrow, 0.0))
            blocks.append(jnp.zeros((heads_kv, hdk), F32))
            qbd = jnp.concatenate(blocks, axis=0).astype(BF16)
            keep = tpos < len_s[b]
            sc = jnp.dot(qbd, k_s[b], preferred_element_type=F32) * (hd ** -0.5)
            sc = jnp.where(keep, sc, NEG_FILL)
            m = jnp.max(sc, axis=1, keepdims=True)
            w = jnp.where(keep, jnp.exp(sc - m), 0.0)
            p_s[b] = w.astype(BF16)
            b8 = (i % 2) * quad + j
            msg_s[half, m_slot, b8:b8 + 1, :] = to_row(m)
            msg_s[half, m_slot + 1, b8:b8 + 1, :] = to_row(jnp.sum(w, axis=1, keepdims=True))

    def outputs(i):
        base = quad_base(i)
        half = other if i < n_quad // 2 else core
        for j in range(quad):
            b = base + j
            o = lax.dot_general(p_s[b], v_s[b], NT, preferred_element_type=F32)
            b8 = (i % 2) * quad + j
            for gs in range(gs_n):
                row = jnp.sum(jnp.where(diag, o[gs * heads_kv:(gs + 1) * heads_kv], 0.0), axis=0, keepdims=True)
                for hp in range(n_hp):
                    msg_s[half, hp * gs_n + gs, b8:b8 + 1, :] = row[:, hp * LANES:(hp + 1) * LANES]

    sends = []
    pair_cp = remote(msg_s.at[other], pair_s, pair_sem.at[0], pair_sem.at[1], partner)
    for i in range(n_quad + 1):
        if i < n_quad:
            k_copies[i].wait()
        if i:
            v_copies[i - 1].wait()
        if i < n_quad:
            scores(i)
        if i:
            outputs(i - 1)
        if i == n_quad // 2:
            pl.semaphore_wait(barrier, n - 1)
            pair_cp.start()
            for g in range(group):
                pltpu.make_async_copy(wo_hbm.at[:, :, g], wo_s.at[:, g], wo_sem.at[0]).start()
            weight_start(wg_hbm, wg_s, exp_sem.at[0])
            weight_start(wu_hbm, wu_s, exp_sem.at[1])
            weight_start(wd_hbm, wd_s, wd_sem.at[0])
    pair_cp.wait_recv()

    lane8 = lax.broadcasted_iota(jnp.int32, (half_b, LANES), 1)
    low8 = lane8 < hd

    def spread(t, gs):
        lane = gs * heads_kv
        return jnp.where(low8, t[:, lane:lane + 1], t[:, lane + 1:lane + 2])

    ma, mb = msg_s[core, m_slot], pair_s[m_slot]
    mm = jnp.maximum(ma, mb)
    ea, eb = jnp.exp(ma - mm), jnp.exp(mb - mm)
    ll = ea * msg_s[core, m_slot + 1] + eb * pair_s[m_slot + 1]
    far = (2, 1, 3, 0)
    for dx in far:
        hp = lax.rem(chip + dx, n_hp)
        shift = lax.rem(LANES - 2 * hp, LANES)
        ra, rb = pltpu.roll(ea, shift, 1), pltpu.roll(eb, shift, 1)
        dst = recv_s.at[chip] if dx == 0 else amsg_s.at[dx]
        for gs in range(gs_n):
            dst[gs] = spread(ra, gs) * msg_s[core, hp * gs_n + gs] + spread(rb, gs) * pair_s[hp * gs_n + gs]
        dst[gs_n] = pltpu.roll(mm, shift, 1)
        dst[gs_n + 1] = pltpu.roll(ll, shift, 1)
    for k, dx in enumerate(far[:-1]):
        cp = remote(amsg_s.at[dx], recv_s.at[chip], a_send.at[k], a_recv.at[chip], lax.rem(chip + dx, n_hp) * 2 + core)
        cp.start()
        sends.append(cp)

    pair_cp.wait_send()
    brow = pl.ds(pl.multiple_of(core * half_b, half_b), half_b)
    m_tail = jnp.full((half_b, LANES), NEG_FILL, F32)
    l_tail = jnp.zeros((half_b, LANES), F32)
    for gs in range(gs_n):
        s = gs % steps
        qt = q_s[chip, gs, brow, :]
        cols = []
        for slot in range(s + 1):
            prod = qt * kt_s[chip, slot, brow, :]
            lo = jnp.sum(jnp.where(low8, prod, 0.0), axis=1, keepdims=True)
            hi = jnp.sum(jnp.where(low8, 0.0, prod), axis=1, keepdims=True)
            cols.append(jnp.where(low8, lo, hi) * (hd ** -0.5))
        mx = functools.reduce(jnp.maximum, cols)
        ws = [jnp.exp(c - mx) for c in cols]
        lsum = functools.reduce(jnp.add, ws)
        acc = functools.reduce(jnp.add, [w.astype(BF16).astype(F32) * vt_s[chip, slot, brow, :] for slot, w in enumerate(ws)])
        recv_s[n_hp, gs] = acc
        for j in range(2):
            sel = lane8 == gs * heads_kv + j
            m_tail = jnp.where(sel, mx[:, j * hd:j * hd + 1], m_tail)
            l_tail = jnp.where(sel, lsum[:, j * hd:j * hd + 1], l_tail)
    recv_s[n_hp, gs_n] = m_tail
    recv_s[n_hp, gs_n + 1] = l_tail

    for src_s, dst, out, i in ((kt_s, tk_s, tk_out, 0), (vt_s, tv_s, tv_out, 1)):
        for hp in range(n_hp):
            t = src_s[hp].reshape(rows, LANES)
            hs_s[:, 2 * hp, :] = t[:, :hd]
            hs_s[:, 2 * hp + 1, :] = pltpu.roll(t, hd, 1)[:, :hd]
        for s in range(steps):
            dst[:, s] = hs_s[s * batch:(s + 1) * batch].astype(BF16)
        pltpu.make_async_copy(dst, out, out_sem.at[i]).start()

    for dx in (1, 3, 2):
        src = lax.rem(chip + dx, n_hp)
        remote(recv_s.at[src], recv_s.at[src], a_send.at[0], a_recv.at[src], me).wait_recv()
    srcs = range(n_hp + 1)
    ms = [recv_s[src, gs_n] for src in srcs]
    mx = functools.reduce(jnp.maximum, ms)
    al = [jnp.exp(m - mx) for m in ms]
    tot = functools.reduce(jnp.add, [a * recv_s[src, gs_n + 1] for src, a in zip(srcs, al)])
    for gs in range(gs_n):
        acc = functools.reduce(jnp.add, [spread(a, gs) * recv_s[src, gs] for src, a in zip(srcs, al)])
        obuf_s[me, gs] = (acc / spread(tot, gs)).astype(BF16).astype(F32)

    order = (1, 3, 2)

    def gather_start(buf, send, recv):
        for i, dx in enumerate((2, 1, 3, 0)):
            dev = partner if dx == 0 else lax.rem(chip + dx, n_hp) * 2 + core
            cp = remote(buf.at[me], buf.at[me], send.at[i], recv.at[me], dev)
            cp.start()
            sends.append(cp)

    def arrived(buf, send, recv, src):
        remote(buf.at[src], buf.at[src], send.at[0], recv.at[src], me).wait_recv()

    def relay(buf, send, recv, i, dx):
        src = lax.rem(chip + dx, n_hp) * 2 + core
        arrived(buf, send, recv, src)
        cp = remote(buf.at[src], buf.at[src], send.at[n_hp + i], recv.at[src], partner)
        cp.start()
        sends.append(cp)

    gather_start(obuf_s, o_send, o_recv)
    weight_wait(wo_s, wo_sem.at[0])
    weight_wait(wg_s, exp_sem.at[0])
    weight_wait(wu_s, exp_sem.at[1])
    weight_wait(wd_s, wd_sem.at[0])

    def wo_part(cx):
        pieces = []
        for g in range(group):
            pieces.append(jnp.concatenate([obuf_s[cx * 2 + half, g * steps + s] for s in range(steps) for half in range(2)], axis=0))
        lhs = jnp.concatenate(pieces, axis=1).astype(BF16)
        return jnp.dot(lhs, wo_s[cx].reshape(group * LANES, dm), preferred_element_type=F32)

    arrived(obuf_s, o_send, o_recv, partner)
    acc = wo_part(chip)
    for i, dx in enumerate(order):
        relay(obuf_s, o_send, o_recv, i, dx)
        if i:
            cx = lax.rem(chip + order[i - 1], n_hp)
            arrived(obuf_s, o_send, o_recv, cx * 2 + other)
            acc = acc + wo_part(cx)
    cx = lax.rem(chip + order[-1], n_hp)
    arrived(obuf_s, o_send, o_recv, cx * 2 + other)
    acc = acc + wo_part(cx)
    x = x_s[...].reshape(rows, dm).astype(F32)
    xm = (x + acc + bo).astype(BF16).astype(F32)
    xm_s[...] = xm.reshape(2, rows // 2, dm)
    h2 = norm_rows(xm, g2, b2)

    logits = lax.dot_general(h2, wr_s[...], NT, preferred_element_type=F32)
    topk = mask_s.shape[1]
    e_iota = lax.broadcasted_iota(jnp.int32, (topk, n_exp), 1)
    grows = []
    for s in range(steps):
        ids = idx_s[s]
        for b in range(batch):
            r = s * batch + b
            lg = jnp.where(mask_s[r] == 1, logits[r:r + 1, :], NEG_FILL)
            ex = jnp.exp(lg - jnp.max(lg, axis=1, keepdims=True))
            pr = ex / jnp.sum(ex, axis=1, keepdims=True)
            grows.append(jnp.sum(jnp.where(ids[:, b:b + 1] == e_iota, pr, 0.0), axis=0, keepdims=True))
    gates = jnp.concatenate(grows, axis=0)
    per = LANES // ff

    def act(c):
        rs = pl.ds(c * LANES, LANES)
        ag = lax.dot_general(h2, wg_s[rs, :], NT, preferred_element_type=F32)
        au = lax.dot_general(h2, wu_s[rs, :], NT, preferred_element_type=F32)
        return ag * (1.0 / (1.0 + jnp.exp(-ag))), au

    peel = n_ec // 4
    for c in range(n_ec):
        gex_s[c] = jnp.where(low_head, gates[:, per * c:per * c + 1], gates[:, per * c + 1:per * c + 2])
    for c in range(peel):
        sg, au = act(c)
        u_s[c] = (gex_s[c] * sg * au).astype(BF16)

    def expert(i, _):
        for j in range(peel):
            c = i * peel + j
            sg, au = act(c)
            u_s[c] = (gex_s[c] * sg * au).astype(BF16)
        return 0

    lax.fori_loop(1, n_ec // peel, expert, 0)
    cw = dm // n_hp
    hr = rows // 2
    u = jnp.concatenate([u_s[c] for c in range(n_ec)], axis=1)

    def add_pair(k, cq, own):
        remote(ppair_s.at[cq], ppair_s.at[cq], d_send.at[0], d_recv.at[cq], me).wait_recv()
        tot = pbuf_s[cq, core] + ppair_s[cq]
        if own:
            return tot
        psum_s[cq] = tot
        cp = remote(psum_s.at[cq], rbuf_s.at[chip], p_send.at[k], p_recv.at[chip], cq * 2 + core)
        cp.start()
        sends.append(cp)

    down = (2, 1, 3, 0)
    for k, dx in enumerate(down):
        cq = lax.rem(chip + dx, n_hp)
        cols = pl.ds(pl.multiple_of(cq * cw, LANES), cw)
        part = jnp.dot(u, wd_s[:, cols], preferred_element_type=F32)
        pbuf_s[cq] = part.astype(BF16).astype(F32).reshape(2, hr, cw)
        cp = remote(pbuf_s.at[cq, other], ppair_s.at[cq], d_send.at[k], d_recv.at[cq], partner)
        cp.start()
        sends.append(cp)
        if k:
            add_pair(k - 1, lax.rem(chip + down[k - 1], n_hp), False)
    y = xm_s[core, :, pl.ds(pl.multiple_of(chip * cw, LANES), cw)] + add_pair(0, chip, True)
    for dx in (1, 3, 2):
        src = lax.rem(chip + dx, n_hp)
        remote(rbuf_s.at[src], rbuf_s.at[src], p_send.at[0], p_recv.at[src], me).wait_recv()
        y = y + rbuf_s[src]
    ybuf_s[me] = y.astype(BF16).astype(F32)
    gather_start(ybuf_s, y_send, y_recv)
    for i, dx in enumerate(order):
        relay(ybuf_s, y_send, y_recv, i, dx)
    for dx in (0,) + order:
        arrived(ybuf_s, y_send, y_recv, lax.rem(chip + dx, n_hp) * 2 + other)
    for cq in range(n_hp):
        blk = jnp.concatenate([ybuf_s[cq * 2], ybuf_s[cq * 2 + 1]], axis=0)
        hid_s[:, :, cq * cw:(cq + 1) * cw] = blk.astype(BF16).reshape(steps, batch, cw)
    hid_cp = pltpu.make_async_copy(hid_s, hid_out, out_sem.at[2])
    hid_cp.start()
    for cp in sends:
        cp.wait_send()
    pltpu.make_async_copy(tk_s, tk_out, out_sem.at[0]).wait()
    pltpu.make_async_copy(tv_s, tv_out, out_sem.at[1]).wait()
    hid_cp.wait()


def emit_kernel(*refs):
    k = len(refs) // 3
    ins, outs, bufs, sem = refs[:k], refs[k:2 * k], refs[2 * k:3 * k], refs[3 * k]
    loads = [pltpu.make_async_copy(ins[i], bufs[i], sem.at[0, i]) for i in range(k)]
    stores = [pltpu.make_async_copy(bufs[i], outs[i], sem.at[1, i]) for i in range(k)]
    for cp in loads:
        cp.start()
    for ld, st in zip(loads, stores):
        ld.wait()
        st.start()
    for cp in stores:
        cp.wait()


def solution(mesh):
    n = mesh.shape['kv']

    def layer_steps(x_first, next_emb, k_cache, v_cache, seq_len, ln1_gain, ln1_bias, w_q, b_q, w_k, b_k, w_v, b_v, w_o, b_o, ln2_gain, ln2_bias, w_router, w_gate, w_up, w_down, long_factor, expert_idx, route_mask):
        batch, shard, heads_kv, hd = k_cache.shape
        dm = x_first.shape[1]
        q_heads = w_q.shape[1] // hd
        group = q_heads // heads_kv
        steps = next_emb.shape[0] + 1
        n_exp, _, ff = w_gate.shape
        topk = expert_idx.shape[-1]
        rows = steps * batch
        hdk = heads_kv * hd
        n_hp = hdk // LANES
        gs_n = group * steps
        qrows = (gs_n + 1) * heads_kv
        fe = n_exp * ff
        dims = (n, steps, batch, heads_kv, hd, group, shard, n_exp, ff, dm)
        args = (
            x_first, next_emb,
            jnp.transpose(k_cache, (0, 2, 3, 1)).reshape(batch, hdk, shard),
            jnp.transpose(v_cache, (0, 2, 3, 1)).reshape(batch, hdk, shard),
            seq_len, ln1_gain, ln1_bias, w_q, b_q, w_k, b_k, w_v, b_v,
            w_o.reshape(n_hp, 2, group, hd, dm), b_o, ln2_gain, ln2_bias,
            jnp.transpose(w_router),
            jnp.transpose(w_gate, (0, 2, 1)).reshape(fe, dm),
            jnp.transpose(w_up, (0, 2, 1)).reshape(fe, dm),
            w_down.reshape(fe, dm), long_factor,
            jnp.transpose(expert_idx, (0, 2, 1)),
            route_mask.reshape(rows, topk, n_exp),
        )
        any_spec = pl.BlockSpec(memory_space=pl.ANY)
        dma = pltpu.SemaphoreType.DMA
        vm = pltpu.VMEM
        outs = (
            jax.ShapeDtypeStruct((steps, batch, dm), BF16),
            jax.ShapeDtypeStruct((batch, steps, heads_kv, hd), BF16),
            jax.ShapeDtypeStruct((batch, steps, heads_kv, hd), BF16),
        )
        blk = vm((n, rows // 2, dm // n_hp), F32)
        qblk = vm((n_hp, rows // 2, dm // n_hp), F32)
        scratch = [
            vm((steps, batch, dm), BF16), pltpu.SMEM((batch,), jnp.int32), pltpu.SMEM((hd // 2,), F32),
            vm((6, dm), F32), vm((hdk,), F32), vm((hdk,), F32), vm((n_exp, dm), BF16),
            vm((steps, topk, batch), jnp.int32), vm((rows, topk, n_exp), jnp.int32),
            vm((n_hp, dm, dm // n_hp), BF16), vm((dm, hdk), BF16), vm((dm, hdk), BF16),
            vm((n_hp, group, 2, hd, dm), BF16), vm((batch, hdk, shard), BF16), vm((batch, hdk, shard), BF16),
            vm((fe, dm), BF16), vm((fe, dm), BF16), vm((fe, dm), BF16),
            vm((n_hp, gs_n, batch, LANES), F32), vm((n_hp, steps, batch, LANES), F32), vm((n_hp, steps, batch, LANES), F32),
            vm((rows, heads_kv, hd), F32), vm((batch, qrows, shard), BF16),
            vm((2, n_hp * gs_n + 2, SUBL, LANES), F32), vm((n_hp * gs_n + 2, SUBL, LANES), F32),
            vm((n_hp, gs_n + 2, SUBL, LANES), F32), vm((n_hp + 1, gs_n + 2, SUBL, LANES), F32),
            vm((n, gs_n, SUBL, LANES), F32), vm((2, rows // 2, dm), F32),
            vm((fe // LANES, rows, LANES), F32), vm((fe // LANES, rows, LANES), BF16),
            vm((n_hp, 2, rows // 2, dm // n_hp), F32), qblk, qblk, qblk, blk,
        ] + [vm(o.shape, o.dtype) for o in outs] + [
            dma((14,)), dma((n_hp,)), dma((2,)), dma((1,)), dma((4,)), dma((4,)), dma((2,)), dma((1,)), dma((3,)),
            dma((2,)), dma((n_hp - 1,)), dma((n_hp,)), dma((n - 1,)), dma((n,)), dma((n_hp,)), dma((n_hp,)), dma((n_hp - 1,)), dma((n_hp,)), dma((n - 1,)), dma((n,)),
        ]
        made = pl.pallas_call(
            functools.partial(layer_kernel, dims),
            out_shape=outs,
            in_specs=[any_spec] * len(args),
            out_specs=(any_spec,) * 3,
            scratch_shapes=scratch,
            compiler_params=pltpu.CompilerParams(collective_id=0, has_side_effects=True, vmem_limit_bytes=64 * 1024 * 1024),
        )(*args)
        return pl.pallas_call(
            emit_kernel,
            out_shape=outs,
            in_specs=[any_spec] * 3,
            out_specs=(any_spec,) * 3,
            scratch_shapes=[vm(o.shape, o.dtype) for o in outs] + [dma((2, 3))],
        )(*made)

    replicated = P()
    in_specs = (P('dp'), P(None, 'dp'), P('dp', 'kv'), P('dp', 'kv'), P('dp')) + (replicated,) * 13 + (P(None, None, 'kv'), P(None, None, 'kv'), P(None, 'kv'), replicated, P(None, 'dp'), P(None, 'dp'))
    out_specs = (P(None, 'dp'), P('dp'), P('dp'))
    return jax.shard_map(layer_steps, mesh=mesh, in_specs=in_specs, out_specs=out_specs, check_vma=False)
```

```python
import functools
import math

import jax
import jax.numpy as jnp
from jax import lax
from jax.experimental import pallas as pl
from jax.experimental.pallas import tpu as pltpu
from jax.sharding import PartitionSpec as P

ROPE_BASE = 10000.0
ROPE_MSCALE = math.sqrt(1.0 + math.log(32.0) / math.log(4096.0))
NORM_EPS = 1e-5
NEG_FILL = -1e30
LANES = 128
SUBL = 8
F32 = jnp.float32
BF16 = jnp.bfloat16
NT = (((1,), (1,)), ((), ()))


def norm_rows(x, gain, bias):
    mean = jnp.mean(x, axis=-1, keepdims=True)
    cent = x - mean
    var = jnp.mean(cent * cent, axis=-1, keepdims=True)
    return (cent * lax.rsqrt(var + NORM_EPS) * gain + bias).astype(BF16)


def layer_kernel(dims, x_first, next_emb, k_hbm, v_hbm, len_hbm, g1_hbm, b1_hbm, wq_hbm, bq_hbm, wk_hbm, bk_hbm, wv_hbm, bv_hbm, wo_hbm, bo_hbm, g2_hbm, b2_hbm, wr_hbm, wg_hbm, wu_hbm, wd_hbm, lf_hbm, idx_hbm, mask_hbm,
                 hid_out, tk_out, tv_out,
                 x_s, len_s, lf_s, vec_s, bk_s, bv_s, wr_s, idx_s, mask_s,
                 wq_s, wk_s, wv_s, wo_s, k_s, v_s, wg_s, wu_s, wd_s,
                 q_s, kt_s, vt_s, hs_s, p_s, msg_s, pair_s, tail_s, recv_s, of_s, xm_s, gex_s, u_s, pbuf_s, ppair_s, psum_s, rbuf_s, ybuf_s,
                 hid_s, tk_s, tv_s,
                 small_sem, wq_sem, wkv_sem, wo_sem, k_sem, v_sem, exp_sem, wd_sem, out_sem,
                 pair_send, pair_recv, g_send, g_recv, d_send, d_recv, p_send, p_recv, y_send, y_recv):
    n, steps, batch, heads_kv, hd, group, shard, n_exp, ff, dm = dims
    rows = steps * batch
    gs_n = group * steps
    qrows = (gs_n + 1) * heads_kv
    hdk = heads_kv * hd
    n_hp = hdk // LANES
    me = lax.axis_index('kv')
    chip = me // 2
    core = lax.rem(me, 2)
    other = 1 - core
    partner = chip * 2 + other
    mesh_id = pl.DeviceIdType.MESH

    def remote(src, dst, send, recv, dev):
        return pltpu.make_async_remote_copy(src_ref=src, dst_ref=dst, send_sem=send, recv_sem=recv, device_id={'kv': dev}, device_id_type=mesh_id)

    vecs = (g1_hbm, b1_hbm, bq_hbm, bo_hbm, g2_hbm, b2_hbm)
    smalls = [(x_first, x_s.at[0], 0), (next_emb, x_s.at[pl.ds(1, steps - 1)], 0)]
    smalls += [(len_hbm, len_s, 1), (lf_hbm, lf_s, 2), (bk_hbm, bk_s, 3), (bv_hbm, bv_s, 4), (wr_hbm, wr_s, 5), (idx_hbm, idx_s, 6), (mask_hbm, mask_s, 7)]
    smalls += [(src, vec_s.at[i], 8 + i) for i, src in enumerate(vecs)]
    small_copies = [pltpu.make_async_copy(src, dst, small_sem.at[i]) for src, dst, i in smalls]
    small_waits = [pltpu.make_async_copy(x_s, x_s, small_sem.at[0])] + small_copies[2:]
    qw = wq_s.shape[2]
    wq_copies = [pltpu.make_async_copy(wq_hbm.at[:, pl.ds(i * qw, qw)], wq_s.at[i], wq_sem.at[i]) for i in range(n_hp)]
    wkv_copies = [pltpu.make_async_copy(wk_hbm, wk_s, wkv_sem.at[0]), pltpu.make_async_copy(wv_hbm, wv_s, wkv_sem.at[1])]
    for cp in small_copies + wq_copies + wkv_copies:
        cp.start()

    barrier = pltpu.get_barrier_semaphore()
    for d in range(1, n):
        pl.semaphore_signal(barrier, inc=1, device_id={'kv': lax.rem(me + d, n)}, device_id_type=mesh_id)

    quad = SUBL // 2
    n_quad = batch // quad

    def cache_copy(src, dst, sem, i):
        sl = pl.ds(i * quad, quad)
        return pltpu.make_async_copy(src.at[sl], dst.at[sl], sem.at[i])

    k_copies = [cache_copy(k_hbm, k_s, k_sem, i) for i in range(n_quad)]
    v_copies = [cache_copy(v_hbm, v_s, v_sem, i) for i in range(n_quad)]
    n_ec = wg_s.shape[0] // LANES

    def weight_start(src, dst, sem, parts=4):
        ec = src.shape[0] // parts
        for i in range(parts):
            pltpu.make_async_copy(src.at[pl.ds(i * ec, ec)], dst.at[pl.ds(i * ec, ec)], sem).start()

    def weight_wait(dst, sem):
        pltpu.make_async_copy(dst, dst, sem).wait()

    for cp in small_waits:
        cp.wait()

    g1, b1, bq, bo, g2, b2 = [vec_s[i].reshape(1, dm) for i in range(6)]
    x = x_s[...].reshape(rows, dm).astype(F32)
    h = norm_rows(x, g1, b1)

    lane1 = lax.broadcasted_iota(jnp.int32, (1, LANES), 1)
    half_dim = hd // 2
    jlane = lax.rem(lane1, half_dim)
    lfv = jnp.zeros((1, LANES), F32)
    for j in range(half_dim):
        lfv = jnp.where(jlane == j, lf_s[j], lfv)
    inv = 1.0 / (lfv * jnp.exp(jlane.astype(F32) * (2.0 * math.log(ROPE_BASE) / hd)))
    subb = lax.broadcasted_iota(jnp.int32, (batch, LANES), 0)
    pos = jnp.zeros((batch, LANES), jnp.int32)
    for b in range(batch):
        pos = jnp.where(subb == b, len_s[b], pos)
    ang = jnp.concatenate([(pos + s).astype(F32) * inv for s in range(steps)], axis=0)
    cos = jnp.cos(ang) * ROPE_MSCALE
    sin = jnp.sin(ang) * ROPE_MSCALE
    lane_r = lax.broadcasted_iota(jnp.int32, (rows, LANES), 1)
    sin = jnp.where(lax.rem(lane_r, hd) < half_dim, -sin, sin)
    low_half = lax.rem(lane_r, hd) < half_dim
    low_head = lane_r < hd

    def rope(t):
        t = t.astype(BF16).astype(F32)
        rot = jnp.where(low_half, pltpu.roll(t, LANES - half_dim, 1), pltpu.roll(t, half_dim, 1))
        return (t * cos + rot * sin).astype(BF16).astype(F32)

    def q_block(hp):
        t = jnp.dot(h, wq_s[hp], preferred_element_type=F32) + bq[:, hp * qw:(hp + 1) * qw]
        parts = [rope(t[:, c * LANES:(c + 1) * LANES]) for c in range(qw // LANES)]
        for g in range(group):
            first, second = g, group + g
            a, a_hi = parts[first // 2], first % 2
            c, c_hi = parts[second // 2], second % 2
            a = pltpu.roll(a, hd, 1) if a_hi else a
            c = c if c_hi else pltpu.roll(c, hd, 1)
            q_s[hp, g * steps:(g + 1) * steps] = jnp.where(low_head, a, c).reshape(steps, batch, LANES)

    wq_copies[0].wait()
    for cp in (k_copies[0], k_copies[1], v_copies[0], k_copies[2]):
        cp.start()
    wq_copies[1].wait()
    for hp in range(2):
        q_block(hp)
    for cp in wq_copies[2:] + wkv_copies:
        cp.wait()
    for cp in (v_copies[1], k_copies[3], v_copies[2], v_copies[3]):
        cp.start()
    for hp in range(2, n_hp):
        q_block(hp)
    t = jnp.dot(h, wk_s[...], preferred_element_type=F32) + bk_s[...].reshape(1, hdk)
    for hp in range(n_hp):
        kt_s[hp] = rope(t[:, hp * LANES:(hp + 1) * LANES]).reshape(steps, batch, LANES)
    t = (jnp.dot(h, wv_s[...], preferred_element_type=F32) + bv_s[...].reshape(1, hdk)).astype(BF16).astype(F32)
    for hp in range(n_hp):
        vt_s[hp] = t[:, hp * LANES:(hp + 1) * LANES].reshape(steps, batch, LANES)

    tpos = me * shard + lax.broadcasted_iota(jnp.int32, (1, shard), 1)
    diag = lax.broadcasted_iota(jnp.int32, (heads_kv, hdk), 0) == lax.broadcasted_iota(jnp.int32, (heads_kv, hdk), 1) // hd
    ident = lax.broadcasted_iota(jnp.int32, (qrows, LANES), 0) == lax.broadcasted_iota(jnp.int32, (qrows, LANES), 1)
    o_rows = gs_n * quad
    last = o_rows // SUBL * SUBL
    n_tile = last // SUBL + 1
    lane8 = lax.broadcasted_iota(jnp.int32, (SUBL, LANES), 1)
    sub8 = lax.broadcasted_iota(jnp.int32, (SUBL, LANES), 0)
    low8 = lane8 < hd
    low4 = sub8 < quad

    tail_hp = 2 * core + lax.rem(chip, 2)
    tail_q = chip // 2 * 2
    brow = pl.ds(pl.multiple_of(tail_q * quad, SUBL), SUBL)
    for q in range(n_quad):
        tail_s[q, :o_rows] = jnp.zeros((o_rows, LANES), F32)
        tail_s[q, o_rows:o_rows + quad] = jnp.full((quad, LANES), NEG_FILL, F32)
        tail_s[q, o_rows + quad:] = jnp.zeros((SUBL, LANES), F32)
    m_tail = jnp.full((SUBL, LANES), NEG_FILL, F32)
    l_tail = jnp.zeros((SUBL, LANES), F32)
    for gs in range(gs_n):
        s = gs % steps
        qt = q_s[tail_hp, gs, brow, :]
        cols = []
        for slot in range(s + 1):
            prod = qt * kt_s[tail_hp, slot, brow, :]
            lo = jnp.sum(jnp.where(low8, prod, 0.0), axis=1, keepdims=True)
            hi = jnp.sum(jnp.where(low8, 0.0, prod), axis=1, keepdims=True)
            cols.append(jnp.where(low8, lo, hi) * (hd ** -0.5))
        mx = functools.reduce(jnp.maximum, cols)
        ws = [jnp.exp(c - mx) for c in cols]
        lsum = functools.reduce(jnp.add, ws)
        acc = functools.reduce(jnp.add, [w.astype(BF16).astype(F32) * vt_s[tail_hp, slot, brow, :] for slot, w in enumerate(ws)])
        for i in range(2):
            tail_s[tail_q + i, gs * quad:(gs + 1) * quad] = acc[i * quad:(i + 1) * quad]
        for j in range(2):
            sel = lane8 == gs * heads_kv + j
            m_tail = jnp.where(sel, mx[:, j * hd:j * hd + 1], m_tail)
            l_tail = jnp.where(sel, lsum[:, j * hd:j * hd + 1], l_tail)
    m_tail = pltpu.roll(m_tail, 2 * tail_hp, 1)
    l_tail = pltpu.roll(l_tail, 2 * tail_hp, 1)
    for i in range(2):
        tail_s[tail_q + i, o_rows:o_rows + quad] = m_tail[i * quad:(i + 1) * quad]
        tail_s[tail_q + i, o_rows + SUBL:] = l_tail[i * quad:(i + 1) * quad]

    def to_row(col):
        return jnp.sum(jnp.where(ident, col, 0.0), axis=0, keepdims=True)

    def scores(i):
        for j in range(quad):
            b = i * quad + j
            blocks = []
            for gs in range(gs_n):
                qrow = jnp.concatenate([q_s[hp, gs, b:b + 1, :] for hp in range(n_hp)], axis=1)
                blocks.append(jnp.where(diag, qrow, 0.0))
            blocks.append(jnp.zeros((heads_kv, hdk), F32))
            qbd = jnp.concatenate(blocks, axis=0).astype(BF16)
            keep = tpos < len_s[b]
            sc = jnp.dot(qbd, k_s[b], preferred_element_type=F32) * (hd ** -0.5)
            sc = jnp.where(keep, sc, NEG_FILL)
            m = jnp.max(sc, axis=1, keepdims=True)
            w = jnp.where(keep, jnp.exp(sc - m), 0.0)
            p_s[b] = w.astype(BF16)
            mrow, lrow = to_row(m), to_row(jnp.sum(w, axis=1, keepdims=True))
            for hp in range(n_hp):
                msg_s[i, hp, o_rows + j:o_rows + j + 1, :] = lrow if hp % 2 else mrow

    def outputs(i):
        for j in range(quad):
            b = i * quad + j
            o = lax.dot_general(p_s[b], v_s[b], NT, preferred_element_type=F32)
            for gs in range(gs_n):
                row = jnp.sum(jnp.where(diag, o[gs * heads_kv:(gs + 1) * heads_kv], 0.0), axis=0, keepdims=True)
                for hp in range(n_hp):
                    msg_s[i, hp, gs * quad + j:gs * quad + j + 1, :] = row[:, hp * LANES:(hp + 1) * LANES]

    def spread(t, lane):
        return jnp.where(low8, t[:, lane:lane + 1], t[:, lane + 1:lane + 2])

    def both_halves(t):
        return jnp.where(low4, pltpu.roll(t, quad, 0), pltpu.roll(t, LANES - heads_kv, 1))

    sends = []
    tiles = [pl.ds(t * SUBL, SUBL) for t in range(n_tile)]

    def pair_start(q):
        cp = remote(msg_s.at[q, pl.ds(2 * other, 2)], pair_s.at[q], pair_send.at[q], pair_recv.at[q], partner)
        cp.start()
        sends.append(cp)

    def pair_merge(q):
        remote(pair_s.at[q], pair_s.at[q], pair_send.at[q], pair_recv.at[q], partner).wait_recv()
        own = [msg_s.at[q, 2 * core + k] for k in range(2)]
        ms = [own[0][tiles[-1]], pair_s[q, 0, tiles[-1]], tail_s[q, tiles[-1]]]
        ls = [own[1][tiles[-1]], pair_s[q, 1, tiles[-1]], tail_s[q, pl.ds(last + SUBL, SUBL)]]
        mm = functools.reduce(jnp.maximum, ms)
        es = [jnp.exp(m - mm) for m in ms]
        ll = functools.reduce(jnp.add, [e * l for e, l in zip(es, ls)])
        es = [both_halves(e) for e in es]
        dst = recv_s.at[q, chip, core]
        for k in range(2):
            shift = lax.rem(LANES - 2 * (2 * core + k), LANES)
            ra, rb = pltpu.roll(es[0], shift, 1), pltpu.roll(es[1], shift, 1)
            for t in range(n_tile):
                lane = t * 2 * heads_kv
                dst[k, tiles[t]] = spread(ra, lane) * own[k][tiles[t]] + spread(rb, lane) * pair_s[q, k, tiles[t]]
        rt = pltpu.roll(es[2], lax.rem(LANES - 2 * tail_hp, LANES), 1)
        kt = lax.rem(chip, 2)
        for t in range(n_tile):
            dst[kt, tiles[t]] = dst[kt, tiles[t]] + spread(rt, t * 2 * heads_kv) * tail_s[q, tiles[t]]
        dst[0, o_rows:] = mm[quad:]
        dst[1, o_rows:] = ll[quad:]
        for dx in (2, 1, 3):
            remote(dst, dst, g_send.at[0], g_recv.at[q, chip, core], lax.rem(chip + dx, n_hp) * 2 + core).start()
        remote(dst, dst, g_send.at[1], g_recv.at[q, chip, core], partner).start()

    def part_arrived(q, cx, c):
        blk = recv_s.at[q, cx, c]
        remote(blk, blk, g_send.at[0], g_recv.at[q, cx, c], me).wait_recv()
        return blk

    def part_relay(q):
        for dx in (1, 3, 2):
            cx = lax.rem(chip + dx, n_hp)
            blk = part_arrived(q, cx, core)
            remote(blk, blk, g_send.at[1], g_recv.at[q, cx, core], partner).start()

    def final_merge(q):
        for dx in (0, 1, 3, 2):
            part_arrived(q, lax.rem(chip + dx, n_hp), other)
        for c in range(2):
            ms = [recv_s[q, cx, c, 0, tiles[-1]] for cx in range(n_hp)]
            mm = functools.reduce(jnp.maximum, ms)
            es = [jnp.exp(m - mm) for m in ms]
            inv_l = 1.0 / functools.reduce(jnp.add, [e * recv_s[q, cx, c, 1, tiles[-1]] for cx, e in enumerate(es)])
            es = [both_halves(e * inv_l) for e in es]
            for k in range(2):
                hp = 2 * c + k
                for t in range(n_tile):
                    lane = t * 2 * heads_kv + 2 * hp
                    o = functools.reduce(jnp.add, [spread(e, lane) * recv_s[q, cx, c, k, tiles[t]] for cx, e in enumerate(es)])
                    for i in range(2):
                        gs = 2 * t + i
                        if gs < gs_n:
                            r = gs % steps * batch + q * quad
                            of_s[gs // steps, r:r + quad, hp * LANES:(hp + 1) * LANES] = o[i * quad:(i + 1) * quad]

    for i in range(n_quad + 1):
        if i < n_quad:
            k_copies[i].wait()
        if i:
            v_copies[i - 1].wait()
        if i < n_quad:
            scores(i)
        if i:
            outputs(i - 1)
            if i == 1:
                pl.semaphore_wait(barrier, n - 1)
            pair_start(i - 1)
        if i == n_quad // 2:
            for g in range(group):
                pltpu.make_async_copy(wo_hbm.at[:, :, g], wo_s.at[:, g], wo_sem.at[0]).start()
            weight_start(wg_hbm, wg_s, exp_sem.at[0])
            weight_start(wu_hbm, wu_s, exp_sem.at[1])
            weight_start(wd_hbm, wd_s, wd_sem.at[0])
        if i > 1:
            pair_merge(i - 2)
    pair_merge(n_quad - 1)

    for src_s, dst, out, i in ((kt_s, tk_s, tk_out, 0), (vt_s, tv_s, tv_out, 1)):
        for hp in range(n_hp):
            t = src_s[hp].reshape(rows, LANES)
            hs_s[:, 2 * hp, :] = t[:, :hd]
            hs_s[:, 2 * hp + 1, :] = pltpu.roll(t, hd, 1)[:, :hd]
        for s in range(steps):
            dst[:, s] = hs_s[s * batch:(s + 1) * batch].astype(BF16)
        pltpu.make_async_copy(dst, out, out_sem.at[i]).start()

    part_relay(0)
    for q in range(n_quad):
        if q + 1 < n_quad:
            part_relay(q + 1)
        else:
            weight_wait(wo_s, wo_sem.at[0])
            weight_wait(wg_s, exp_sem.at[0])
            weight_wait(wu_s, exp_sem.at[1])
            weight_wait(wd_s, wd_sem.at[0])
        final_merge(q)

    order = (1, 3, 2)

    def gather_start(buf, send, recv):
        for i, dx in enumerate((2, 1, 3, 0)):
            dev = partner if dx == 0 else lax.rem(chip + dx, n_hp) * 2 + core
            cp = remote(buf.at[me], buf.at[me], send.at[i], recv.at[me], dev)
            cp.start()
            sends.append(cp)

    def arrived(buf, send, recv, src):
        remote(buf.at[src], buf.at[src], send.at[0], recv.at[src], me).wait_recv()

    def relay(buf, send, recv, i, dx):
        src = lax.rem(chip + dx, n_hp) * 2 + core
        arrived(buf, send, recv, src)
        cp = remote(buf.at[src], buf.at[src], send.at[n_hp + i], recv.at[src], partner)
        cp.start()
        sends.append(cp)

    lhs = jnp.concatenate([of_s[g, :, hp * LANES:(hp + 1) * LANES] for hp in range(n_hp) for g in range(group)], axis=1).astype(BF16)
    acc = jnp.dot(lhs, wo_s[...].reshape(dm, dm), preferred_element_type=F32)
    x = x_s[...].reshape(rows, dm).astype(F32)
    xm = (x + acc + bo).astype(BF16).astype(F32)
    xm_s[...] = xm.reshape(2, rows // 2, dm)
    h2 = norm_rows(xm, g2, b2)

    logits = lax.dot_general(h2, wr_s[...], NT, preferred_element_type=F32)
    topk = mask_s.shape[1]
    e_iota = lax.broadcasted_iota(jnp.int32, (topk, n_exp), 1)
    grows = []
    for s in range(steps):
        ids = idx_s[s]
        for b in range(batch):
            r = s * batch + b
            lg = jnp.where(mask_s[r] == 1, logits[r:r + 1, :], NEG_FILL)
            ex = jnp.exp(lg - jnp.max(lg, axis=1, keepdims=True))
            pr = ex / jnp.sum(ex, axis=1, keepdims=True)
            grows.append(jnp.sum(jnp.where(ids[:, b:b + 1] == e_iota, pr, 0.0), axis=0, keepdims=True))
    gates = jnp.concatenate(grows, axis=0)
    per = LANES // ff

    def act(c):
        rs = pl.ds(c * LANES, LANES)
        ag = lax.dot_general(h2, wg_s[rs, :], NT, preferred_element_type=F32)
        au = lax.dot_general(h2, wu_s[rs, :], NT, preferred_element_type=F32)
        return ag * (1.0 / (1.0 + jnp.exp(-ag))), au

    peel = n_ec // 4
    for c in range(n_ec):
        gex_s[c] = jnp.where(low_head, gates[:, per * c:per * c + 1], gates[:, per * c + 1:per * c + 2])
    for c in range(peel):
        sg, au = act(c)
        u_s[c] = (gex_s[c] * sg * au).astype(BF16)

    def expert(i, _):
        for j in range(peel):
            c = i * peel + j
            sg, au = act(c)
            u_s[c] = (gex_s[c] * sg * au).astype(BF16)
        return 0

    lax.fori_loop(1, n_ec // peel, expert, 0)
    cw = dm // n_hp
    hr = rows // 2
    u = jnp.concatenate([u_s[c] for c in range(n_ec)], axis=1)

    def add_pair(k, cq, own):
        remote(ppair_s.at[cq], ppair_s.at[cq], d_send.at[0], d_recv.at[cq], me).wait_recv()
        tot = pbuf_s[cq, core] + ppair_s[cq]
        if own:
            return tot
        psum_s[cq] = tot
        cp = remote(psum_s.at[cq], rbuf_s.at[chip], p_send.at[k], p_recv.at[chip], cq * 2 + core)
        cp.start()
        sends.append(cp)

    down = (2, 1, 3, 0)
    for k, dx in enumerate(down):
        cq = lax.rem(chip + dx, n_hp)
        cols = pl.ds(pl.multiple_of(cq * cw, LANES), cw)
        part = jnp.dot(u, wd_s[:, cols], preferred_element_type=F32)
        pbuf_s[cq] = part.astype(BF16).astype(F32).reshape(2, hr, cw)
        cp = remote(pbuf_s.at[cq, other], ppair_s.at[cq], d_send.at[k], d_recv.at[cq], partner)
        cp.start()
        sends.append(cp)
        if k:
            add_pair(k - 1, lax.rem(chip + down[k - 1], n_hp), False)
    y = xm_s[core, :, pl.ds(pl.multiple_of(chip * cw, LANES), cw)] + add_pair(0, chip, True)
    for dx in (1, 3, 2):
        src = lax.rem(chip + dx, n_hp)
        remote(rbuf_s.at[src], rbuf_s.at[src], p_send.at[0], p_recv.at[src], me).wait_recv()
        y = y + rbuf_s[src]
    ybuf_s[me] = y.astype(BF16).astype(F32)
    gather_start(ybuf_s, y_send, y_recv)
    for i, dx in enumerate(order):
        relay(ybuf_s, y_send, y_recv, i, dx)
    for dx in (0,) + order:
        arrived(ybuf_s, y_send, y_recv, lax.rem(chip + dx, n_hp) * 2 + other)
    for cq in range(n_hp):
        blk = jnp.concatenate([ybuf_s[cq * 2], ybuf_s[cq * 2 + 1]], axis=0)
        hid_s[:, :, cq * cw:(cq + 1) * cw] = blk.astype(BF16).reshape(steps, batch, cw)
    hid_cp = pltpu.make_async_copy(hid_s, hid_out, out_sem.at[2])
    hid_cp.start()
    for cp in sends:
        cp.wait_send()
    for i, blks in enumerate((recv_s.at[pl.ds(0, n_quad - 1), :, pl.ds(0, 1)], recv_s.at[:, :, pl.ds(0, 1)])):
        pltpu.make_async_copy(blks, blks, g_send.at[i]).wait()
    pltpu.make_async_copy(tk_s, tk_out, out_sem.at[0]).wait()
    pltpu.make_async_copy(tv_s, tv_out, out_sem.at[1]).wait()
    hid_cp.wait()


def emit_kernel(*refs):
    k = len(refs) // 3
    ins, outs, bufs, sem = refs[:k], refs[k:2 * k], refs[2 * k:3 * k], refs[3 * k]
    loads = [pltpu.make_async_copy(ins[i], bufs[i], sem.at[0, i]) for i in range(k)]
    stores = [pltpu.make_async_copy(bufs[i], outs[i], sem.at[1, i]) for i in range(k)]
    for cp in loads:
        cp.start()
    for ld, st in zip(loads, stores):
        ld.wait()
        st.start()
    for cp in stores:
        cp.wait()


def solution(mesh):
    n = mesh.shape['kv']

    def layer_steps(x_first, next_emb, k_cache, v_cache, seq_len, ln1_gain, ln1_bias, w_q, b_q, w_k, b_k, w_v, b_v, w_o, b_o, ln2_gain, ln2_bias, w_router, w_gate, w_up, w_down, long_factor, expert_idx, route_mask):
        batch, shard, heads_kv, hd = k_cache.shape
        dm = x_first.shape[1]
        q_heads = w_q.shape[1] // hd
        group = q_heads // heads_kv
        steps = next_emb.shape[0] + 1
        n_exp, _, ff = w_gate.shape
        topk = expert_idx.shape[-1]
        rows = steps * batch
        hdk = heads_kv * hd
        n_hp = hdk // LANES
        gs_n = group * steps
        qrows = (gs_n + 1) * heads_kv
        fe = n_exp * ff
        dims = (n, steps, batch, heads_kv, hd, group, shard, n_exp, ff, dm)
        args = (
            x_first, next_emb,
            jnp.transpose(k_cache, (0, 2, 3, 1)).reshape(batch, hdk, shard),
            jnp.transpose(v_cache, (0, 2, 3, 1)).reshape(batch, hdk, shard),
            seq_len, ln1_gain, ln1_bias, w_q, b_q, w_k, b_k, w_v, b_v,
            w_o.reshape(n_hp, 2, group, hd, dm), b_o, ln2_gain, ln2_bias,
            jnp.transpose(w_router),
            jnp.transpose(w_gate, (0, 2, 1)).reshape(fe, dm),
            jnp.transpose(w_up, (0, 2, 1)).reshape(fe, dm),
            w_down.reshape(fe, dm), long_factor,
            jnp.transpose(expert_idx, (0, 2, 1)),
            route_mask.reshape(rows, topk, n_exp),
        )
        any_spec = pl.BlockSpec(memory_space=pl.ANY)
        dma = pltpu.SemaphoreType.DMA
        vm = pltpu.VMEM
        outs = (
            jax.ShapeDtypeStruct((steps, batch, dm), BF16),
            jax.ShapeDtypeStruct((batch, steps, heads_kv, hd), BF16),
            jax.ShapeDtypeStruct((batch, steps, heads_kv, hd), BF16),
        )
        n_quad = batch // (SUBL // 2)
        m_rows = (gs_n + 1) * (SUBL // 2)
        blk = vm((n, rows // 2, dm // n_hp), F32)
        qblk = vm((n_hp, rows // 2, dm // n_hp), F32)
        scratch = [
            vm((steps, batch, dm), BF16), pltpu.SMEM((batch,), jnp.int32), pltpu.SMEM((hd // 2,), F32),
            vm((6, dm), F32), vm((hdk,), F32), vm((hdk,), F32), vm((n_exp, dm), BF16),
            vm((steps, topk, batch), jnp.int32), vm((rows, topk, n_exp), jnp.int32),
            vm((n_hp, dm, dm // n_hp), BF16), vm((dm, hdk), BF16), vm((dm, hdk), BF16),
            vm((n_hp, group, 2, hd, dm), BF16), vm((batch, hdk, shard), BF16), vm((batch, hdk, shard), BF16),
            vm((fe, dm), BF16), vm((fe, dm), BF16), vm((fe, dm), BF16),
            vm((n_hp, gs_n, batch, LANES), F32), vm((n_hp, steps, batch, LANES), F32), vm((n_hp, steps, batch, LANES), F32),
            vm((rows, heads_kv, hd), F32), vm((batch, qrows, shard), BF16),
            vm((n_quad, n_hp, m_rows, LANES), F32), vm((n_quad, 2, m_rows, LANES), F32), vm((n_quad, m_rows + SUBL, LANES), F32),
            vm((n_quad, n_hp, 2, 2, m_rows, LANES), F32), vm((group, rows, hdk), F32), vm((2, rows // 2, dm), F32),
            vm((fe // LANES, rows, LANES), F32), vm((fe // LANES, rows, LANES), BF16),
            vm((n_hp, 2, rows // 2, dm // n_hp), F32), qblk, qblk, qblk, blk,
        ] + [vm(o.shape, o.dtype) for o in outs] + [
            dma((14,)), dma((n_hp,)), dma((2,)), dma((1,)), dma((4,)), dma((4,)), dma((2,)), dma((1,)), dma((3,)),
            dma((n_quad,)), dma((n_quad,)), dma((2,)), dma((n_quad, n_hp, 2)), dma((n_hp,)), dma((n_hp,)), dma((n_hp - 1,)), dma((n_hp,)), dma((n - 1,)), dma((n,)),
        ]
        made = pl.pallas_call(
            functools.partial(layer_kernel, dims),
            out_shape=outs,
            in_specs=[any_spec] * len(args),
            out_specs=(any_spec,) * 3,
            scratch_shapes=scratch,
            compiler_params=pltpu.CompilerParams(collective_id=0, has_side_effects=True, vmem_limit_bytes=64 * 1024 * 1024),
        )(*args)
        return pl.pallas_call(
            emit_kernel,
            out_shape=outs,
            in_specs=[any_spec] * 3,
            out_specs=(any_spec,) * 3,
            scratch_shapes=[vm(o.shape, o.dtype) for o in outs] + [dma((2, 3))],
        )(*made)

    replicated = P()
    in_specs = (P('dp'), P(None, 'dp'), P('dp', 'kv'), P('dp', 'kv'), P('dp')) + (replicated,) * 13 + (P(None, None, 'kv'), P(None, None, 'kv'), P(None, 'kv'), replicated, P(None, 'dp'), P(None, 'dp'))
    out_specs = (P(None, 'dp'), P('dp'), P('dp'))
    return jax.shard_map(layer_steps, mesh=mesh, in_specs=in_specs, out_specs=out_specs, check_vma=False)
```

```python
import functools
import math

import jax
import jax.numpy as jnp
from jax import lax
from jax.experimental import pallas as pl
from jax.experimental.pallas import tpu as pltpu
from jax.sharding import PartitionSpec as P

ROPE_BASE = 10000.0
ROPE_MSCALE = math.sqrt(1.0 + math.log(32.0) / math.log(4096.0))
NORM_EPS = 1e-5
NEG_FILL = -1e30
LANES = 128
SUBL = 8
F32 = jnp.float32
BF16 = jnp.bfloat16
NT = (((1,), (1,)), ((), ()))


def norm_rows(x, gain, bias):
    mean = jnp.mean(x, axis=-1, keepdims=True)
    cent = x - mean
    var = jnp.mean(cent * cent, axis=-1, keepdims=True)
    return (cent * lax.rsqrt(var + NORM_EPS) * gain + bias).astype(BF16)


def layer_kernel(dims, x_first, next_emb, k_hbm, v_hbm, len_hbm, g1_hbm, b1_hbm, wq_hbm, bq_hbm, wk_hbm, bk_hbm, wv_hbm, bv_hbm, wo_hbm, bo_hbm, g2_hbm, b2_hbm, wr_hbm, wg_hbm, wu_hbm, wd_hbm, lf_hbm, idx_hbm, mask_hbm,
                 hid_out, tk_out, tv_out,
                 x_s, len_s, lf_s, vec_s, bk_s, bv_s, wr_s, idx_s, mask_s,
                 wq_s, wk_s, wv_s, wo_s, k_s, v_s, wg_s, wu_s, wd_s,
                 q_s, kt_s, vt_s, hs_s, p_s, msg_s, pair_s, ml_s, mlp_s, cf_s, tail_s, recv_s, of_s, xm_s, gex_s, u_s, pbuf_s, ppair_s, psum_s, rbuf_s, ybuf_s,
                 hid_s, tk_s, tv_s,
                 small_sem, wq_sem, wkv_sem, wo_sem, k_sem, v_sem, exp_sem, wd_sem, out_sem,
                 ml_send, ml_recv, pair_send, pair_recv, g_send, g_recv, d_send, d_recv, p_send, p_recv, y_send, y_recv):
    n, steps, batch, heads_kv, hd, group, shard, n_exp, ff, dm = dims
    rows = steps * batch
    gs_n = group * steps
    qrows = (gs_n + 1) * heads_kv
    hdk = heads_kv * hd
    n_hp = hdk // LANES
    me = lax.axis_index('kv')
    chip = me // 2
    core = lax.rem(me, 2)
    other = 1 - core
    partner = chip * 2 + other
    mesh_id = pl.DeviceIdType.MESH

    def remote(src, dst, send, recv, dev):
        return pltpu.make_async_remote_copy(src_ref=src, dst_ref=dst, send_sem=send, recv_sem=recv, device_id={'kv': dev}, device_id_type=mesh_id)

    vecs = (g1_hbm, b1_hbm, bq_hbm, bo_hbm, g2_hbm, b2_hbm)
    smalls = [(x_first, x_s.at[0], 0), (next_emb, x_s.at[pl.ds(1, steps - 1)], 0)]
    smalls += [(len_hbm, len_s, 1), (lf_hbm, lf_s, 2), (bk_hbm, bk_s, 3), (bv_hbm, bv_s, 4), (wr_hbm, wr_s, 5), (idx_hbm, idx_s, 6), (mask_hbm, mask_s, 7)]
    smalls += [(src, vec_s.at[i], 8 + i) for i, src in enumerate(vecs)]
    small_copies = [pltpu.make_async_copy(src, dst, small_sem.at[i]) for src, dst, i in smalls]
    small_waits = [pltpu.make_async_copy(x_s, x_s, small_sem.at[0])] + small_copies[2:]
    qw = wq_s.shape[2]
    wq_copies = [pltpu.make_async_copy(wq_hbm.at[:, pl.ds(i * qw, qw)], wq_s.at[i], wq_sem.at[i]) for i in range(n_hp)]
    wkv_copies = [pltpu.make_async_copy(wk_hbm, wk_s, wkv_sem.at[0]), pltpu.make_async_copy(wv_hbm, wv_s, wkv_sem.at[1])]
    for cp in small_copies + wq_copies + wkv_copies:
        cp.start()

    barrier = pltpu.get_barrier_semaphore()
    for d in range(1, n):
        pl.semaphore_signal(barrier, inc=1, device_id={'kv': lax.rem(me + d, n)}, device_id_type=mesh_id)

    quad = SUBL // 2
    n_quad = batch // quad

    def cache_copy(src, dst, sem, i):
        sl = pl.ds(i * quad, quad)
        return pltpu.make_async_copy(src.at[sl], dst.at[sl], sem.at[i])

    k_copies = [cache_copy(k_hbm, k_s, k_sem, i) for i in range(n_quad)]
    v_copies = [cache_copy(v_hbm, v_s, v_sem, i) for i in range(n_quad)]
    n_ec = wg_s.shape[0] // LANES

    def weight_start(src, dst, sem, parts=4):
        ec = src.shape[0] // parts
        for i in range(parts):
            pltpu.make_async_copy(src.at[pl.ds(i * ec, ec)], dst.at[pl.ds(i * ec, ec)], sem).start()

    def weight_wait(dst, sem):
        pltpu.make_async_copy(dst, dst, sem).wait()

    for cp in small_waits:
        cp.wait()

    g1, b1, bq, bo, g2, b2 = [vec_s[i].reshape(1, dm) for i in range(6)]
    x = x_s[...].reshape(rows, dm).astype(F32)
    h = norm_rows(x, g1, b1)

    lane1 = lax.broadcasted_iota(jnp.int32, (1, LANES), 1)
    half_dim = hd // 2
    jlane = lax.rem(lane1, half_dim)
    lfv = jnp.zeros((1, LANES), F32)
    for j in range(half_dim):
        lfv = jnp.where(jlane == j, lf_s[j], lfv)
    inv = 1.0 / (lfv * jnp.exp(jlane.astype(F32) * (2.0 * math.log(ROPE_BASE) / hd)))
    subb = lax.broadcasted_iota(jnp.int32, (batch, LANES), 0)
    pos = jnp.zeros((batch, LANES), jnp.int32)
    for b in range(batch):
        pos = jnp.where(subb == b, len_s[b], pos)
    ang = jnp.concatenate([(pos + s).astype(F32) * inv for s in range(steps)], axis=0)
    cos = jnp.cos(ang) * ROPE_MSCALE
    sin = jnp.sin(ang) * ROPE_MSCALE
    lane_r = lax.broadcasted_iota(jnp.int32, (rows, LANES), 1)
    sin = jnp.where(lax.rem(lane_r, hd) < half_dim, -sin, sin)
    low_half = lax.rem(lane_r, hd) < half_dim
    low_head = lane_r < hd

    def rope(t):
        t = t.astype(BF16).astype(F32)
        rot = jnp.where(low_half, pltpu.roll(t, LANES - half_dim, 1), pltpu.roll(t, half_dim, 1))
        return (t * cos + rot * sin).astype(BF16).astype(F32)

    def q_block(hp):
        t = jnp.dot(h, wq_s[hp], preferred_element_type=F32) + bq[:, hp * qw:(hp + 1) * qw]
        parts = [rope(t[:, c * LANES:(c + 1) * LANES]) for c in range(qw // LANES)]
        for g in range(group):
            first, second = g, group + g
            a, a_hi = parts[first // 2], first % 2
            c, c_hi = parts[second // 2], second % 2
            a = pltpu.roll(a, hd, 1) if a_hi else a
            c = c if c_hi else pltpu.roll(c, hd, 1)
            q_s[hp, g * steps:(g + 1) * steps] = jnp.where(low_head, a, c).reshape(steps, batch, LANES)

    wq_copies[0].wait()
    for cp in (k_copies[0], k_copies[1], v_copies[0], k_copies[2]):
        cp.start()
    wq_copies[1].wait()
    for hp in range(2):
        q_block(hp)
    for cp in wq_copies[2:] + wkv_copies:
        cp.wait()
    for cp in (v_copies[1], k_copies[3], v_copies[2], v_copies[3]):
        cp.start()
    for hp in range(2, n_hp):
        q_block(hp)
    t = jnp.dot(h, wk_s[...], preferred_element_type=F32) + bk_s[...].reshape(1, hdk)
    for hp in range(n_hp):
        kt_s[hp] = rope(t[:, hp * LANES:(hp + 1) * LANES]).reshape(steps, batch, LANES)
    t = (jnp.dot(h, wv_s[...], preferred_element_type=F32) + bv_s[...].reshape(1, hdk)).astype(BF16).astype(F32)
    for hp in range(n_hp):
        vt_s[hp] = t[:, hp * LANES:(hp + 1) * LANES].reshape(steps, batch, LANES)

    tpos = me * shard + lax.broadcasted_iota(jnp.int32, (1, shard), 1)
    diag = lax.broadcasted_iota(jnp.int32, (heads_kv, hdk), 0) == lax.broadcasted_iota(jnp.int32, (heads_kv, hdk), 1) // hd
    ident = lax.broadcasted_iota(jnp.int32, (qrows, LANES), 0) == lax.broadcasted_iota(jnp.int32, (qrows, LANES), 1)
    o_rows = gs_n * quad
    m_rows = o_rows + quad
    last = o_rows // SUBL * SUBL
    n_tile = last // SUBL + 1
    lane8 = lax.broadcasted_iota(jnp.int32, (SUBL, LANES), 1)
    sub8 = lax.broadcasted_iota(jnp.int32, (SUBL, LANES), 0)
    low8 = lane8 < hd
    low4 = sub8 < quad

    tail_hp = 2 * core + lax.rem(chip, 2)
    tail_q = chip // 2 * 2
    brow = pl.ds(pl.multiple_of(tail_q * quad, SUBL), SUBL)
    for q in range(n_quad):
        tail_s[q, :m_rows] = jnp.zeros((m_rows, LANES), F32)
        tail_s[q, m_rows:m_rows + SUBL] = jnp.full((SUBL, LANES), NEG_FILL, F32)
        tail_s[q, m_rows + SUBL:] = jnp.zeros((SUBL, LANES), F32)
        for hp in range(n_hp):
            msg_s[q, hp, o_rows:] = jnp.zeros((quad, LANES), F32)
    m_tail = jnp.full((SUBL, LANES), NEG_FILL, F32)
    l_tail = jnp.zeros((SUBL, LANES), F32)
    for gs in range(gs_n):
        s = gs % steps
        qt = q_s[tail_hp, gs, brow, :]
        cols = []
        for slot in range(s + 1):
            prod = qt * kt_s[tail_hp, slot, brow, :]
            lo = jnp.sum(jnp.where(low8, prod, 0.0), axis=1, keepdims=True)
            hi = jnp.sum(jnp.where(low8, 0.0, prod), axis=1, keepdims=True)
            cols.append(jnp.where(low8, lo, hi) * (hd ** -0.5))
        mx = functools.reduce(jnp.maximum, cols)
        ws = [jnp.exp(c - mx) for c in cols]
        lsum = functools.reduce(jnp.add, ws)
        acc = functools.reduce(jnp.add, [w.astype(BF16).astype(F32) * vt_s[tail_hp, slot, brow, :] for slot, w in enumerate(ws)])
        for i in range(2):
            tail_s[tail_q + i, gs * quad:(gs + 1) * quad] = acc[i * quad:(i + 1) * quad]
        for j in range(2):
            sel = lane8 == gs * heads_kv + j
            m_tail = jnp.where(sel, mx[:, j * hd:j * hd + 1], m_tail)
            l_tail = jnp.where(sel, lsum[:, j * hd:j * hd + 1], l_tail)
    m_tail = pltpu.roll(m_tail, 2 * tail_hp, 1)
    l_tail = pltpu.roll(l_tail, 2 * tail_hp, 1)
    for i in range(2):
        for k in range(2):
            rs = slice(m_rows + k * quad, m_rows + (k + 1) * quad)
            tail_s[tail_q + i, rs] = m_tail[i * quad:(i + 1) * quad]
            rs = slice(m_rows + SUBL + k * quad, m_rows + SUBL + (k + 1) * quad)
            tail_s[tail_q + i, rs] = l_tail[i * quad:(i + 1) * quad]

    def to_row(col):
        return jnp.sum(jnp.where(ident, col, 0.0), axis=0, keepdims=True)

    def scores(i):
        for j in range(quad):
            b = i * quad + j
            blocks = []
            for gs in range(gs_n):
                qrow = jnp.concatenate([q_s[hp, gs, b:b + 1, :] for hp in range(n_hp)], axis=1)
                blocks.append(jnp.where(diag, qrow, 0.0))
            blocks.append(jnp.zeros((heads_kv, hdk), F32))
            qbd = jnp.concatenate(blocks, axis=0).astype(BF16)
            keep = tpos < len_s[b]
            sc = jnp.dot(qbd, k_s[b], preferred_element_type=F32) * (hd ** -0.5)
            sc = jnp.where(keep, sc, NEG_FILL)
            m = jnp.max(sc, axis=1, keepdims=True)
            w = jnp.where(keep, jnp.exp(sc - m), 0.0)
            p_s[b] = w.astype(BF16)
            mrow, lrow = to_row(m), to_row(jnp.sum(w, axis=1, keepdims=True))
            for k in range(2):
                r = k * quad + j
                ml_s[i, 0, r:r + 1, :] = mrow
                ml_s[i, 1, r:r + 1, :] = lrow

    def outputs(i):
        for j in range(quad):
            b = i * quad + j
            o = lax.dot_general(p_s[b], v_s[b], NT, preferred_element_type=F32)
            for gs in range(gs_n):
                row = jnp.sum(jnp.where(diag, o[gs * heads_kv:(gs + 1) * heads_kv], 0.0), axis=0, keepdims=True)
                for hp in range(n_hp):
                    msg_s[i, hp, gs * quad + j:gs * quad + j + 1, :] = row[:, hp * LANES:(hp + 1) * LANES]

    def spread(t, lane):
        return jnp.where(low8, t[:, lane:lane + 1], t[:, lane + 1:lane + 2])

    def both_halves(t):
        return jnp.where(low4, t, pltpu.roll(t, LANES - heads_kv, 1))

    tiles = [pl.ds(t * SUBL, SUBL) for t in range(n_tile)]

    def ml_copy(q):
        return remote(ml_s.at[q], mlp_s.at[q], ml_send.at[0], ml_recv.at[q], partner)

    def pair_copy(q):
        return remote(msg_s.at[q, pl.ds(2 * other, 2)], pair_s.at[q], pair_send.at[0], pair_recv.at[q], partner)

    def pair_factors(q):
        ms = [ml_s[q, 0], mlp_s[q, 0], tail_s[q, pl.ds(m_rows, SUBL)]]
        ls = [ml_s[q, 1], mlp_s[q, 1], tail_s[q, pl.ds(m_rows + SUBL, SUBL)]]
        mm = functools.reduce(jnp.maximum, ms)
        es = [jnp.exp(m - mm) for m in ms]
        ll = functools.reduce(jnp.add, [e * l for e, l in zip(es, ls)])
        recv_s[q, chip, core, 0, o_rows:] = mm[quad:]
        recv_s[q, chip, core, 1, o_rows:] = ll[quad:]
        es = [both_halves(e) for e in es]
        es[2] = pltpu.roll(es[2], lax.rem(LANES - 2 * tail_hp, LANES), 1)
        for k in range(2):
            shift = lax.rem(LANES - 2 * (2 * core + k), LANES)
            fs = [pltpu.roll(es[0], shift, 1), pltpu.roll(es[1], shift, 1), jnp.where(lax.rem(chip, 2) == k, es[2], 0.0)]
            for i, f in enumerate(fs):
                for t in range(n_tile):
                    cf_s[q, k, i, tiles[t]] = spread(f, t * 2 * heads_kv)

    def pair_merge(q):
        pair_copy(q).wait_recv()
        dst = recv_s.at[q, chip, core]
        for k in range(2):
            rs = pl.ds(0, o_rows)
            dst[k, rs] = cf_s[q, k, 0, rs] * msg_s[q, 2 * core + k, rs] + cf_s[q, k, 1, rs] * pair_s[q, k, rs] + cf_s[q, k, 2, rs] * tail_s[q, rs]
        for dx in (2, 1, 3):
            remote(dst, dst, g_send.at[0], g_recv.at[q, chip, core], lax.rem(chip + dx, n_hp) * 2 + core).start()
        remote(dst, dst, g_send.at[1], g_recv.at[q, chip, core], partner).start()

    def part_arrived(q, cx, c):
        blk = recv_s.at[q, cx, c]
        remote(blk, blk, g_send.at[0], g_recv.at[q, cx, c], me).wait_recv()
        return blk

    def part_relay(q):
        for dx in (1, 3, 2):
            cx = lax.rem(chip + dx, n_hp)
            blk = part_arrived(q, cx, core)
            remote(blk, blk, g_send.at[1], g_recv.at[q, cx, core], partner).start()

    def final_merge(q):
        for dx in (0, 1, 3, 2):
            part_arrived(q, lax.rem(chip + dx, n_hp), other)
        for c in range(2):
            ms = [recv_s[q, cx, c, 0, tiles[-1]] for cx in range(n_hp)]
            mm = functools.reduce(jnp.maximum, ms)
            es = [jnp.exp(m - mm) for m in ms]
            inv_l = 1.0 / functools.reduce(jnp.add, [e * recv_s[q, cx, c, 1, tiles[-1]] for cx, e in enumerate(es)])
            es = [jnp.where(low4, pltpu.roll(e * inv_l, quad, 0), pltpu.roll(e * inv_l, LANES - heads_kv, 1)) for e in es]
            for k in range(2):
                hp = 2 * c + k
                for t in range(n_tile):
                    lane = t * 2 * heads_kv + 2 * hp
                    o = functools.reduce(jnp.add, [spread(e, lane) * recv_s[q, cx, c, k, tiles[t]] for cx, e in enumerate(es)])
                    for i in range(2):
                        gs = 2 * t + i
                        if gs < gs_n:
                            r = gs % steps * batch + q * quad
                            of_s[gs // steps, r:r + quad, hp * LANES:(hp + 1) * LANES] = o[i * quad:(i + 1) * quad]

    for i in range(n_quad + 1):
        if i < n_quad:
            k_copies[i].wait()
        if i:
            v_copies[i - 1].wait()
        if i > 1:
            ml_copy(i - 2).wait_recv()
        if i < n_quad:
            scores(i)
        if i:
            outputs(i - 1)
        if i > 1:
            pair_factors(i - 2)
        if i == 0:
            pl.semaphore_wait(barrier, n - 1)
        if i < n_quad:
            ml_copy(i).start()
        if i:
            pair_copy(i - 1).start()
        if i == n_quad // 2:
            for g in range(group):
                pltpu.make_async_copy(wo_hbm.at[:, :, g], wo_s.at[:, g], wo_sem.at[0]).start()
            weight_start(wg_hbm, wg_s, exp_sem.at[0])
            weight_start(wu_hbm, wu_s, exp_sem.at[1])
            weight_start(wd_hbm, wd_s, wd_sem.at[0])
        if i > 1:
            pair_merge(i - 2)
    ml_copy(n_quad - 1).wait_recv()
    pair_factors(n_quad - 1)
    pair_merge(n_quad - 1)

    part_relay(0)
    for q in range(n_quad):
        if q + 1 < n_quad:
            part_relay(q + 1)
        else:
            weight_wait(wo_s, wo_sem.at[0])
            weight_wait(wg_s, exp_sem.at[0])
            weight_wait(wu_s, exp_sem.at[1])
            weight_wait(wd_s, wd_sem.at[0])
        final_merge(q)

    lhs = jnp.concatenate([of_s[g, :, hp * LANES:(hp + 1) * LANES] for hp in range(n_hp) for g in range(group)], axis=1).astype(BF16)
    acc = jnp.dot(lhs, wo_s[...].reshape(dm, dm), preferred_element_type=F32)
    x = x_s[...].reshape(rows, dm).astype(F32)
    xm = (x + acc + bo).astype(BF16).astype(F32)
    xm_s[...] = xm.reshape(2, rows // 2, dm)
    h2 = norm_rows(xm, g2, b2)

    logits = lax.dot_general(h2, wr_s[...], NT, preferred_element_type=F32)
    topk = mask_s.shape[1]
    e_iota = lax.broadcasted_iota(jnp.int32, (topk, n_exp), 1)
    grows = []
    for s in range(steps):
        ids = idx_s[s]
        for b in range(batch):
            r = s * batch + b
            lg = jnp.where(mask_s[r] == 1, logits[r:r + 1, :], NEG_FILL)
            ex = jnp.exp(lg - jnp.max(lg, axis=1, keepdims=True))
            pr = ex / jnp.sum(ex, axis=1, keepdims=True)
            grows.append(jnp.sum(jnp.where(ids[:, b:b + 1] == e_iota, pr, 0.0), axis=0, keepdims=True))
    gates = jnp.concatenate(grows, axis=0)
    per = LANES // ff

    def act(c):
        rs = pl.ds(c * LANES, LANES)
        ag = lax.dot_general(h2, wg_s[rs, :], NT, preferred_element_type=F32)
        au = lax.dot_general(h2, wu_s[rs, :], NT, preferred_element_type=F32)
        return ag * (1.0 / (1.0 + jnp.exp(-ag))), au

    peel = n_ec // 4
    for c in range(n_ec):
        gex_s[c] = jnp.where(low_head, gates[:, per * c:per * c + 1], gates[:, per * c + 1:per * c + 2])
    for c in range(peel):
        sg, au = act(c)
        u_s[c] = (gex_s[c] * sg * au).astype(BF16)

    def expert(i, _):
        for j in range(peel):
            c = i * peel + j
            sg, au = act(c)
            u_s[c] = (gex_s[c] * sg * au).astype(BF16)
        return 0

    lax.fori_loop(1, n_ec // peel, expert, 0)
    cw = n_hp * LANES
    n_ch = dm // cw
    hr = rows // 2
    u = jnp.concatenate([u_s[c] for c in range(n_ec)], axis=1)

    def d_copy(k):
        return remote(pbuf_s.at[k, other], ppair_s.at[k], d_send.at[0], d_recv.at[k], partner)

    def add_pair(k):
        d_copy(k).wait_recv()
        psum_s[k] = pbuf_s[k, core] + ppair_s[k]
        for dx in (2, 1, 3):
            cx = lax.rem(chip + dx, n_hp)
            remote(psum_s.at[k, cx], rbuf_s.at[k, chip], p_send.at[0], p_recv.at[k, chip], cx * 2 + core).start()

    for k in range(n_ch):
        part = jnp.dot(u, wd_s[:, k * cw:(k + 1) * cw], preferred_element_type=F32)
        part = part.astype(BF16).astype(F32)
        for half in range(2):
            for cx in range(n_hp):
                pbuf_s[k, half, cx] = part[half * hr:(half + 1) * hr, cx * LANES:(cx + 1) * LANES]
        d_copy(k).start()
        if k:
            add_pair(k - 1)
    add_pair(n_ch - 1)

    for src_s, dst, out, i in ((kt_s, tk_s, tk_out, 0), (vt_s, tv_s, tv_out, 1)):
        for hp in range(n_hp):
            t = src_s[hp].reshape(rows, LANES)
            hs_s[:, 2 * hp, :] = t[:, :hd]
            hs_s[:, 2 * hp + 1, :] = pltpu.roll(t, hd, 1)[:, :hd]
        for s in range(steps):
            dst[:, s] = hs_s[s * batch:(s + 1) * batch].astype(BF16)
        pltpu.make_async_copy(dst, out, out_sem.at[i]).start()

    def y_arrived(k, cx, c):
        blk = ybuf_s.at[k, cx, c]
        remote(blk, blk, y_send.at[0], y_recv.at[k, cx, c], me).wait_recv()
        return blk

    for k in range(n_ch):
        y = xm_s[core, :, pl.ds(pl.multiple_of(k * cw + chip * LANES, LANES), LANES)] + psum_s[k, chip]
        for dx in (1, 3, 2):
            cx = lax.rem(chip + dx, n_hp)
            remote(rbuf_s.at[k, cx], rbuf_s.at[k, cx], p_send.at[0], p_recv.at[k, cx], me).wait_recv()
            y = y + rbuf_s[k, cx]
        ybuf_s[k, chip, core] = y.astype(BF16).astype(F32)
        blk = ybuf_s.at[k, chip, core]
        for dx in (2, 1, 3):
            remote(blk, blk, y_send.at[0], y_recv.at[k, chip, core], lax.rem(chip + dx, n_hp) * 2 + core).start()
        remote(blk, blk, y_send.at[1], y_recv.at[k, chip, core], partner).start()
    for k in range(n_ch):
        for dx in (1, 3, 2):
            cx = lax.rem(chip + dx, n_hp)
            blk = y_arrived(k, cx, core)
            remote(blk, blk, y_send.at[1], y_recv.at[k, cx, core], partner).start()
    for k in range(n_ch):
        for dx in (0, 1, 3, 2):
            y_arrived(k, lax.rem(chip + dx, n_hp), other)
        for cx in range(n_hp):
            blk = jnp.concatenate([ybuf_s[k, cx, 0], ybuf_s[k, cx, 1]], axis=0)
            hid_s[:, :, k * cw + cx * LANES:k * cw + (cx + 1) * LANES] = blk.astype(BF16).reshape(steps, batch, LANES)
    hid_cp = pltpu.make_async_copy(hid_s, hid_out, out_sem.at[2])
    hid_cp.start()
    one = pl.ds(0, 1)
    part_blocks = pl.ds(0, n_hp - 1)
    for blks, sem in ((mlp_s, ml_send.at[0]), (pair_s, pair_send.at[0]), (recv_s.at[part_blocks, :, one], g_send.at[0]), (recv_s.at[:, :, one], g_send.at[1]),
                      (ppair_s, d_send.at[0]), (rbuf_s.at[:, part_blocks], p_send.at[0]), (ybuf_s.at[:, part_blocks, one], y_send.at[0]), (ybuf_s.at[:, :, one], y_send.at[1])):
        pltpu.make_async_copy(blks, blks, sem).wait()
    pltpu.make_async_copy(tk_s, tk_out, out_sem.at[0]).wait()
    pltpu.make_async_copy(tv_s, tv_out, out_sem.at[1]).wait()
    hid_cp.wait()


def emit_kernel(*refs):
    k = len(refs) // 3
    ins, outs, bufs, sem = refs[:k], refs[k:2 * k], refs[2 * k:3 * k], refs[3 * k]
    loads = [pltpu.make_async_copy(ins[i], bufs[i], sem.at[0, i]) for i in range(k)]
    stores = [pltpu.make_async_copy(bufs[i], outs[i], sem.at[1, i]) for i in range(k)]
    for cp in loads:
        cp.start()
    for ld, st in zip(loads, stores):
        ld.wait()
        st.start()
    for cp in stores:
        cp.wait()


def solution(mesh):
    n = mesh.shape['kv']

    def layer_steps(x_first, next_emb, k_cache, v_cache, seq_len, ln1_gain, ln1_bias, w_q, b_q, w_k, b_k, w_v, b_v, w_o, b_o, ln2_gain, ln2_bias, w_router, w_gate, w_up, w_down, long_factor, expert_idx, route_mask):
        batch, shard, heads_kv, hd = k_cache.shape
        dm = x_first.shape[1]
        q_heads = w_q.shape[1] // hd
        group = q_heads // heads_kv
        steps = next_emb.shape[0] + 1
        n_exp, _, ff = w_gate.shape
        topk = expert_idx.shape[-1]
        rows = steps * batch
        hdk = heads_kv * hd
        n_hp = hdk // LANES
        gs_n = group * steps
        qrows = (gs_n + 1) * heads_kv
        fe = n_exp * ff
        dims = (n, steps, batch, heads_kv, hd, group, shard, n_exp, ff, dm)
        args = (
            x_first, next_emb,
            jnp.transpose(k_cache, (0, 2, 3, 1)).reshape(batch, hdk, shard),
            jnp.transpose(v_cache, (0, 2, 3, 1)).reshape(batch, hdk, shard),
            seq_len, ln1_gain, ln1_bias, w_q, b_q, w_k, b_k, w_v, b_v,
            w_o.reshape(n_hp, 2, group, hd, dm), b_o, ln2_gain, ln2_bias,
            jnp.transpose(w_router),
            jnp.transpose(w_gate, (0, 2, 1)).reshape(fe, dm),
            jnp.transpose(w_up, (0, 2, 1)).reshape(fe, dm),
            w_down.reshape(fe, dm), long_factor,
            jnp.transpose(expert_idx, (0, 2, 1)),
            route_mask.reshape(rows, topk, n_exp),
        )
        any_spec = pl.BlockSpec(memory_space=pl.ANY)
        dma = pltpu.SemaphoreType.DMA
        vm = pltpu.VMEM
        outs = (
            jax.ShapeDtypeStruct((steps, batch, dm), BF16),
            jax.ShapeDtypeStruct((batch, steps, heads_kv, hd), BF16),
            jax.ShapeDtypeStruct((batch, steps, heads_kv, hd), BF16),
        )
        n_quad = batch // (SUBL // 2)
        m_rows = (gs_n + 1) * (SUBL // 2)
        n_ch = dm // hdk
        qblk = vm((n_ch, n_hp, rows // 2, LANES), F32)
        scratch = [
            vm((steps, batch, dm), BF16), pltpu.SMEM((batch,), jnp.int32), pltpu.SMEM((hd // 2,), F32),
            vm((6, dm), F32), vm((hdk,), F32), vm((hdk,), F32), vm((n_exp, dm), BF16),
            vm((steps, topk, batch), jnp.int32), vm((rows, topk, n_exp), jnp.int32),
            vm((n_hp, dm, dm // n_hp), BF16), vm((dm, hdk), BF16), vm((dm, hdk), BF16),
            vm((n_hp, group, 2, hd, dm), BF16), vm((batch, hdk, shard), BF16), vm((batch, hdk, shard), BF16),
            vm((fe, dm), BF16), vm((fe, dm), BF16), vm((fe, dm), BF16),
            vm((n_hp, gs_n, batch, LANES), F32), vm((n_hp, steps, batch, LANES), F32), vm((n_hp, steps, batch, LANES), F32),
            vm((rows, heads_kv, hd), F32), vm((batch, qrows, shard), BF16),
            vm((n_quad, n_hp, m_rows, LANES), F32), vm((n_quad, 2, m_rows, LANES), F32),
            vm((n_quad, 2, SUBL, LANES), F32), vm((n_quad, 2, SUBL, LANES), F32), vm((n_quad, 2, 3, m_rows, LANES), F32), vm((n_quad, m_rows + 2 * SUBL, LANES), F32),
            vm((n_quad, n_hp, 2, 2, m_rows, LANES), F32), vm((group, rows, hdk), F32), vm((2, rows // 2, dm), F32),
            vm((fe // LANES, rows, LANES), F32), vm((fe // LANES, rows, LANES), BF16),
            vm((n_ch, 2, n_hp, rows // 2, LANES), F32), qblk, qblk, qblk, vm((n_ch, n_hp, 2, rows // 2, LANES), F32),
        ] + [vm(o.shape, o.dtype) for o in outs] + [
            dma((14,)), dma((n_hp,)), dma((2,)), dma((1,)), dma((4,)), dma((4,)), dma((2,)), dma((1,)), dma((3,)),
            dma((1,)), dma((n_quad,)), dma((1,)), dma((n_quad,)), dma((2,)), dma((n_quad, n_hp, 2)),
            dma((1,)), dma((n_ch,)), dma((1,)), dma((n_ch, n_hp)), dma((2,)), dma((n_ch, n_hp, 2)),
        ]
        made = pl.pallas_call(
            functools.partial(layer_kernel, dims),
            out_shape=outs,
            in_specs=[any_spec] * len(args),
            out_specs=(any_spec,) * 3,
            scratch_shapes=scratch,
            compiler_params=pltpu.CompilerParams(collective_id=0, has_side_effects=True, vmem_limit_bytes=64 * 1024 * 1024),
        )(*args)
        return pl.pallas_call(
            emit_kernel,
            out_shape=outs,
            in_specs=[any_spec] * 3,
            out_specs=(any_spec,) * 3,
            scratch_shapes=[vm(o.shape, o.dtype) for o in outs] + [dma((2, 3))],
        )(*made)

    replicated = P()
    in_specs = (P('dp'), P(None, 'dp'), P('dp', 'kv'), P('dp', 'kv'), P('dp')) + (replicated,) * 13 + (P(None, None, 'kv'), P(None, None, 'kv'), P(None, 'kv'), replicated, P(None, 'dp'), P(None, 'dp'))
    out_specs = (P(None, 'dp'), P('dp'), P('dp'))
    return jax.shard_map(layer_steps, mesh=mesh, in_specs=in_specs, out_specs=out_specs, check_vma=False)
```

```python
import functools
import math

import jax
import jax.numpy as jnp
from jax import lax
from jax.experimental import pallas as pl
from jax.experimental.pallas import tpu as pltpu
from jax.sharding import PartitionSpec as P

ROPE_BASE = 10000.0
ROPE_MSCALE = math.sqrt(1.0 + math.log(32.0) / math.log(4096.0))
NORM_EPS = 1e-5
NEG_FILL = -1e30
LANES = 128
SUBL = 8
F32 = jnp.float32
BF16 = jnp.bfloat16
NT = (((1,), (1,)), ((), ()))


def norm_rows(x, gain, bias):
    mean = jnp.mean(x, axis=-1, keepdims=True)
    cent = x - mean
    var = jnp.mean(cent * cent, axis=-1, keepdims=True)
    return (cent * lax.rsqrt(var + NORM_EPS) * gain + bias).astype(BF16)


def layer_kernel(dims, x_first, next_emb, k_hbm, v_hbm, len_hbm, g1_hbm, b1_hbm, wq_hbm, bq_hbm, wk_hbm, bk_hbm, wv_hbm, bv_hbm, wo_hbm, bo_hbm, g2_hbm, b2_hbm, wr_hbm, wg_hbm, wu_hbm, wd_hbm, lf_hbm, idx_hbm, mask_hbm,
                 hid_out, tk_out, tv_out,
                 x_s, len_s, lf_s, vec_s, bk_s, bv_s, wr_s, idx_s, mask_s,
                 wq_s, wk_s, wv_s, wo_s, k_s, v_s, wg_s, wu_s, wd_s,
                 q_s, kt_s, vt_s, hs_s, p_s, msg_s, pair_s, ml_s, mlp_s, cf_s, tail_s, recv_s, of_s, xm_s, gex_s, u_s, pbuf_s, ppair_s, psum_s, rbuf_s, ybuf_s,
                 hid_s, tk_s, tv_s,
                 small_sem, wq_sem, wkv_sem, wo_sem, k_sem, v_sem, exp_sem, wd_sem, out_sem,
                 ml_send, ml_recv, pair_send, pair_recv, g_send, g_recv, d_send, d_recv, p_send, p_recv, y_send, y_recv):
    n, steps, batch, heads_kv, hd, group, shard, n_exp, ff, dm = dims
    rows = steps * batch
    gs_n = group * steps
    qrows = (gs_n + 1) * heads_kv
    hdk = heads_kv * hd
    n_hp = hdk // LANES
    me = lax.axis_index('kv')
    chip = me // 2
    core = lax.rem(me, 2)
    other = 1 - core
    partner = chip * 2 + other
    mesh_id = pl.DeviceIdType.MESH

    def remote(src, dst, send, recv, dev):
        return pltpu.make_async_remote_copy(src_ref=src, dst_ref=dst, send_sem=send, recv_sem=recv, device_id={'kv': dev}, device_id_type=mesh_id)

    vecs = (g1_hbm, b1_hbm, bq_hbm, bo_hbm, g2_hbm, b2_hbm)
    smalls = [(x_first, x_s.at[0], 0), (next_emb, x_s.at[pl.ds(1, steps - 1)], 0)]
    smalls += [(len_hbm, len_s, 1), (lf_hbm, lf_s, 2), (bk_hbm, bk_s, 3), (bv_hbm, bv_s, 4), (wr_hbm, wr_s, 5), (idx_hbm, idx_s, 6), (mask_hbm, mask_s, 7)]
    smalls += [(src, vec_s.at[i], 8 + i) for i, src in enumerate(vecs)]
    small_copies = [pltpu.make_async_copy(src, dst, small_sem.at[i]) for src, dst, i in smalls]
    small_waits = [pltpu.make_async_copy(x_s, x_s, small_sem.at[0])] + small_copies[2:]
    qw = wq_s.shape[2]
    wq_copies = [pltpu.make_async_copy(wq_hbm.at[:, pl.ds(i * qw, qw)], wq_s.at[i], wq_sem.at[i]) for i in range(n_hp)]
    wkv_copies = [pltpu.make_async_copy(wk_hbm, wk_s, wkv_sem.at[0]), pltpu.make_async_copy(wv_hbm, wv_s, wkv_sem.at[1])]
    for cp in small_copies + wq_copies + wkv_copies:
        cp.start()

    barrier = pltpu.get_barrier_semaphore()
    for d in range(1, n):
        pl.semaphore_signal(barrier, inc=1, device_id={'kv': lax.rem(me + d, n)}, device_id_type=mesh_id)

    quad = SUBL // 2
    n_quad = batch // quad

    def cache_copy(src, dst, sem, i):
        sl = pl.ds(i * quad, quad)
        return pltpu.make_async_copy(src.at[sl], dst.at[sl], sem.at[i])

    k_copies = [cache_copy(k_hbm, k_s, k_sem, i) for i in range(n_quad)]
    v_copies = [cache_copy(v_hbm, v_s, v_sem, i) for i in range(n_quad)]
    n_ec = wg_s.shape[0] // LANES

    def weight_start(src, dst, sem, parts=4):
        ec = src.shape[0] // parts
        for i in range(parts):
            pltpu.make_async_copy(src.at[pl.ds(i * ec, ec)], dst.at[pl.ds(i * ec, ec)], sem).start()

    def weight_wait(dst, sem):
        pltpu.make_async_copy(dst, dst, sem).wait()

    for cp in small_waits:
        cp.wait()

    g1, b1, bq, bo, g2, b2 = [vec_s[i].reshape(1, dm) for i in range(6)]
    x = x_s[...].reshape(rows, dm).astype(F32)
    h = norm_rows(x, g1, b1)

    lane1 = lax.broadcasted_iota(jnp.int32, (1, LANES), 1)
    half_dim = hd // 2
    jlane = lax.rem(lane1, half_dim)
    lfv = jnp.zeros((1, LANES), F32)
    for j in range(half_dim):
        lfv = jnp.where(jlane == j, lf_s[j], lfv)
    inv = 1.0 / (lfv * jnp.exp(jlane.astype(F32) * (2.0 * math.log(ROPE_BASE) / hd)))
    subb = lax.broadcasted_iota(jnp.int32, (batch, LANES), 0)
    pos = jnp.zeros((batch, LANES), jnp.int32)
    for b in range(batch):
        pos = jnp.where(subb == b, len_s[b], pos)
    ang = jnp.concatenate([(pos + s).astype(F32) * inv for s in range(steps)], axis=0)
    cos = jnp.cos(ang) * ROPE_MSCALE
    sin = jnp.sin(ang) * ROPE_MSCALE
    lane_r = lax.broadcasted_iota(jnp.int32, (rows, LANES), 1)
    sin = jnp.where(lax.rem(lane_r, hd) < half_dim, -sin, sin)
    low_half = lax.rem(lane_r, hd) < half_dim
    low_head = lane_r < hd

    def rope(t):
        t = t.astype(BF16).astype(F32)
        rot = jnp.where(low_half, pltpu.roll(t, LANES - half_dim, 1), pltpu.roll(t, half_dim, 1))
        return (t * cos + rot * sin).astype(BF16).astype(F32)

    def q_block(hp):
        t = jnp.dot(h, wq_s[hp], preferred_element_type=F32) + bq[:, hp * qw:(hp + 1) * qw]
        parts = [rope(t[:, c * LANES:(c + 1) * LANES]) for c in range(qw // LANES)]
        for g in range(group):
            first, second = g, group + g
            a, a_hi = parts[first // 2], first % 2
            c, c_hi = parts[second // 2], second % 2
            a = pltpu.roll(a, hd, 1) if a_hi else a
            c = c if c_hi else pltpu.roll(c, hd, 1)
            q_s[hp, g * steps:(g + 1) * steps] = jnp.where(low_head, a, c).reshape(steps, batch, LANES)

    wq_copies[0].wait()
    for cp in (k_copies[0], k_copies[1], v_copies[0], k_copies[2]):
        cp.start()
    wq_copies[1].wait()
    for hp in range(2):
        q_block(hp)
    for cp in wq_copies[2:] + wkv_copies:
        cp.wait()
    for cp in (v_copies[1], k_copies[3], v_copies[2], v_copies[3]):
        cp.start()
    for hp in range(2, n_hp):
        q_block(hp)
    t = jnp.dot(h, wk_s[...], preferred_element_type=F32) + bk_s[...].reshape(1, hdk)
    for hp in range(n_hp):
        kt_s[hp] = rope(t[:, hp * LANES:(hp + 1) * LANES]).reshape(steps, batch, LANES)
    t = (jnp.dot(h, wv_s[...], preferred_element_type=F32) + bv_s[...].reshape(1, hdk)).astype(BF16).astype(F32)
    for hp in range(n_hp):
        vt_s[hp] = t[:, hp * LANES:(hp + 1) * LANES].reshape(steps, batch, LANES)

    tpos = me * shard + lax.broadcasted_iota(jnp.int32, (1, shard), 1)
    diag = lax.broadcasted_iota(jnp.int32, (heads_kv, hdk), 0) == lax.broadcasted_iota(jnp.int32, (heads_kv, hdk), 1) // hd
    ident = lax.broadcasted_iota(jnp.int32, (qrows, LANES), 0) == lax.broadcasted_iota(jnp.int32, (qrows, LANES), 1)
    o_rows = gs_n * quad
    m_rows = o_rows + quad
    last = o_rows // SUBL * SUBL
    n_tile = last // SUBL + 1
    lane8 = lax.broadcasted_iota(jnp.int32, (SUBL, LANES), 1)
    sub8 = lax.broadcasted_iota(jnp.int32, (SUBL, LANES), 0)
    low8 = lane8 < hd
    low4 = sub8 < quad

    tail_hp = 2 * core + lax.rem(chip, 2)
    tail_q = chip // 2 * 2
    brow = pl.ds(pl.multiple_of(tail_q * quad, SUBL), SUBL)
    for q in range(n_quad):
        tail_s[q, :m_rows] = jnp.zeros((m_rows, LANES), F32)
        tail_s[q, m_rows:m_rows + SUBL] = jnp.full((SUBL, LANES), NEG_FILL, F32)
        tail_s[q, m_rows + SUBL:] = jnp.zeros((SUBL, LANES), F32)
        for hp in range(n_hp):
            msg_s[q, hp, o_rows:] = jnp.zeros((quad, LANES), F32)
    m_tail = jnp.full((SUBL, LANES), NEG_FILL, F32)
    l_tail = jnp.zeros((SUBL, LANES), F32)
    for gs in range(gs_n):
        s = gs % steps
        qt = q_s[tail_hp, gs, brow, :]
        cols = []
        for slot in range(s + 1):
            prod = qt * kt_s[tail_hp, slot, brow, :]
            lo = jnp.sum(jnp.where(low8, prod, 0.0), axis=1, keepdims=True)
            hi = jnp.sum(jnp.where(low8, 0.0, prod), axis=1, keepdims=True)
            cols.append(jnp.where(low8, lo, hi) * (hd ** -0.5))
        mx = functools.reduce(jnp.maximum, cols)
        ws = [jnp.exp(c - mx) for c in cols]
        lsum = functools.reduce(jnp.add, ws)
        acc = functools.reduce(jnp.add, [w.astype(BF16).astype(F32) * vt_s[tail_hp, slot, brow, :] for slot, w in enumerate(ws)])
        for i in range(2):
            tail_s[tail_q + i, gs * quad:(gs + 1) * quad] = acc[i * quad:(i + 1) * quad]
        for j in range(2):
            sel = lane8 == gs * heads_kv + j
            m_tail = jnp.where(sel, mx[:, j * hd:j * hd + 1], m_tail)
            l_tail = jnp.where(sel, lsum[:, j * hd:j * hd + 1], l_tail)
    m_tail = pltpu.roll(m_tail, 2 * tail_hp, 1)
    l_tail = pltpu.roll(l_tail, 2 * tail_hp, 1)
    for i in range(2):
        for k in range(2):
            rs = slice(m_rows + k * quad, m_rows + (k + 1) * quad)
            tail_s[tail_q + i, rs] = m_tail[i * quad:(i + 1) * quad]
            rs = slice(m_rows + SUBL + k * quad, m_rows + SUBL + (k + 1) * quad)
            tail_s[tail_q + i, rs] = l_tail[i * quad:(i + 1) * quad]

    def to_row(col):
        return jnp.sum(jnp.where(ident, col, 0.0), axis=0, keepdims=True)

    def scores(i):
        for j in range(quad):
            b = i * quad + j
            blocks = []
            for gs in range(gs_n):
                qrow = jnp.concatenate([q_s[hp, gs, b:b + 1, :] for hp in range(n_hp)], axis=1)
                blocks.append(jnp.where(diag, qrow, 0.0))
            blocks.append(jnp.zeros((heads_kv, hdk), F32))
            qbd = jnp.concatenate(blocks, axis=0).astype(BF16)
            keep = tpos < len_s[b]
            sc = jnp.dot(qbd, k_s[b], preferred_element_type=F32) * (hd ** -0.5)
            sc = jnp.where(keep, sc, NEG_FILL)
            m = jnp.max(sc, axis=1, keepdims=True)
            w = jnp.where(keep, jnp.exp(sc - m), 0.0)
            p_s[b] = w.astype(BF16)
            mrow, lrow = to_row(m), to_row(jnp.sum(w, axis=1, keepdims=True))
            for k in range(2):
                r = k * quad + j
                ml_s[i, 0, r:r + 1, :] = mrow
                ml_s[i, 1, r:r + 1, :] = lrow

    def outputs(i):
        for j in range(quad):
            b = i * quad + j
            o = lax.dot_general(p_s[b], v_s[b], NT, preferred_element_type=F32)
            for gs in range(gs_n):
                row = jnp.sum(jnp.where(diag, o[gs * heads_kv:(gs + 1) * heads_kv], 0.0), axis=0, keepdims=True)
                for hp in range(n_hp):
                    msg_s[i, hp, gs * quad + j:gs * quad + j + 1, :] = row[:, hp * LANES:(hp + 1) * LANES]

    def spread(t, lane):
        return jnp.where(low8, t[:, lane:lane + 1], t[:, lane + 1:lane + 2])

    def both_halves(t):
        return jnp.where(low4, t, pltpu.roll(t, LANES - heads_kv, 1))

    tiles = [pl.ds(t * SUBL, SUBL) for t in range(n_tile)]

    def ml_copy(q):
        return remote(ml_s.at[q], mlp_s.at[q], ml_send.at[0], ml_recv.at[q], partner)

    def pair_copy(q):
        return remote(msg_s.at[q, pl.ds(2 * other, 2)], pair_s.at[q], pair_send.at[0], pair_recv.at[q], partner)

    def pair_factors(q):
        ms = [ml_s[q, 0], mlp_s[q, 0], tail_s[q, pl.ds(m_rows, SUBL)]]
        ls = [ml_s[q, 1], mlp_s[q, 1], tail_s[q, pl.ds(m_rows + SUBL, SUBL)]]
        mm = functools.reduce(jnp.maximum, ms)
        es = [jnp.exp(m - mm) for m in ms]
        ll = functools.reduce(jnp.add, [e * l for e, l in zip(es, ls)])
        recv_s[q, chip, core, 0, o_rows:] = mm[quad:]
        recv_s[q, chip, core, 1, o_rows:] = ll[quad:]
        es = [both_halves(e) for e in es]
        es[2] = pltpu.roll(es[2], lax.rem(LANES - 2 * tail_hp, LANES), 1)
        for k in range(2):
            shift = lax.rem(LANES - 2 * (2 * core + k), LANES)
            fs = [pltpu.roll(es[0], shift, 1), pltpu.roll(es[1], shift, 1), jnp.where(lax.rem(chip, 2) == k, es[2], 0.0)]
            for i, f in enumerate(fs):
                for t in range(n_tile):
                    cf_s[q, k, i, tiles[t]] = spread(f, t * 2 * heads_kv)

    def pair_merge(q):
        pair_copy(q).wait_recv()
        dst = recv_s.at[q, chip, core]
        for k in range(2):
            rs = pl.ds(0, o_rows)
            dst[k, rs] = cf_s[q, k, 0, rs] * msg_s[q, 2 * core + k, rs] + cf_s[q, k, 1, rs] * pair_s[q, k, rs] + cf_s[q, k, 2, rs] * tail_s[q, rs]
        for dx in (2, 1, 3):
            remote(dst, dst, g_send.at[0], g_recv.at[q, chip, core], lax.rem(chip + dx, n_hp) * 2 + core).start()
        remote(dst, dst, g_send.at[1], g_recv.at[q, chip, core], partner).start()

    def part_arrived(q, cx, c):
        blk = recv_s.at[q, cx, c]
        remote(blk, blk, g_send.at[0], g_recv.at[q, cx, c], me).wait_recv()
        return blk

    def part_relay(q):
        for dx in (1, 3, 2):
            cx = lax.rem(chip + dx, n_hp)
            blk = part_arrived(q, cx, core)
            remote(blk, blk, g_send.at[1], g_recv.at[q, cx, core], partner).start()

    def final_merge(q):
        for dx in (0, 1, 3, 2):
            part_arrived(q, lax.rem(chip + dx, n_hp), other)
        for c in range(2):
            ms = [recv_s[q, cx, c, 0, tiles[-1]] for cx in range(n_hp)]
            mm = functools.reduce(jnp.maximum, ms)
            es = [jnp.exp(m - mm) for m in ms]
            inv_l = 1.0 / functools.reduce(jnp.add, [e * recv_s[q, cx, c, 1, tiles[-1]] for cx, e in enumerate(es)])
            es = [jnp.where(low4, pltpu.roll(e * inv_l, quad, 0), pltpu.roll(e * inv_l, LANES - heads_kv, 1)) for e in es]
            for k in range(2):
                hp = 2 * c + k
                for t in range(n_tile):
                    lane = t * 2 * heads_kv + 2 * hp
                    o = functools.reduce(jnp.add, [spread(e, lane) * recv_s[q, cx, c, k, tiles[t]] for cx, e in enumerate(es)])
                    for i in range(2):
                        gs = 2 * t + i
                        if gs < gs_n:
                            r = gs % steps * batch + q * quad
                            of_s[gs // steps, r:r + quad, hp * LANES:(hp + 1) * LANES] = o[i * quad:(i + 1) * quad]

    for i in range(n_quad + 1):
        if i < n_quad:
            k_copies[i].wait()
        if i:
            v_copies[i - 1].wait()
        if i == n_quad - 1:
            for g in range(group):
                pltpu.make_async_copy(wo_hbm.at[:, :, g], wo_s.at[:, g], wo_sem.at[0]).start()
            weight_start(wg_hbm, wg_s, exp_sem.at[0])
            weight_start(wu_hbm, wu_s, exp_sem.at[1])
            weight_start(wd_hbm, wd_s, wd_sem.at[0])
        if i > 1:
            ml_copy(i - 2).wait_recv()
        if i < n_quad:
            scores(i)
        if i:
            outputs(i - 1)
        if i > 1:
            pair_factors(i - 2)
        if i == 0:
            pl.semaphore_wait(barrier, n - 1)
        if i < n_quad:
            ml_copy(i).start()
        if i:
            pair_copy(i - 1).start()
        if i > 1:
            pair_merge(i - 2)
    ml_copy(n_quad - 1).wait_recv()
    pair_factors(n_quad - 1)
    pair_merge(n_quad - 1)

    part_relay(0)
    for q in range(n_quad):
        if q + 1 < n_quad:
            part_relay(q + 1)
        else:
            weight_wait(wo_s, wo_sem.at[0])
            weight_wait(wg_s, exp_sem.at[0])
            weight_wait(wu_s, exp_sem.at[1])
        final_merge(q)

    lhs = jnp.concatenate([of_s[g, :, hp * LANES:(hp + 1) * LANES] for hp in range(n_hp) for g in range(group)], axis=1).astype(BF16)
    acc = jnp.dot(lhs, wo_s[...].reshape(dm, dm), preferred_element_type=F32)
    x = x_s[...].reshape(rows, dm).astype(F32)
    xm = (x + acc + bo).astype(BF16).astype(F32)
    xm_s[...] = xm.reshape(2, rows // 2, dm)
    h2 = norm_rows(xm, g2, b2)

    logits = lax.dot_general(h2, wr_s[...], NT, preferred_element_type=F32)
    topk = mask_s.shape[1]
    e_iota = lax.broadcasted_iota(jnp.int32, (topk, n_exp), 1)
    grows = []
    for s in range(steps):
        ids = idx_s[s]
        for b in range(batch):
            r = s * batch + b
            lg = jnp.where(mask_s[r] == 1, logits[r:r + 1, :], NEG_FILL)
            ex = jnp.exp(lg - jnp.max(lg, axis=1, keepdims=True))
            pr = ex / jnp.sum(ex, axis=1, keepdims=True)
            grows.append(jnp.sum(jnp.where(ids[:, b:b + 1] == e_iota, pr, 0.0), axis=0, keepdims=True))
    gates = jnp.concatenate(grows, axis=0)
    per = LANES // ff

    def act(c):
        rs = pl.ds(c * LANES, LANES)
        ag = lax.dot_general(h2, wg_s[rs, :], NT, preferred_element_type=F32)
        au = lax.dot_general(h2, wu_s[rs, :], NT, preferred_element_type=F32)
        return ag * (1.0 / (1.0 + jnp.exp(-ag))), au

    peel = n_ec // 4
    for c in range(n_ec):
        gex_s[c] = jnp.where(low_head, gates[:, per * c:per * c + 1], gates[:, per * c + 1:per * c + 2])
    for c in range(peel):
        sg, au = act(c)
        u_s[c] = (gex_s[c] * sg * au).astype(BF16)

    def expert(i, _):
        for j in range(peel):
            c = i * peel + j
            sg, au = act(c)
            u_s[c] = (gex_s[c] * sg * au).astype(BF16)
        return 0

    lax.fori_loop(1, n_ec // peel, expert, 0)
    cw = n_hp * LANES
    n_ch = dm // cw
    hr = rows // 2
    u = jnp.concatenate([u_s[c] for c in range(n_ec)], axis=1)

    def d_copy(k):
        return remote(pbuf_s.at[k, other], ppair_s.at[k], d_send.at[0], d_recv.at[k], partner)

    def add_pair(k):
        d_copy(k).wait_recv()
        psum_s[k] = pbuf_s[k, core] + ppair_s[k]
        for dx in (2, 1, 3):
            cx = lax.rem(chip + dx, n_hp)
            remote(psum_s.at[k, cx], rbuf_s.at[k, chip], p_send.at[0], p_recv.at[k, chip], cx * 2 + core).start()

    weight_wait(wd_s, wd_sem.at[0])
    for k in range(n_ch):
        part = jnp.dot(u, wd_s[:, k * cw:(k + 1) * cw], preferred_element_type=F32)
        part = part.astype(BF16).astype(F32)
        for half in range(2):
            for cx in range(n_hp):
                pbuf_s[k, half, cx] = part[half * hr:(half + 1) * hr, cx * LANES:(cx + 1) * LANES]
        d_copy(k).start()
        if k:
            add_pair(k - 1)
    add_pair(n_ch - 1)

    for src_s, dst, out, i in ((kt_s, tk_s, tk_out, 0), (vt_s, tv_s, tv_out, 1)):
        for hp in range(n_hp):
            t = src_s[hp].reshape(rows, LANES)
            hs_s[:, 2 * hp, :] = t[:, :hd]
            hs_s[:, 2 * hp + 1, :] = pltpu.roll(t, hd, 1)[:, :hd]
        for s in range(steps):
            dst[:, s] = hs_s[s * batch:(s + 1) * batch].astype(BF16)
        pltpu.make_async_copy(dst, out, out_sem.at[i]).start()

    def y_arrived(k, cx, c):
        blk = ybuf_s.at[k, cx, c]
        remote(blk, blk, y_send.at[0], y_recv.at[k, cx, c], me).wait_recv()
        return blk

    for k in range(n_ch):
        y = xm_s[core, :, pl.ds(pl.multiple_of(k * cw + chip * LANES, LANES), LANES)] + psum_s[k, chip]
        for dx in (1, 3, 2):
            cx = lax.rem(chip + dx, n_hp)
            remote(rbuf_s.at[k, cx], rbuf_s.at[k, cx], p_send.at[0], p_recv.at[k, cx], me).wait_recv()
            y = y + rbuf_s[k, cx]
        ybuf_s[k, chip, core] = y.astype(BF16).astype(F32)
        blk = ybuf_s.at[k, chip, core]
        for dx in (2, 1, 3):
            remote(blk, blk, y_send.at[0], y_recv.at[k, chip, core], lax.rem(chip + dx, n_hp) * 2 + core).start()
        remote(blk, blk, y_send.at[1], y_recv.at[k, chip, core], partner).start()
    for k in range(n_ch):
        for dx in (1, 3, 2):
            cx = lax.rem(chip + dx, n_hp)
            blk = y_arrived(k, cx, core)
            remote(blk, blk, y_send.at[1], y_recv.at[k, cx, core], partner).start()
    for k in range(n_ch):
        for dx in (0, 1, 3, 2):
            y_arrived(k, lax.rem(chip + dx, n_hp), other)
        for cx in range(n_hp):
            blk = jnp.concatenate([ybuf_s[k, cx, 0], ybuf_s[k, cx, 1]], axis=0)
            hid_s[:, :, k * cw + cx * LANES:k * cw + (cx + 1) * LANES] = blk.astype(BF16).reshape(steps, batch, LANES)
    hid_cp = pltpu.make_async_copy(hid_s, hid_out, out_sem.at[2])
    hid_cp.start()
    one = pl.ds(0, 1)
    part_blocks = pl.ds(0, n_hp - 1)
    for blks, sem in ((mlp_s, ml_send.at[0]), (pair_s, pair_send.at[0]), (recv_s.at[part_blocks, :, one], g_send.at[0]), (recv_s.at[:, :, one], g_send.at[1]),
                      (ppair_s, d_send.at[0]), (rbuf_s.at[:, part_blocks], p_send.at[0]), (ybuf_s.at[:, part_blocks, one], y_send.at[0]), (ybuf_s.at[:, :, one], y_send.at[1])):
        pltpu.make_async_copy(blks, blks, sem).wait()
    pltpu.make_async_copy(tk_s, tk_out, out_sem.at[0]).wait()
    pltpu.make_async_copy(tv_s, tv_out, out_sem.at[1]).wait()
    hid_cp.wait()


def emit_kernel(*refs):
    k = len(refs) // 3
    ins, outs, bufs, sem = refs[:k], refs[k:2 * k], refs[2 * k:3 * k], refs[3 * k]
    loads = [pltpu.make_async_copy(ins[i], bufs[i], sem.at[0, i]) for i in range(k)]
    stores = [pltpu.make_async_copy(bufs[i], outs[i], sem.at[1, i]) for i in range(k)]
    for cp in loads:
        cp.start()
    for ld, st in zip(loads, stores):
        ld.wait()
        st.start()
    for cp in stores:
        cp.wait()


def solution(mesh):
    n = mesh.shape['kv']

    def layer_steps(x_first, next_emb, k_cache, v_cache, seq_len, ln1_gain, ln1_bias, w_q, b_q, w_k, b_k, w_v, b_v, w_o, b_o, ln2_gain, ln2_bias, w_router, w_gate, w_up, w_down, long_factor, expert_idx, route_mask):
        batch, shard, heads_kv, hd = k_cache.shape
        dm = x_first.shape[1]
        q_heads = w_q.shape[1] // hd
        group = q_heads // heads_kv
        steps = next_emb.shape[0] + 1
        n_exp, _, ff = w_gate.shape
        topk = expert_idx.shape[-1]
        rows = steps * batch
        hdk = heads_kv * hd
        n_hp = hdk // LANES
        gs_n = group * steps
        qrows = (gs_n + 1) * heads_kv
        fe = n_exp * ff
        dims = (n, steps, batch, heads_kv, hd, group, shard, n_exp, ff, dm)
        args = (
            x_first, next_emb,
            jnp.transpose(k_cache, (0, 2, 3, 1)).reshape(batch, hdk, shard),
            jnp.transpose(v_cache, (0, 2, 3, 1)).reshape(batch, hdk, shard),
            seq_len, ln1_gain, ln1_bias, w_q, b_q, w_k, b_k, w_v, b_v,
            w_o.reshape(n_hp, 2, group, hd, dm), b_o, ln2_gain, ln2_bias,
            jnp.transpose(w_router),
            jnp.transpose(w_gate, (0, 2, 1)).reshape(fe, dm),
            jnp.transpose(w_up, (0, 2, 1)).reshape(fe, dm),
            w_down.reshape(fe, dm), long_factor,
            jnp.transpose(expert_idx, (0, 2, 1)),
            route_mask.reshape(rows, topk, n_exp),
        )
        any_spec = pl.BlockSpec(memory_space=pl.ANY)
        dma = pltpu.SemaphoreType.DMA
        vm = pltpu.VMEM
        outs = (
            jax.ShapeDtypeStruct((steps, batch, dm), BF16),
            jax.ShapeDtypeStruct((batch, steps, heads_kv, hd), BF16),
            jax.ShapeDtypeStruct((batch, steps, heads_kv, hd), BF16),
        )
        n_quad = batch // (SUBL // 2)
        m_rows = (gs_n + 1) * (SUBL // 2)
        n_ch = dm // hdk
        qblk = vm((n_ch, n_hp, rows // 2, LANES), F32)
        scratch = [
            vm((steps, batch, dm), BF16), pltpu.SMEM((batch,), jnp.int32), pltpu.SMEM((hd // 2,), F32),
            vm((6, dm), F32), vm((hdk,), F32), vm((hdk,), F32), vm((n_exp, dm), BF16),
            vm((steps, topk, batch), jnp.int32), vm((rows, topk, n_exp), jnp.int32),
            vm((n_hp, dm, dm // n_hp), BF16), vm((dm, hdk), BF16), vm((dm, hdk), BF16),
            vm((n_hp, group, 2, hd, dm), BF16), vm((batch, hdk, shard), BF16), vm((batch, hdk, shard), BF16),
            vm((fe, dm), BF16), vm((fe, dm), BF16), vm((fe, dm), BF16),
            vm((n_hp, gs_n, batch, LANES), F32), vm((n_hp, steps, batch, LANES), F32), vm((n_hp, steps, batch, LANES), F32),
            vm((rows, heads_kv, hd), F32), vm((batch, qrows, shard), BF16),
            vm((n_quad, n_hp, m_rows, LANES), F32), vm((n_quad, 2, m_rows, LANES), F32),
            vm((n_quad, 2, SUBL, LANES), F32), vm((n_quad, 2, SUBL, LANES), F32), vm((n_quad, 2, 3, m_rows, LANES), F32), vm((n_quad, m_rows + 2 * SUBL, LANES), F32),
            vm((n_quad, n_hp, 2, 2, m_rows, LANES), F32), vm((group, rows, hdk), F32), vm((2, rows // 2, dm), F32),
            vm((fe // LANES, rows, LANES), F32), vm((fe // LANES, rows, LANES), BF16),
            vm((n_ch, 2, n_hp, rows // 2, LANES), F32), qblk, qblk, qblk, vm((n_ch, n_hp, 2, rows // 2, LANES), F32),
        ] + [vm(o.shape, o.dtype) for o in outs] + [
            dma((14,)), dma((n_hp,)), dma((2,)), dma((1,)), dma((4,)), dma((4,)), dma((2,)), dma((1,)), dma((3,)),
            dma((1,)), dma((n_quad,)), dma((1,)), dma((n_quad,)), dma((2,)), dma((n_quad, n_hp, 2)),
            dma((1,)), dma((n_ch,)), dma((1,)), dma((n_ch, n_hp)), dma((2,)), dma((n_ch, n_hp, 2)),
        ]
        made = pl.pallas_call(
            functools.partial(layer_kernel, dims),
            out_shape=outs,
            in_specs=[any_spec] * len(args),
            out_specs=(any_spec,) * 3,
            scratch_shapes=scratch,
            compiler_params=pltpu.CompilerParams(collective_id=0, has_side_effects=True, vmem_limit_bytes=64 * 1024 * 1024),
        )(*args)
        return pl.pallas_call(
            emit_kernel,
            out_shape=outs,
            in_specs=[any_spec] * 3,
            out_specs=(any_spec,) * 3,
            scratch_shapes=[vm(o.shape, o.dtype) for o in outs] + [dma((2, 3))],
        )(*made)

    replicated = P()
    in_specs = (P('dp'), P(None, 'dp'), P('dp', 'kv'), P('dp', 'kv'), P('dp')) + (replicated,) * 13 + (P(None, None, 'kv'), P(None, None, 'kv'), P(None, 'kv'), replicated, P(None, 'dp'), P(None, 'dp'))
    out_specs = (P(None, 'dp'), P('dp'), P('dp'))
    return jax.shard_map(layer_steps, mesh=mesh, in_specs=in_specs, out_specs=out_specs, check_vma=False)
```

```python
import functools
import math

import jax
import jax.numpy as jnp
from jax import lax
from jax.experimental import pallas as pl
from jax.experimental.pallas import tpu as pltpu
from jax.sharding import PartitionSpec as P

ROPE_BASE = 10000.0
ROPE_MSCALE = math.sqrt(1.0 + math.log(32.0) / math.log(4096.0))
NORM_EPS = 1e-5
NEG_FILL = -1e30
LANES = 128
SUBL = 8
F32 = jnp.float32
BF16 = jnp.bfloat16
NT = (((1,), (1,)), ((), ()))
VMEM_BYTES = 61 * 1024 * 1024


def norm_rows(x, gain, bias):
    mean = jnp.mean(x, axis=-1, keepdims=True)
    cent = x - mean
    var = jnp.mean(cent * cent, axis=-1, keepdims=True)
    return (cent * lax.rsqrt(var + NORM_EPS) * gain + bias).astype(BF16)


def layer_kernel(dims, x_first, next_emb, k_hbm, v_hbm, len_hbm, g1_hbm, b1_hbm, wq_hbm, bq_hbm, wk_hbm, bk_hbm, wv_hbm, bv_hbm, wo_hbm, bo_hbm, g2_hbm, b2_hbm, wr_hbm, wg_hbm, wu_hbm, wd_hbm, lf_hbm, idx_hbm, mask_hbm,
                 hid_out, tk_out, tv_out,
                 x_s, len_s, lf_s, vec_s, bk_s, bv_s, wr_s, idx_s, mask_s,
                 wq_s, wk_s, wv_s, wo_s, k_s, v_s, wg_s, wu_s, wd_s,
                 q_s, kt_s, vt_s, hs_s, p_s, msg_s, pair_s, ml_s, mlp_s, cf_s, tail_s, recv_s, of_s, xm_s, gex_s, u_s, pbuf_s, ppair_s, psum_s, rbuf_s, ybuf_s,
                 small_sem, wq_sem, wkv_sem, wo_sem, k_sem, v_sem, exp_sem, wd_sem,
                 ml_send, ml_recv, pair_send, pair_recv, g_send, g_recv, d_send, d_recv, p_send, p_recv, y_send, y_recv):
    n, steps, batch, heads_kv, hd, group, shard, n_exp, ff, dm = dims
    rows = steps * batch
    gs_n = group * steps
    qrows = (gs_n + 1) * heads_kv
    hdk = heads_kv * hd
    n_hp = hdk // LANES
    me = lax.axis_index('kv')
    chip = me // 2
    core = lax.rem(me, 2)
    other = 1 - core
    partner = chip * 2 + other
    mesh_id = pl.DeviceIdType.MESH

    def remote(src, dst, send, recv, dev):
        return pltpu.make_async_remote_copy(src_ref=src, dst_ref=dst, send_sem=send, recv_sem=recv, device_id={'kv': dev}, device_id_type=mesh_id)

    vecs = (g1_hbm, b1_hbm, bq_hbm, bo_hbm, g2_hbm, b2_hbm)
    smalls = [(x_first, x_s.at[0], 0), (next_emb, x_s.at[pl.ds(1, steps - 1)], 0)]
    smalls += [(len_hbm, len_s, 1), (lf_hbm, lf_s, 2), (bk_hbm, bk_s, 3), (bv_hbm, bv_s, 4), (wr_hbm, wr_s, 5), (idx_hbm, idx_s, 6), (mask_hbm, mask_s, 7)]
    smalls += [(src, vec_s.at[i], 8 + i) for i, src in enumerate(vecs)]
    small_copies = [pltpu.make_async_copy(src, dst, small_sem.at[i]) for src, dst, i in smalls]
    small_waits = [pltpu.make_async_copy(x_s, x_s, small_sem.at[0])] + small_copies[2:]
    qw = wq_s.shape[2]
    wq_copies = [pltpu.make_async_copy(wq_hbm.at[:, pl.ds(i * qw, qw)], wq_s.at[i], wq_sem.at[i]) for i in range(n_hp)]
    wkv_copies = [pltpu.make_async_copy(wk_hbm, wk_s, wkv_sem.at[0]), pltpu.make_async_copy(wv_hbm, wv_s, wkv_sem.at[1])]
    for cp in small_copies + wq_copies + wkv_copies:
        cp.start()

    barrier = pltpu.get_barrier_semaphore()
    for d in range(1, n):
        pl.semaphore_signal(barrier, inc=1, device_id={'kv': lax.rem(me + d, n)}, device_id_type=mesh_id)

    quad = SUBL // 2
    n_quad = batch // quad

    def cache_copy(src, dst, sem, i):
        sl = pl.ds(i * quad, quad)
        return pltpu.make_async_copy(src.at[sl], dst.at[sl], sem.at[i])

    k_copies = [cache_copy(k_hbm, k_s, k_sem, i) for i in range(n_quad)]
    v_copies = [cache_copy(v_hbm, v_s, v_sem, i) for i in range(n_quad)]
    n_ec = wg_s.shape[0] // LANES

    def weight_start(src, dst, sem, parts=4):
        ec = src.shape[0] // parts
        for i in range(parts):
            pltpu.make_async_copy(src.at[pl.ds(i * ec, ec)], dst.at[pl.ds(i * ec, ec)], sem).start()

    def weight_wait(dst, sem):
        pltpu.make_async_copy(dst, dst, sem).wait()

    for cp in small_waits:
        cp.wait()

    g1, b1, bq, bo, g2, b2 = [vec_s[i].reshape(1, dm) for i in range(6)]
    x = x_s[...].reshape(rows, dm).astype(F32)
    h = norm_rows(x, g1, b1)

    lane1 = lax.broadcasted_iota(jnp.int32, (1, LANES), 1)
    half_dim = hd // 2
    jlane = lax.rem(lane1, half_dim)
    lfv = jnp.zeros((1, LANES), F32)
    for j in range(half_dim):
        lfv = jnp.where(jlane == j, lf_s[j], lfv)
    inv = 1.0 / (lfv * jnp.exp(jlane.astype(F32) * (2.0 * math.log(ROPE_BASE) / hd)))
    subb = lax.broadcasted_iota(jnp.int32, (batch, LANES), 0)
    pos = jnp.zeros((batch, LANES), jnp.int32)
    for b in range(batch):
        pos = jnp.where(subb == b, len_s[b], pos)
    ang = jnp.concatenate([(pos + s).astype(F32) * inv for s in range(steps)], axis=0)
    cos = jnp.cos(ang) * ROPE_MSCALE
    sin = jnp.sin(ang) * ROPE_MSCALE
    lane_r = lax.broadcasted_iota(jnp.int32, (rows, LANES), 1)
    sin = jnp.where(lax.rem(lane_r, hd) < half_dim, -sin, sin)
    low_half = lax.rem(lane_r, hd) < half_dim
    low_head = lane_r < hd

    def rope(t):
        t = t.astype(BF16).astype(F32)
        rot = jnp.where(low_half, pltpu.roll(t, LANES - half_dim, 1), pltpu.roll(t, half_dim, 1))
        return (t * cos + rot * sin).astype(BF16).astype(F32)

    def q_block(hp):
        t = jnp.dot(h, wq_s[hp], preferred_element_type=F32) + bq[:, hp * qw:(hp + 1) * qw]
        parts = [rope(t[:, c * LANES:(c + 1) * LANES]) for c in range(qw // LANES)]
        for g in range(group):
            first, second = g, group + g
            a, a_hi = parts[first // 2], first % 2
            c, c_hi = parts[second // 2], second % 2
            a = pltpu.roll(a, hd, 1) if a_hi else a
            c = c if c_hi else pltpu.roll(c, hd, 1)
            q_s[hp, g * steps:(g + 1) * steps] = jnp.where(low_head, a, c).reshape(steps, batch, LANES)

    wq_copies[0].wait()
    for cp in (k_copies[0], k_copies[1], v_copies[0], k_copies[2]):
        cp.start()
    wq_copies[1].wait()
    for hp in range(2):
        q_block(hp)
    for cp in wq_copies[2:] + wkv_copies:
        cp.wait()
    for cp in (v_copies[1], k_copies[3], v_copies[2], v_copies[3]):
        cp.start()
    for hp in range(2, n_hp):
        q_block(hp)
    t = jnp.dot(h, wk_s[...], preferred_element_type=F32) + bk_s[...].reshape(1, hdk)
    for hp in range(n_hp):
        kt_s[hp] = rope(t[:, hp * LANES:(hp + 1) * LANES]).reshape(steps, batch, LANES)
    t = (jnp.dot(h, wv_s[...], preferred_element_type=F32) + bv_s[...].reshape(1, hdk)).astype(BF16).astype(F32)
    for hp in range(n_hp):
        vt_s[hp] = t[:, hp * LANES:(hp + 1) * LANES].reshape(steps, batch, LANES)

    tpos = me * shard + lax.broadcasted_iota(jnp.int32, (1, shard), 1)
    diag = lax.broadcasted_iota(jnp.int32, (heads_kv, hdk), 0) == lax.broadcasted_iota(jnp.int32, (heads_kv, hdk), 1) // hd
    ident = lax.broadcasted_iota(jnp.int32, (qrows, LANES), 0) == lax.broadcasted_iota(jnp.int32, (qrows, LANES), 1)
    o_rows = gs_n * quad
    m_rows = o_rows + quad
    last = o_rows // SUBL * SUBL
    n_tile = last // SUBL + 1
    lane8 = lax.broadcasted_iota(jnp.int32, (SUBL, LANES), 1)
    sub8 = lax.broadcasted_iota(jnp.int32, (SUBL, LANES), 0)
    low8 = lane8 < hd
    low4 = sub8 < quad

    tail_hp = 2 * core + lax.rem(chip, 2)
    tail_q = chip // 2 * 2
    brow = pl.ds(pl.multiple_of(tail_q * quad, SUBL), SUBL)
    for q in range(n_quad):
        tail_s[q, :m_rows] = jnp.zeros((m_rows, LANES), F32)
        tail_s[q, m_rows:m_rows + SUBL] = jnp.full((SUBL, LANES), NEG_FILL, F32)
        tail_s[q, m_rows + SUBL:] = jnp.zeros((SUBL, LANES), F32)
        for hp in range(n_hp):
            msg_s[q, hp, o_rows:] = jnp.zeros((quad, LANES), F32)
    m_tail = jnp.full((SUBL, LANES), NEG_FILL, F32)
    l_tail = jnp.zeros((SUBL, LANES), F32)
    for gs in range(gs_n):
        s = gs % steps
        qt = q_s[tail_hp, gs, brow, :]
        cols = []
        for slot in range(s + 1):
            prod = qt * kt_s[tail_hp, slot, brow, :]
            lo = jnp.sum(jnp.where(low8, prod, 0.0), axis=1, keepdims=True)
            hi = jnp.sum(jnp.where(low8, 0.0, prod), axis=1, keepdims=True)
            cols.append(jnp.where(low8, lo, hi) * (hd ** -0.5))
        mx = functools.reduce(jnp.maximum, cols)
        ws = [jnp.exp(c - mx) for c in cols]
        lsum = functools.reduce(jnp.add, ws)
        acc = functools.reduce(jnp.add, [w.astype(BF16).astype(F32) * vt_s[tail_hp, slot, brow, :] for slot, w in enumerate(ws)])
        for i in range(2):
            tail_s[tail_q + i, gs * quad:(gs + 1) * quad] = acc[i * quad:(i + 1) * quad]
        for j in range(2):
            sel = lane8 == gs * heads_kv + j
            m_tail = jnp.where(sel, mx[:, j * hd:j * hd + 1], m_tail)
            l_tail = jnp.where(sel, lsum[:, j * hd:j * hd + 1], l_tail)
    m_tail = pltpu.roll(m_tail, 2 * tail_hp, 1)
    l_tail = pltpu.roll(l_tail, 2 * tail_hp, 1)
    for i in range(2):
        for k in range(2):
            rs = slice(m_rows + k * quad, m_rows + (k + 1) * quad)
            tail_s[tail_q + i, rs] = m_tail[i * quad:(i + 1) * quad]
            rs = slice(m_rows + SUBL + k * quad, m_rows + SUBL + (k + 1) * quad)
            tail_s[tail_q + i, rs] = l_tail[i * quad:(i + 1) * quad]

    def to_row(col):
        return jnp.sum(jnp.where(ident, col, 0.0), axis=0, keepdims=True)

    def scores(i):
        for j in range(quad):
            b = i * quad + j
            blocks = []
            for gs in range(gs_n):
                qrow = jnp.concatenate([q_s[hp, gs, b:b + 1, :] for hp in range(n_hp)], axis=1)
                blocks.append(jnp.where(diag, qrow, 0.0))
            blocks.append(jnp.zeros((heads_kv, hdk), F32))
            qbd = jnp.concatenate(blocks, axis=0).astype(BF16)
            keep = tpos < len_s[b]
            sc = jnp.dot(qbd, k_s[b], preferred_element_type=F32) * (hd ** -0.5)
            sc = jnp.where(keep, sc, NEG_FILL)
            m = jnp.max(sc, axis=1, keepdims=True)
            w = jnp.where(keep, jnp.exp(sc - m), 0.0)
            p_s[b] = w.astype(BF16)
            mrow, lrow = to_row(m), to_row(jnp.sum(w, axis=1, keepdims=True))
            for k in range(2):
                r = k * quad + j
                ml_s[i, 0, r:r + 1, :] = mrow
                ml_s[i, 1, r:r + 1, :] = lrow

    def outputs(i):
        for j in range(quad):
            b = i * quad + j
            o = lax.dot_general(p_s[b], v_s[b], NT, preferred_element_type=F32)
            for gs in range(gs_n):
                row = jnp.sum(jnp.where(diag, o[gs * heads_kv:(gs + 1) * heads_kv], 0.0), axis=0, keepdims=True)
                for hp in range(n_hp):
                    msg_s[i, hp, gs * quad + j:gs * quad + j + 1, :] = row[:, hp * LANES:(hp + 1) * LANES]

    def spread(t, lane):
        return jnp.where(low8, t[:, lane:lane + 1], t[:, lane + 1:lane + 2])

    def both_halves(t):
        return jnp.where(low4, t, pltpu.roll(t, LANES - heads_kv, 1))

    tiles = [pl.ds(t * SUBL, SUBL) for t in range(n_tile)]

    def ml_copy(q):
        return remote(ml_s.at[q], mlp_s.at[q], ml_send.at[0], ml_recv.at[q], partner)

    def pair_copy(q):
        return remote(msg_s.at[q, pl.ds(2 * other, 2)], pair_s.at[q], pair_send.at[0], pair_recv.at[q], partner)

    def pair_factors(q):
        ms = [ml_s[q, 0], mlp_s[q, 0], tail_s[q, pl.ds(m_rows, SUBL)]]
        ls = [ml_s[q, 1], mlp_s[q, 1], tail_s[q, pl.ds(m_rows + SUBL, SUBL)]]
        mm = functools.reduce(jnp.maximum, ms)
        es = [jnp.exp(m - mm) for m in ms]
        ll = functools.reduce(jnp.add, [e * l for e, l in zip(es, ls)])
        recv_s[q, chip, core, 0, o_rows:] = mm[quad:]
        recv_s[q, chip, core, 1, o_rows:] = ll[quad:]
        es = [both_halves(e) for e in es]
        es[2] = pltpu.roll(es[2], lax.rem(LANES - 2 * tail_hp, LANES), 1)
        for k in range(2):
            shift = lax.rem(LANES - 2 * (2 * core + k), LANES)
            fs = [pltpu.roll(es[0], shift, 1), pltpu.roll(es[1], shift, 1), jnp.where(lax.rem(chip, 2) == k, es[2], 0.0)]
            for i, f in enumerate(fs):
                for t in range(n_tile):
                    cf_s[q, k, i, tiles[t]] = spread(f, t * 2 * heads_kv)

    def pair_merge(q):
        pair_copy(q).wait_recv()
        dst = recv_s.at[q, chip, core]
        for k in range(2):
            rs = pl.ds(0, o_rows)
            dst[k, rs] = cf_s[q, k, 0, rs] * msg_s[q, 2 * core + k, rs] + cf_s[q, k, 1, rs] * pair_s[q, k, rs] + cf_s[q, k, 2, rs] * tail_s[q, rs]
        for dx in (2, 1, 3):
            remote(dst, dst, g_send.at[0], g_recv.at[q, chip, core], lax.rem(chip + dx, n_hp) * 2 + core).start()
        remote(dst, dst, g_send.at[1], g_recv.at[q, chip, core], partner).start()

    def part_arrived(q, cx, c):
        blk = recv_s.at[q, cx, c]
        remote(blk, blk, g_send.at[0], g_recv.at[q, cx, c], me).wait_recv()
        return blk

    def part_relay(q):
        for dx in (1, 3, 2):
            cx = lax.rem(chip + dx, n_hp)
            blk = part_arrived(q, cx, core)
            remote(blk, blk, g_send.at[1], g_recv.at[q, cx, core], partner).start()

    def final_merge(q):
        for dx in (0, 1, 3, 2):
            part_arrived(q, lax.rem(chip + dx, n_hp), other)
        for c in range(2):
            ms = [recv_s[q, cx, c, 0, tiles[-1]] for cx in range(n_hp)]
            mm = functools.reduce(jnp.maximum, ms)
            es = [jnp.exp(m - mm) for m in ms]
            inv_l = 1.0 / functools.reduce(jnp.add, [e * recv_s[q, cx, c, 1, tiles[-1]] for cx, e in enumerate(es)])
            es = [jnp.where(low4, pltpu.roll(e * inv_l, quad, 0), pltpu.roll(e * inv_l, LANES - heads_kv, 1)) for e in es]
            for k in range(2):
                hp = 2 * c + k
                for t in range(n_tile):
                    lane = t * 2 * heads_kv + 2 * hp
                    o = functools.reduce(jnp.add, [spread(e, lane) * recv_s[q, cx, c, k, tiles[t]] for cx, e in enumerate(es)])
                    for i in range(2):
                        gs = 2 * t + i
                        if gs < gs_n:
                            r = gs % steps * batch + q * quad
                            of_s[gs // steps, r:r + quad, hp * LANES:(hp + 1) * LANES] = o[i * quad:(i + 1) * quad]

    for i in range(n_quad + 1):
        if i < n_quad:
            k_copies[i].wait()
        if i:
            v_copies[i - 1].wait()
        if i == n_quad - 1:
            for g in range(group):
                pltpu.make_async_copy(wo_hbm.at[:, :, g], wo_s.at[:, g], wo_sem.at[0]).start()
            weight_start(wg_hbm, wg_s, exp_sem.at[0])
            weight_start(wu_hbm, wu_s, exp_sem.at[1])
            weight_start(wd_hbm, wd_s, wd_sem.at[0])
        if i > 1:
            ml_copy(i - 2).wait_recv()
        if i < n_quad:
            scores(i)
        if i:
            outputs(i - 1)
        if i > 1:
            pair_factors(i - 2)
        if i == 0:
            pl.semaphore_wait(barrier, n - 1)
        if i < n_quad:
            ml_copy(i).start()
        if i:
            pair_copy(i - 1).start()
        if i > 1:
            pair_merge(i - 2)
    ml_copy(n_quad - 1).wait_recv()
    pair_factors(n_quad - 1)
    pair_merge(n_quad - 1)

    part_relay(0)
    for q in range(n_quad):
        if q + 1 < n_quad:
            part_relay(q + 1)
        else:
            weight_wait(wo_s, wo_sem.at[0])
            weight_wait(wg_s, exp_sem.at[0])
            weight_wait(wu_s, exp_sem.at[1])
        final_merge(q)

    lhs = jnp.concatenate([of_s[g, :, hp * LANES:(hp + 1) * LANES] for hp in range(n_hp) for g in range(group)], axis=1).astype(BF16)
    acc = jnp.dot(lhs, wo_s[...].reshape(dm, dm), preferred_element_type=F32)
    x = x_s[...].reshape(rows, dm).astype(F32)
    xm = (x + acc + bo).astype(BF16).astype(F32)
    xm_s[...] = xm.reshape(2, rows // 2, dm)
    h2 = norm_rows(xm, g2, b2)

    logits = lax.dot_general(h2, wr_s[...], NT, preferred_element_type=F32)
    topk = mask_s.shape[1]
    e_iota = lax.broadcasted_iota(jnp.int32, (topk, n_exp), 1)
    grows = []
    for s in range(steps):
        ids = idx_s[s]
        for b in range(batch):
            r = s * batch + b
            lg = jnp.where(mask_s[r] == 1, logits[r:r + 1, :], NEG_FILL)
            ex = jnp.exp(lg - jnp.max(lg, axis=1, keepdims=True))
            pr = ex / jnp.sum(ex, axis=1, keepdims=True)
            grows.append(jnp.sum(jnp.where(ids[:, b:b + 1] == e_iota, pr, 0.0), axis=0, keepdims=True))
    gates = jnp.concatenate(grows, axis=0)
    per = LANES // ff

    def act(c):
        rs = pl.ds(c * LANES, LANES)
        ag = lax.dot_general(h2, wg_s[rs, :], NT, preferred_element_type=F32)
        au = lax.dot_general(h2, wu_s[rs, :], NT, preferred_element_type=F32)
        return ag * (1.0 / (1.0 + jnp.exp(-ag))), au

    peel = n_ec // 4
    for c in range(n_ec):
        gex_s[c] = jnp.where(low_head, gates[:, per * c:per * c + 1], gates[:, per * c + 1:per * c + 2])
    for c in range(peel):
        sg, au = act(c)
        u_s[c] = (gex_s[c] * sg * au).astype(BF16)

    def expert(i, _):
        for j in range(peel):
            c = i * peel + j
            sg, au = act(c)
            u_s[c] = (gex_s[c] * sg * au).astype(BF16)
        return 0

    lax.fori_loop(1, n_ec // peel, expert, 0)
    cw = n_hp * LANES
    n_ch = dm // cw
    hr = rows // 2
    u = jnp.concatenate([u_s[c] for c in range(n_ec)], axis=1)

    def d_copy(k):
        return remote(pbuf_s.at[k, other], ppair_s.at[k], d_send.at[0], d_recv.at[k], partner)

    def add_pair(k):
        d_copy(k).wait_recv()
        psum_s[k] = pbuf_s[k, core] + ppair_s[k]
        for dx in (2, 1, 3):
            cx = lax.rem(chip + dx, n_hp)
            remote(psum_s.at[k, cx], rbuf_s.at[k, chip], p_send.at[0], p_recv.at[k, chip], cx * 2 + core).start()

    weight_wait(wd_s, wd_sem.at[0])
    for k in range(n_ch):
        part = jnp.dot(u, wd_s[:, k * cw:(k + 1) * cw], preferred_element_type=F32)
        part = part.astype(BF16).astype(F32)
        for half in range(2):
            for cx in range(n_hp):
                pbuf_s[k, half, cx] = part[half * hr:(half + 1) * hr, cx * LANES:(cx + 1) * LANES]
        d_copy(k).start()
        if k:
            add_pair(k - 1)
    add_pair(n_ch - 1)

    for src_s, dst in ((kt_s, tk_out), (vt_s, tv_out)):
        for hp in range(n_hp):
            t = src_s[hp].reshape(rows, LANES)
            hs_s[:, 2 * hp, :] = t[:, :hd]
            hs_s[:, 2 * hp + 1, :] = pltpu.roll(t, hd, 1)[:, :hd]
        for s in range(steps):
            dst[:, s] = hs_s[s * batch:(s + 1) * batch].astype(BF16)

    def y_arrived(k, cx, c):
        blk = ybuf_s.at[k, cx, c]
        remote(blk, blk, y_send.at[0], y_recv.at[k, cx, c], me).wait_recv()
        return blk

    for k in range(n_ch):
        y = xm_s[core, :, pl.ds(pl.multiple_of(k * cw + chip * LANES, LANES), LANES)] + psum_s[k, chip]
        for dx in (1, 3, 2):
            cx = lax.rem(chip + dx, n_hp)
            remote(rbuf_s.at[k, cx], rbuf_s.at[k, cx], p_send.at[0], p_recv.at[k, cx], me).wait_recv()
            y = y + rbuf_s[k, cx]
        ybuf_s[k, chip, core] = y.astype(BF16).astype(F32)
        blk = ybuf_s.at[k, chip, core]
        for dx in (2, 1, 3):
            remote(blk, blk, y_send.at[0], y_recv.at[k, chip, core], lax.rem(chip + dx, n_hp) * 2 + core).start()
        remote(blk, blk, y_send.at[1], y_recv.at[k, chip, core], partner).start()
    for k in range(n_ch):
        for dx in (1, 3, 2):
            cx = lax.rem(chip + dx, n_hp)
            blk = y_arrived(k, cx, core)
            remote(blk, blk, y_send.at[1], y_recv.at[k, cx, core], partner).start()
    for k in range(n_ch):
        for dx in (0, 1, 3, 2):
            y_arrived(k, lax.rem(chip + dx, n_hp), other)
        for cx in range(n_hp):
            blk = jnp.concatenate([ybuf_s[k, cx, 0], ybuf_s[k, cx, 1]], axis=0)
            hid_out[:, :, k * cw + cx * LANES:k * cw + (cx + 1) * LANES] = blk.astype(BF16).reshape(steps, batch, LANES)
    one = pl.ds(0, 1)
    part_blocks = pl.ds(0, n_hp - 1)
    for blks, sem in ((mlp_s, ml_send.at[0]), (pair_s, pair_send.at[0]), (recv_s.at[part_blocks, :, one], g_send.at[0]), (recv_s.at[:, :, one], g_send.at[1]),
                      (ppair_s, d_send.at[0]), (rbuf_s.at[:, part_blocks], p_send.at[0]), (ybuf_s.at[:, part_blocks, one], y_send.at[0]), (ybuf_s.at[:, :, one], y_send.at[1])):
        pltpu.make_async_copy(blks, blks, sem).wait()


def emit_kernel(*refs):
    k = len(refs) // 2
    stores = [pltpu.make_async_copy(refs[i], refs[k + i], refs[2 * k].at[i]) for i in range(k)]
    for cp in stores:
        cp.start()
    for cp in stores:
        cp.wait()


def solution(mesh):
    n = mesh.shape['kv']

    def layer_steps(x_first, next_emb, k_cache, v_cache, seq_len, ln1_gain, ln1_bias, w_q, b_q, w_k, b_k, w_v, b_v, w_o, b_o, ln2_gain, ln2_bias, w_router, w_gate, w_up, w_down, long_factor, expert_idx, route_mask):
        batch, shard, heads_kv, hd = k_cache.shape
        dm = x_first.shape[1]
        q_heads = w_q.shape[1] // hd
        group = q_heads // heads_kv
        steps = next_emb.shape[0] + 1
        n_exp, _, ff = w_gate.shape
        topk = expert_idx.shape[-1]
        rows = steps * batch
        hdk = heads_kv * hd
        n_hp = hdk // LANES
        gs_n = group * steps
        qrows = (gs_n + 1) * heads_kv
        fe = n_exp * ff
        dims = (n, steps, batch, heads_kv, hd, group, shard, n_exp, ff, dm)
        args = (
            x_first, next_emb,
            jnp.transpose(k_cache, (0, 2, 3, 1)).reshape(batch, hdk, shard),
            jnp.transpose(v_cache, (0, 2, 3, 1)).reshape(batch, hdk, shard),
            seq_len, ln1_gain, ln1_bias, w_q, b_q, w_k, b_k, w_v, b_v,
            w_o.reshape(n_hp, 2, group, hd, dm), b_o, ln2_gain, ln2_bias,
            jnp.transpose(w_router),
            jnp.transpose(w_gate, (0, 2, 1)).reshape(fe, dm),
            jnp.transpose(w_up, (0, 2, 1)).reshape(fe, dm),
            w_down.reshape(fe, dm), long_factor,
            jnp.transpose(expert_idx, (0, 2, 1)),
            route_mask.reshape(rows, topk, n_exp),
        )
        any_spec = pl.BlockSpec(memory_space=pl.ANY)
        dma = pltpu.SemaphoreType.DMA
        vm = pltpu.VMEM
        outs = (
            jax.ShapeDtypeStruct((steps, batch, dm), BF16),
            jax.ShapeDtypeStruct((batch, steps, heads_kv, hd), BF16),
            jax.ShapeDtypeStruct((batch, steps, heads_kv, hd), BF16),
        )
        n_quad = batch // (SUBL // 2)
        m_rows = (gs_n + 1) * (SUBL // 2)
        n_ch = dm // hdk
        qblk = vm((n_ch, n_hp, rows // 2, LANES), F32)
        scratch = [
            vm((steps, batch, dm), BF16), pltpu.SMEM((batch,), jnp.int32), pltpu.SMEM((hd // 2,), F32),
            vm((6, dm), F32), vm((hdk,), F32), vm((hdk,), F32), vm((n_exp, dm), BF16),
            vm((steps, topk, batch), jnp.int32), vm((rows, topk, n_exp), jnp.int32),
            vm((n_hp, dm, dm // n_hp), BF16), vm((dm, hdk), BF16), vm((dm, hdk), BF16),
            vm((n_hp, group, 2, hd, dm), BF16), vm((batch, hdk, shard), BF16), vm((batch, hdk, shard), BF16),
            vm((fe, dm), BF16), vm((fe, dm), BF16), vm((fe, dm), BF16),
            vm((n_hp, gs_n, batch, LANES), F32), vm((n_hp, steps, batch, LANES), F32), vm((n_hp, steps, batch, LANES), F32),
            vm((rows, heads_kv, hd), F32), vm((batch, qrows, shard), BF16),
            vm((n_quad, n_hp, m_rows, LANES), F32), vm((n_quad, 2, m_rows, LANES), F32),
            vm((n_quad, 2, SUBL, LANES), F32), vm((n_quad, 2, SUBL, LANES), F32), vm((n_quad, 2, 3, m_rows, LANES), F32), vm((n_quad, m_rows + 2 * SUBL, LANES), F32),
            vm((n_quad, n_hp, 2, 2, m_rows, LANES), F32), vm((group, rows, hdk), F32), vm((2, rows // 2, dm), F32),
            vm((fe // LANES, rows, LANES), F32), vm((fe // LANES, rows, LANES), BF16),
            vm((n_ch, 2, n_hp, rows // 2, LANES), F32), qblk, qblk, qblk, vm((n_ch, n_hp, 2, rows // 2, LANES), F32),
            dma((14,)), dma((n_hp,)), dma((2,)), dma((1,)), dma((4,)), dma((4,)), dma((2,)), dma((1,)),
            dma((1,)), dma((n_quad,)), dma((1,)), dma((n_quad,)), dma((2,)), dma((n_quad, n_hp, 2)),
            dma((1,)), dma((n_ch,)), dma((1,)), dma((n_ch, n_hp)), dma((2,)), dma((n_ch, n_hp, 2)),
        ]
        vmem_spec = pl.BlockSpec(memory_space=pltpu.VMEM)
        made = pl.pallas_call(
            functools.partial(layer_kernel, dims),
            out_shape=tuple(vm(o.shape, o.dtype) for o in outs),
            in_specs=[any_spec] * len(args),
            out_specs=(vmem_spec,) * 3,
            scratch_shapes=scratch,
            compiler_params=pltpu.CompilerParams(collective_id=0, has_side_effects=True, vmem_limit_bytes=VMEM_BYTES),
        )(*args)
        made = [pltpu.with_memory_space_constraint(m, pltpu.VMEM) for m in made]
        return pl.pallas_call(
            emit_kernel,
            out_shape=outs,
            in_specs=[any_spec] * 3,
            out_specs=(any_spec,) * 3,
            scratch_shapes=[dma((3,))],
        )(*made)

    replicated = P()
    in_specs = (P('dp'), P(None, 'dp'), P('dp', 'kv'), P('dp', 'kv'), P('dp')) + (replicated,) * 13 + (P(None, None, 'kv'), P(None, None, 'kv'), P(None, 'kv'), replicated, P(None, 'dp'), P(None, 'dp'))
    out_specs = (P(None, 'dp'), P('dp'), P('dp'))
    return jax.shard_map(layer_steps, mesh=mesh, in_specs=in_specs, out_specs=out_specs, check_vma=False)
```

```python
import functools
import math

import jax
import jax.numpy as jnp
from jax import lax
from jax.experimental import pallas as pl
from jax.experimental.pallas import tpu as pltpu
from jax.sharding import PartitionSpec as P

ROPE_BASE = 10000.0
ROPE_MSCALE = math.sqrt(1.0 + math.log(32.0) / math.log(4096.0))
NORM_EPS = 1e-5
NEG_FILL = -1e30
LANES = 128
SUBL = 8
F32 = jnp.float32
BF16 = jnp.bfloat16
NT = (((1,), (1,)), ((), ()))
VMEM_BYTES = 61 * 1024 * 1024


def norm_rows(x, gain, bias):
    mean = jnp.mean(x, axis=-1, keepdims=True)
    cent = x - mean
    var = jnp.mean(cent * cent, axis=-1, keepdims=True)
    return (cent * lax.rsqrt(var + NORM_EPS) * gain + bias).astype(BF16)


def layer_kernel(dims, x_first, next_emb, k_hbm, v_hbm, len_hbm, g1_hbm, b1_hbm, wq_hbm, bq_hbm, wk_hbm, bk_hbm, wv_hbm, bv_hbm, wo_hbm, bo_hbm, g2_hbm, b2_hbm, wr_hbm, wg_hbm, wu_hbm, wd_hbm, lf_hbm, idx_hbm, mask_hbm,
                 hid_out, tk_out, tv_out,
                 x_s, len_s, lf_s, vec_s, bk_s, bv_s, wr_s, idx_s, mask_s,
                 wq_s, wk_s, wv_s, wo_s, k_s, v_s, wg_s, wu_s, wd_s,
                 q_s, kt_s, vt_s, hs_s, p_s, msg_s, pair_s, ml_s, mlp_s, cf_s, tail_s, recv_s, of_s, xm_s, gex_s, u_s, pbuf_s, ppair_s, psum_s, rbuf_s, ybuf_s,
                 small_sem, wq_sem, wkv_sem, wo_sem, k_sem, v_sem, exp_sem, wd_sem,
                 ml_send, ml_recv, pair_send, pair_recv, g_send, g_recv, d_send, d_recv, p_send, p_recv, y_send, y_recv):
    n, steps, batch, heads_kv, hd, group, shard, n_exp, ff, dm = dims
    rows = steps * batch
    gs_n = group * steps
    qrows = (gs_n + 1) * heads_kv
    hdk = heads_kv * hd
    n_hp = hdk // LANES
    me = lax.axis_index('kv')
    chip = me // 2
    core = lax.rem(me, 2)
    other = 1 - core
    partner = chip * 2 + other
    mesh_id = pl.DeviceIdType.MESH

    def remote(src, dst, send, recv, dev):
        return pltpu.make_async_remote_copy(src_ref=src, dst_ref=dst, send_sem=send, recv_sem=recv, device_id={'kv': dev}, device_id_type=mesh_id)

    vecs = (g1_hbm, b1_hbm, bq_hbm, bo_hbm, g2_hbm, b2_hbm)
    smalls = [(x_first, x_s.at[0], 0), (next_emb, x_s.at[pl.ds(1, steps - 1)], 0)]
    smalls += [(len_hbm, len_s, 1), (lf_hbm, lf_s, 2), (bk_hbm, bk_s, 3), (bv_hbm, bv_s, 4), (wr_hbm, wr_s, 5), (idx_hbm, idx_s, 6), (mask_hbm, mask_s, 7)]
    smalls += [(src, vec_s.at[i], 8 + i) for i, src in enumerate(vecs)]
    small_copies = [pltpu.make_async_copy(src, dst, small_sem.at[i]) for src, dst, i in smalls]
    small_waits = [pltpu.make_async_copy(x_s, x_s, small_sem.at[0])] + small_copies[2:]
    qw = wq_s.shape[2]
    wq_copies = [pltpu.make_async_copy(wq_hbm.at[:, pl.ds(i * qw, qw)], wq_s.at[i], wq_sem.at[i]) for i in range(n_hp)]
    wkv_copies = [pltpu.make_async_copy(wk_hbm, wk_s, wkv_sem.at[0]), pltpu.make_async_copy(wv_hbm, wv_s, wkv_sem.at[1])]
    for cp in small_copies + wq_copies + wkv_copies:
        cp.start()

    barrier = pltpu.get_barrier_semaphore()
    for d in range(1, n):
        pl.semaphore_signal(barrier, inc=1, device_id={'kv': lax.rem(me + d, n)}, device_id_type=mesh_id)

    quad = SUBL // 2
    n_quad = batch // quad

    def cache_copy(src, dst, sem, i):
        sl = pl.ds(i * quad, quad)
        return pltpu.make_async_copy(src.at[sl], dst.at[sl], sem.at[i])

    k_copies = [cache_copy(k_hbm, k_s, k_sem, i) for i in range(n_quad)]
    v_copies = [cache_copy(v_hbm, v_s, v_sem, i) for i in range(n_quad)]
    n_ec = wg_s.shape[0] // LANES

    def weight_start(src, dst, sem, parts=4):
        ec = src.shape[0] // parts
        for i in range(parts):
            pltpu.make_async_copy(src.at[pl.ds(i * ec, ec)], dst.at[pl.ds(i * ec, ec)], sem).start()

    def weight_wait(dst, sem):
        pltpu.make_async_copy(dst, dst, sem).wait()

    for cp in small_waits:
        cp.wait()

    g1, b1, bq, bo, g2, b2 = [vec_s[i].reshape(1, dm) for i in range(6)]
    x = x_s[...].reshape(rows, dm).astype(F32)
    h = norm_rows(x, g1, b1)

    lane1 = lax.broadcasted_iota(jnp.int32, (1, LANES), 1)
    half_dim = hd // 2
    jlane = lax.rem(lane1, half_dim)
    lfv = jnp.zeros((1, LANES), F32)
    for j in range(half_dim):
        lfv = jnp.where(jlane == j, lf_s[j], lfv)
    inv = 1.0 / (lfv * jnp.exp(jlane.astype(F32) * (2.0 * math.log(ROPE_BASE) / hd)))
    subb = lax.broadcasted_iota(jnp.int32, (batch, LANES), 0)
    pos = jnp.zeros((batch, LANES), jnp.int32)
    for b in range(batch):
        pos = jnp.where(subb == b, len_s[b], pos)
    ang = jnp.concatenate([(pos + s).astype(F32) * inv for s in range(steps)], axis=0)
    cos = jnp.cos(ang) * ROPE_MSCALE
    sin = jnp.sin(ang) * ROPE_MSCALE
    lane_r = lax.broadcasted_iota(jnp.int32, (rows, LANES), 1)
    sin = jnp.where(lax.rem(lane_r, hd) < half_dim, -sin, sin)
    low_half = lax.rem(lane_r, hd) < half_dim
    low_head = lane_r < hd

    def rope(t):
        t = t.astype(BF16).astype(F32)
        rot = jnp.where(low_half, pltpu.roll(t, LANES - half_dim, 1), pltpu.roll(t, half_dim, 1))
        return (t * cos + rot * sin).astype(BF16).astype(F32)

    def q_block(hp):
        t = jnp.dot(h, wq_s[hp], preferred_element_type=F32) + bq[:, hp * qw:(hp + 1) * qw]
        parts = [rope(t[:, c * LANES:(c + 1) * LANES]) for c in range(qw // LANES)]
        for g in range(group):
            first, second = g, group + g
            a, a_hi = parts[first // 2], first % 2
            c, c_hi = parts[second // 2], second % 2
            a = pltpu.roll(a, hd, 1) if a_hi else a
            c = c if c_hi else pltpu.roll(c, hd, 1)
            q_s[hp, g * steps:(g + 1) * steps] = jnp.where(low_head, a, c).reshape(steps, batch, LANES)

    wq_copies[0].wait()
    for cp in (k_copies[0], k_copies[1], v_copies[0], k_copies[2]):
        cp.start()
    wq_copies[1].wait()
    for hp in range(2):
        q_block(hp)
    for cp in wq_copies[2:] + wkv_copies:
        cp.wait()
    for cp in (v_copies[1], k_copies[3], v_copies[2], v_copies[3]):
        cp.start()
    for hp in range(2, n_hp):
        q_block(hp)
    t = jnp.dot(h, wk_s[...], preferred_element_type=F32) + bk_s[...].reshape(1, hdk)
    for hp in range(n_hp):
        kt_s[hp] = rope(t[:, hp * LANES:(hp + 1) * LANES]).reshape(steps, batch, LANES)
    t = (jnp.dot(h, wv_s[...], preferred_element_type=F32) + bv_s[...].reshape(1, hdk)).astype(BF16).astype(F32)
    for hp in range(n_hp):
        vt_s[hp] = t[:, hp * LANES:(hp + 1) * LANES].reshape(steps, batch, LANES)

    tpos = me * shard + lax.broadcasted_iota(jnp.int32, (1, shard), 1)
    diag = lax.broadcasted_iota(jnp.int32, (heads_kv, hdk), 0) == lax.broadcasted_iota(jnp.int32, (heads_kv, hdk), 1) // hd
    ident = lax.broadcasted_iota(jnp.int32, (qrows, LANES), 0) == lax.broadcasted_iota(jnp.int32, (qrows, LANES), 1)
    o_rows = gs_n * quad
    m_rows = o_rows + quad
    last = o_rows // SUBL * SUBL
    n_tile = last // SUBL + 1
    lane8 = lax.broadcasted_iota(jnp.int32, (SUBL, LANES), 1)
    sub8 = lax.broadcasted_iota(jnp.int32, (SUBL, LANES), 0)
    low8 = lane8 < hd
    low4 = sub8 < quad

    tail_hp = 2 * core + lax.rem(chip, 2)
    tail_q = chip // 2 * 2
    brow = pl.ds(pl.multiple_of(tail_q * quad, SUBL), SUBL)

    def tail_slots():
        for q in range(n_quad):
            tail_s[q, :m_rows] = jnp.zeros((m_rows, LANES), F32)
            tail_s[q, m_rows:m_rows + SUBL] = jnp.full((SUBL, LANES), NEG_FILL, F32)
            tail_s[q, m_rows + SUBL:] = jnp.zeros((SUBL, LANES), F32)
            for hp in range(n_hp):
                msg_s[q, hp, o_rows:] = jnp.zeros((quad, LANES), F32)
        m_tail = jnp.full((SUBL, LANES), NEG_FILL, F32)
        l_tail = jnp.zeros((SUBL, LANES), F32)
        for gs in range(gs_n):
            s = gs % steps
            qt = q_s[tail_hp, gs, brow, :]
            cols = []
            for slot in range(s + 1):
                prod = qt * kt_s[tail_hp, slot, brow, :]
                lo = jnp.sum(jnp.where(low8, prod, 0.0), axis=1, keepdims=True)
                hi = jnp.sum(jnp.where(low8, 0.0, prod), axis=1, keepdims=True)
                cols.append(jnp.where(low8, lo, hi) * (hd ** -0.5))
            mx = functools.reduce(jnp.maximum, cols)
            ws = [jnp.exp(c - mx) for c in cols]
            lsum = functools.reduce(jnp.add, ws)
            acc = functools.reduce(jnp.add, [w.astype(BF16).astype(F32) * vt_s[tail_hp, slot, brow, :] for slot, w in enumerate(ws)])
            for i in range(2):
                tail_s[tail_q + i, gs * quad:(gs + 1) * quad] = acc[i * quad:(i + 1) * quad]
            for j in range(2):
                sel = lane8 == gs * heads_kv + j
                m_tail = jnp.where(sel, mx[:, j * hd:j * hd + 1], m_tail)
                l_tail = jnp.where(sel, lsum[:, j * hd:j * hd + 1], l_tail)
        m_tail = pltpu.roll(m_tail, 2 * tail_hp, 1)
        l_tail = pltpu.roll(l_tail, 2 * tail_hp, 1)
        for i in range(2):
            for k in range(2):
                rs = slice(m_rows + k * quad, m_rows + (k + 1) * quad)
                tail_s[tail_q + i, rs] = m_tail[i * quad:(i + 1) * quad]
                rs = slice(m_rows + SUBL + k * quad, m_rows + SUBL + (k + 1) * quad)
                tail_s[tail_q + i, rs] = l_tail[i * quad:(i + 1) * quad]

    def to_row(col):
        return jnp.sum(jnp.where(ident, col, 0.0), axis=0, keepdims=True)

    def scores(i):
        for j in range(quad):
            b = i * quad + j
            blocks = []
            for gs in range(gs_n):
                qrow = jnp.concatenate([q_s[hp, gs, b:b + 1, :] for hp in range(n_hp)], axis=1)
                blocks.append(jnp.where(diag, qrow, 0.0))
            blocks.append(jnp.zeros((heads_kv, hdk), F32))
            qbd = jnp.concatenate(blocks, axis=0).astype(BF16)
            keep = tpos < len_s[b]
            sc = jnp.dot(qbd, k_s[b], preferred_element_type=F32) * (hd ** -0.5)
            sc = jnp.where(keep, sc, NEG_FILL)
            m = jnp.max(sc, axis=1, keepdims=True)
            w = jnp.where(keep, jnp.exp(sc - m), 0.0)
            p_s[b] = w.astype(BF16)
            mrow, lrow = to_row(m), to_row(jnp.sum(w, axis=1, keepdims=True))
            for k in range(2):
                r = k * quad + j
                ml_s[i, 0, r:r + 1, :] = mrow
                ml_s[i, 1, r:r + 1, :] = lrow

    def outputs(i):
        for j in range(quad):
            b = i * quad + j
            o = lax.dot_general(p_s[b], v_s[b], NT, preferred_element_type=F32)
            for gs in range(gs_n):
                row = jnp.sum(jnp.where(diag, o[gs * heads_kv:(gs + 1) * heads_kv], 0.0), axis=0, keepdims=True)
                for hp in range(n_hp):
                    msg_s[i, hp, gs * quad + j:gs * quad + j + 1, :] = row[:, hp * LANES:(hp + 1) * LANES]

    def spread(t, lane):
        return jnp.where(low8, t[:, lane:lane + 1], t[:, lane + 1:lane + 2])

    def both_halves(t):
        return jnp.where(low4, t, pltpu.roll(t, LANES - heads_kv, 1))

    tiles = [pl.ds(t * SUBL, SUBL) for t in range(n_tile)]

    def ml_copy(q):
        return remote(ml_s.at[q], mlp_s.at[q], ml_send.at[0], ml_recv.at[q], partner)

    def pair_copy(q):
        return remote(msg_s.at[q, pl.ds(2 * other, 2)], pair_s.at[q], pair_send.at[0], pair_recv.at[q], partner)

    def pair_factors(q):
        ms = [ml_s[q, 0], mlp_s[q, 0], tail_s[q, pl.ds(m_rows, SUBL)]]
        ls = [ml_s[q, 1], mlp_s[q, 1], tail_s[q, pl.ds(m_rows + SUBL, SUBL)]]
        mm = functools.reduce(jnp.maximum, ms)
        es = [jnp.exp(m - mm) for m in ms]
        ll = functools.reduce(jnp.add, [e * l for e, l in zip(es, ls)])
        recv_s[q, chip, core, 0, o_rows:] = mm[quad:]
        recv_s[q, chip, core, 1, o_rows:] = ll[quad:]
        es = [both_halves(e) for e in es]
        es[2] = pltpu.roll(es[2], lax.rem(LANES - 2 * tail_hp, LANES), 1)
        for k in range(2):
            shift = lax.rem(LANES - 2 * (2 * core + k), LANES)
            fs = [pltpu.roll(es[0], shift, 1), pltpu.roll(es[1], shift, 1), jnp.where(lax.rem(chip, 2) == k, es[2], 0.0)]
            for i, f in enumerate(fs):
                for t in range(n_tile):
                    cf_s[q, k, i, tiles[t]] = spread(f, t * 2 * heads_kv)

    def pair_merge(q):
        pair_copy(q).wait_recv()
        dst = recv_s.at[q, chip, core]
        for k in range(2):
            rs = pl.ds(0, o_rows)
            dst[k, rs] = cf_s[q, k, 0, rs] * msg_s[q, 2 * core + k, rs] + cf_s[q, k, 1, rs] * pair_s[q, k, rs] + cf_s[q, k, 2, rs] * tail_s[q, rs]
        for dx in (2, 1, 3):
            remote(dst, dst, g_send.at[0], g_recv.at[q, chip, core], lax.rem(chip + dx, n_hp) * 2 + core).start()
        remote(dst, dst, g_send.at[1], g_recv.at[q, chip, core], partner).start()

    def part_arrived(q, cx, c):
        blk = recv_s.at[q, cx, c]
        remote(blk, blk, g_send.at[0], g_recv.at[q, cx, c], me).wait_recv()
        return blk

    def part_relay(q):
        for dx in (1, 3, 2):
            cx = lax.rem(chip + dx, n_hp)
            blk = part_arrived(q, cx, core)
            remote(blk, blk, g_send.at[1], g_recv.at[q, cx, core], partner).start()

    def final_merge(q):
        for dx in (0, 1, 3, 2):
            part_arrived(q, lax.rem(chip + dx, n_hp), other)
        for c in range(2):
            ms = [recv_s[q, cx, c, 0, tiles[-1]] for cx in range(n_hp)]
            mm = functools.reduce(jnp.maximum, ms)
            es = [jnp.exp(m - mm) for m in ms]
            inv_l = 1.0 / functools.reduce(jnp.add, [e * recv_s[q, cx, c, 1, tiles[-1]] for cx, e in enumerate(es)])
            es = [jnp.where(low4, pltpu.roll(e * inv_l, quad, 0), pltpu.roll(e * inv_l, LANES - heads_kv, 1)) for e in es]
            for k in range(2):
                hp = 2 * c + k
                for t in range(n_tile):
                    lane = t * 2 * heads_kv + 2 * hp
                    o = functools.reduce(jnp.add, [spread(e, lane) * recv_s[q, cx, c, k, tiles[t]] for cx, e in enumerate(es)])
                    for i in range(2):
                        gs = 2 * t + i
                        if gs < gs_n:
                            r = gs % steps * batch + q * quad
                            of_s[gs // steps, r:r + quad, hp * LANES:(hp + 1) * LANES] = o[i * quad:(i + 1) * quad]

    for i in range(n_quad + 1):
        if i < n_quad:
            k_copies[i].wait()
        if i:
            v_copies[i - 1].wait()
        if i == n_quad - 1:
            for g in range(group):
                pltpu.make_async_copy(wo_hbm.at[:, :, g], wo_s.at[:, g], wo_sem.at[0]).start()
            weight_start(wg_hbm, wg_s, exp_sem.at[0])
            weight_start(wu_hbm, wu_s, exp_sem.at[1])
            weight_start(wd_hbm, wd_s, wd_sem.at[0])
        if i > 1:
            ml_copy(i - 2).wait_recv()
        if i < n_quad:
            scores(i)
        if i == 1:
            tail_slots()
        if i:
            outputs(i - 1)
        if i > 1:
            pair_factors(i - 2)
        if i == 0:
            pl.semaphore_wait(barrier, n - 1)
        if i < n_quad:
            ml_copy(i).start()
        if i:
            pair_copy(i - 1).start()
        if i > 1:
            pair_merge(i - 2)
    ml_copy(n_quad - 1).wait_recv()
    pair_factors(n_quad - 1)
    pair_merge(n_quad - 1)

    part_relay(0)
    for q in range(n_quad):
        if q + 1 < n_quad:
            part_relay(q + 1)
        else:
            weight_wait(wo_s, wo_sem.at[0])
            weight_wait(wg_s, exp_sem.at[0])
            weight_wait(wu_s, exp_sem.at[1])
        final_merge(q)

    lhs = jnp.concatenate([of_s[g, :, hp * LANES:(hp + 1) * LANES] for hp in range(n_hp) for g in range(group)], axis=1).astype(BF16)
    acc = jnp.dot(lhs, wo_s[...].reshape(dm, dm), preferred_element_type=F32)
    x = x_s[...].reshape(rows, dm).astype(F32)
    xm = (x + acc + bo).astype(BF16).astype(F32)
    xm_s[...] = xm.reshape(2, rows // 2, dm)
    h2 = norm_rows(xm, g2, b2)

    logits = lax.dot_general(h2, wr_s[...], NT, preferred_element_type=F32)
    topk = mask_s.shape[1]
    e_iota = lax.broadcasted_iota(jnp.int32, (topk, n_exp), 1)
    grows = []
    for s in range(steps):
        ids = idx_s[s]
        for b in range(batch):
            r = s * batch + b
            lg = jnp.where(mask_s[r] == 1, logits[r:r + 1, :], NEG_FILL)
            ex = jnp.exp(lg - jnp.max(lg, axis=1, keepdims=True))
            pr = ex / jnp.sum(ex, axis=1, keepdims=True)
            grows.append(jnp.sum(jnp.where(ids[:, b:b + 1] == e_iota, pr, 0.0), axis=0, keepdims=True))
    gates = jnp.concatenate(grows, axis=0)
    per = LANES // ff

    def act(c):
        rs = pl.ds(c * LANES, LANES)
        ag = lax.dot_general(h2, wg_s[rs, :], NT, preferred_element_type=F32)
        au = lax.dot_general(h2, wu_s[rs, :], NT, preferred_element_type=F32)
        return ag * (1.0 / (1.0 + jnp.exp(-ag))), au

    peel = n_ec // 4
    for c in range(n_ec):
        gex_s[c] = jnp.where(low_head, gates[:, per * c:per * c + 1], gates[:, per * c + 1:per * c + 2])
    for c in range(peel):
        sg, au = act(c)
        u_s[c] = (gex_s[c] * sg * au).astype(BF16)

    def expert(i, _):
        for j in range(peel):
            c = i * peel + j
            sg, au = act(c)
            u_s[c] = (gex_s[c] * sg * au).astype(BF16)
        return 0

    lax.fori_loop(1, n_ec // peel, expert, 0)
    cw = n_hp * LANES
    n_ch = dm // cw
    hr = rows // 2
    u = jnp.concatenate([u_s[c] for c in range(n_ec)], axis=1)

    def d_copy(k):
        return remote(pbuf_s.at[k, other], ppair_s.at[k], d_send.at[0], d_recv.at[k], partner)

    def add_pair(k):
        d_copy(k).wait_recv()
        psum_s[k] = pbuf_s[k, core] + ppair_s[k]
        for dx in (2, 1, 3):
            cx = lax.rem(chip + dx, n_hp)
            remote(psum_s.at[k, cx], rbuf_s.at[k, chip], p_send.at[0], p_recv.at[k, chip], cx * 2 + core).start()

    weight_wait(wd_s, wd_sem.at[0])
    for k in range(n_ch):
        part = jnp.dot(u, wd_s[:, k * cw:(k + 1) * cw], preferred_element_type=F32)
        part = part.astype(BF16).astype(F32)
        for half in range(2):
            for cx in range(n_hp):
                pbuf_s[k, half, cx] = part[half * hr:(half + 1) * hr, cx * LANES:(cx + 1) * LANES]
        d_copy(k).start()
        if k:
            add_pair(k - 1)
    add_pair(n_ch - 1)

    for src_s, dst in ((kt_s, tk_out), (vt_s, tv_out)):
        for hp in range(n_hp):
            t = src_s[hp].reshape(rows, LANES)
            hs_s[:, 2 * hp, :] = t[:, :hd]
            hs_s[:, 2 * hp + 1, :] = pltpu.roll(t, hd, 1)[:, :hd]
        for s in range(steps):
            dst[:, s] = hs_s[s * batch:(s + 1) * batch].astype(BF16)

    def y_arrived(k, cx, c):
        blk = ybuf_s.at[k, cx, c]
        remote(blk, blk, y_send.at[0], y_recv.at[k, cx, c], me).wait_recv()
        return blk

    for k in range(n_ch):
        y = xm_s[core, :, pl.ds(pl.multiple_of(k * cw + chip * LANES, LANES), LANES)] + psum_s[k, chip]
        for dx in (1, 3, 2):
            cx = lax.rem(chip + dx, n_hp)
            remote(rbuf_s.at[k, cx], rbuf_s.at[k, cx], p_send.at[0], p_recv.at[k, cx], me).wait_recv()
            y = y + rbuf_s[k, cx]
        ybuf_s[k, chip, core] = y.astype(BF16).astype(F32)
        blk = ybuf_s.at[k, chip, core]
        for dx in (2, 1, 3):
            remote(blk, blk, y_send.at[0], y_recv.at[k, chip, core], lax.rem(chip + dx, n_hp) * 2 + core).start()
        remote(blk, blk, y_send.at[1], y_recv.at[k, chip, core], partner).start()
    for k in range(n_ch):
        for dx in (1, 3, 2):
            cx = lax.rem(chip + dx, n_hp)
            blk = y_arrived(k, cx, core)
            remote(blk, blk, y_send.at[1], y_recv.at[k, cx, core], partner).start()
    for k in range(n_ch):
        for dx in (0, 1, 3, 2):
            y_arrived(k, lax.rem(chip + dx, n_hp), other)
        for cx in range(n_hp):
            blk = jnp.concatenate([ybuf_s[k, cx, 0], ybuf_s[k, cx, 1]], axis=0)
            hid_out[:, :, k * cw + cx * LANES:k * cw + (cx + 1) * LANES] = blk.astype(BF16).reshape(steps, batch, LANES)
    one = pl.ds(0, 1)
    part_blocks = pl.ds(0, n_hp - 1)
    for blks, sem in ((mlp_s, ml_send.at[0]), (pair_s, pair_send.at[0]), (recv_s.at[part_blocks, :, one], g_send.at[0]), (recv_s.at[:, :, one], g_send.at[1]),
                      (ppair_s, d_send.at[0]), (rbuf_s.at[:, part_blocks], p_send.at[0]), (ybuf_s.at[:, part_blocks, one], y_send.at[0]), (ybuf_s.at[:, :, one], y_send.at[1])):
        pltpu.make_async_copy(blks, blks, sem).wait()


def emit_kernel(*refs):
    k = len(refs) // 2
    stores = [pltpu.make_async_copy(refs[i], refs[k + i], refs[2 * k].at[i]) for i in range(k)]
    for cp in stores:
        cp.start()
    for cp in stores:
        cp.wait()


def solution(mesh):
    n = mesh.shape['kv']

    def layer_steps(x_first, next_emb, k_cache, v_cache, seq_len, ln1_gain, ln1_bias, w_q, b_q, w_k, b_k, w_v, b_v, w_o, b_o, ln2_gain, ln2_bias, w_router, w_gate, w_up, w_down, long_factor, expert_idx, route_mask):
        batch, shard, heads_kv, hd = k_cache.shape
        dm = x_first.shape[1]
        q_heads = w_q.shape[1] // hd
        group = q_heads // heads_kv
        steps = next_emb.shape[0] + 1
        n_exp, _, ff = w_gate.shape
        topk = expert_idx.shape[-1]
        rows = steps * batch
        hdk = heads_kv * hd
        n_hp = hdk // LANES
        gs_n = group * steps
        qrows = (gs_n + 1) * heads_kv
        fe = n_exp * ff
        dims = (n, steps, batch, heads_kv, hd, group, shard, n_exp, ff, dm)
        args = (
            x_first, next_emb,
            jnp.transpose(k_cache, (0, 2, 3, 1)).reshape(batch, hdk, shard),
            jnp.transpose(v_cache, (0, 2, 3, 1)).reshape(batch, hdk, shard),
            seq_len, ln1_gain, ln1_bias, w_q, b_q, w_k, b_k, w_v, b_v,
            w_o.reshape(n_hp, 2, group, hd, dm), b_o, ln2_gain, ln2_bias,
            jnp.transpose(w_router),
            jnp.transpose(w_gate, (0, 2, 1)).reshape(fe, dm),
            jnp.transpose(w_up, (0, 2, 1)).reshape(fe, dm),
            w_down.reshape(fe, dm), long_factor,
            jnp.transpose(expert_idx, (0, 2, 1)),
            route_mask.reshape(rows, topk, n_exp),
        )
        any_spec = pl.BlockSpec(memory_space=pl.ANY)
        dma = pltpu.SemaphoreType.DMA
        vm = pltpu.VMEM
        outs = (
            jax.ShapeDtypeStruct((steps, batch, dm), BF16),
            jax.ShapeDtypeStruct((batch, steps, heads_kv, hd), BF16),
            jax.ShapeDtypeStruct((batch, steps, heads_kv, hd), BF16),
        )
        n_quad = batch // (SUBL // 2)
        m_rows = (gs_n + 1) * (SUBL // 2)
        n_ch = dm // hdk
        qblk = vm((n_ch, n_hp, rows // 2, LANES), F32)
        scratch = [
            vm((steps, batch, dm), BF16), pltpu.SMEM((batch,), jnp.int32), pltpu.SMEM((hd // 2,), F32),
            vm((6, dm), F32), vm((hdk,), F32), vm((hdk,), F32), vm((n_exp, dm), BF16),
            vm((steps, topk, batch), jnp.int32), vm((rows, topk, n_exp), jnp.int32),
            vm((n_hp, dm, dm // n_hp), BF16), vm((dm, hdk), BF16), vm((dm, hdk), BF16),
            vm((n_hp, group, 2, hd, dm), BF16), vm((batch, hdk, shard), BF16), vm((batch, hdk, shard), BF16),
            vm((fe, dm), BF16), vm((fe, dm), BF16), vm((fe, dm), BF16),
            vm((n_hp, gs_n, batch, LANES), F32), vm((n_hp, steps, batch, LANES), F32), vm((n_hp, steps, batch, LANES), F32),
            vm((rows, heads_kv, hd), F32), vm((batch, qrows, shard), BF16),
            vm((n_quad, n_hp, m_rows, LANES), F32), vm((n_quad, 2, m_rows, LANES), F32),
            vm((n_quad, 2, SUBL, LANES), F32), vm((n_quad, 2, SUBL, LANES), F32), vm((n_quad, 2, 3, m_rows, LANES), F32), vm((n_quad, m_rows + 2 * SUBL, LANES), F32),
            vm((n_quad, n_hp, 2, 2, m_rows, LANES), F32), vm((group, rows, hdk), F32), vm((2, rows // 2, dm), F32),
            vm((fe // LANES, rows, LANES), F32), vm((fe // LANES, rows, LANES), BF16),
            vm((n_ch, 2, n_hp, rows // 2, LANES), F32), qblk, qblk, qblk, vm((n_ch, n_hp, 2, rows // 2, LANES), F32),
            dma((14,)), dma((n_hp,)), dma((2,)), dma((1,)), dma((4,)), dma((4,)), dma((2,)), dma((1,)),
            dma((1,)), dma((n_quad,)), dma((1,)), dma((n_quad,)), dma((2,)), dma((n_quad, n_hp, 2)),
            dma((1,)), dma((n_ch,)), dma((1,)), dma((n_ch, n_hp)), dma((2,)), dma((n_ch, n_hp, 2)),
        ]
        vmem_spec = pl.BlockSpec(memory_space=pltpu.VMEM)
        made = pl.pallas_call(
            functools.partial(layer_kernel, dims),
            out_shape=tuple(vm(o.shape, o.dtype) for o in outs),
            in_specs=[any_spec] * len(args),
            out_specs=(vmem_spec,) * 3,
            scratch_shapes=scratch,
            compiler_params=pltpu.CompilerParams(collective_id=0, has_side_effects=True, vmem_limit_bytes=VMEM_BYTES),
        )(*args)
        made = [pltpu.with_memory_space_constraint(m, pltpu.VMEM) for m in made]
        return pl.pallas_call(
            emit_kernel,
            out_shape=outs,
            in_specs=[any_spec] * 3,
            out_specs=(any_spec,) * 3,
            scratch_shapes=[dma((3,))],
        )(*made)

    replicated = P()
    in_specs = (P('dp'), P(None, 'dp'), P('dp', 'kv'), P('dp', 'kv'), P('dp')) + (replicated,) * 13 + (P(None, None, 'kv'), P(None, None, 'kv'), P(None, 'kv'), replicated, P(None, 'dp'), P(None, 'dp'))
    out_specs = (P(None, 'dp'), P('dp'), P('dp'))
    return jax.shard_map(layer_steps, mesh=mesh, in_specs=in_specs, out_specs=out_specs, check_vma=False)
```

```python
import functools
import math

import jax
import jax.numpy as jnp
from jax import lax
from jax.experimental import pallas as pl
from jax.experimental.pallas import tpu as pltpu
from jax.sharding import PartitionSpec as P

ROPE_BASE = 10000.0
ROPE_MSCALE = math.sqrt(1.0 + math.log(32.0) / math.log(4096.0))
NORM_EPS = 1e-5
NEG_FILL = -1e30
LANES = 128
SUBL = 8
F32 = jnp.float32
BF16 = jnp.bfloat16
NT = (((1,), (1,)), ((), ()))
VMEM_BYTES = 61 * 1024 * 1024


def norm_rows(x, gain, bias):
    mean = jnp.mean(x, axis=-1, keepdims=True)
    cent = x - mean
    var = jnp.mean(cent * cent, axis=-1, keepdims=True)
    return (cent * lax.rsqrt(var + NORM_EPS) * gain + bias).astype(BF16)


def layer_kernel(dims, x_first, next_emb, k_hbm, v_hbm, len_hbm, g1_hbm, b1_hbm, wq_hbm, bq_hbm, wk_hbm, bk_hbm, wv_hbm, bv_hbm, wo_hbm, bo_hbm, g2_hbm, b2_hbm, wr_hbm, wg_hbm, wu_hbm, wd_hbm, lf_hbm, idx_hbm, mask_hbm,
                 hid_out, tk_out, tv_out,
                 x_s, len_s, lf_s, vec_s, bk_s, bv_s, wr_s, idx_s, mask_s,
                 wq_s, wk_s, wv_s, wo_s, k_s, v_s, wg_s, wu_s, wd_s,
                 q_s, kt_s, vt_s, hs_s, p_s, msg_s, pair_s, ml_s, mlp_s, cf_s, tail_s, recv_s, of_s, xm_s, gex_s, u_s, pbuf_s, ppair_s, psum_s, rbuf_s, ybuf_s,
                 small_sem, wq_sem, wkv_sem, wo_sem, k_sem, v_sem, exp_sem, wd_sem,
                 ml_send, ml_recv, pair_send, pair_recv, g_send, g_recv, d_send, d_recv, p_send, p_recv, y_send, y_recv):
    n, steps, batch, heads_kv, hd, group, shard, n_exp, ff, dm = dims
    rows = steps * batch
    gs_n = group * steps
    qrows = (gs_n + 1) * heads_kv
    hdk = heads_kv * hd
    n_hp = hdk // LANES
    me = lax.axis_index('kv')
    chip = me // 2
    core = lax.rem(me, 2)
    other = 1 - core
    partner = chip * 2 + other
    mesh_id = pl.DeviceIdType.MESH

    def remote(src, dst, send, recv, dev):
        return pltpu.make_async_remote_copy(src_ref=src, dst_ref=dst, send_sem=send, recv_sem=recv, device_id={'kv': dev}, device_id_type=mesh_id)

    vecs = (g1_hbm, b1_hbm, bq_hbm, bo_hbm, g2_hbm, b2_hbm)
    smalls = [(x_first, x_s.at[0], 0), (next_emb, x_s.at[pl.ds(1, steps - 1)], 0)]
    smalls += [(len_hbm, len_s, 1), (lf_hbm, lf_s, 2), (bk_hbm, bk_s, 3), (bv_hbm, bv_s, 4), (wr_hbm, wr_s, 5), (idx_hbm, idx_s, 6), (mask_hbm, mask_s, 7)]
    smalls += [(src, vec_s.at[i], 8 + i) for i, src in enumerate(vecs)]
    small_copies = [pltpu.make_async_copy(src, dst, small_sem.at[i]) for src, dst, i in smalls]
    small_waits = [pltpu.make_async_copy(x_s, x_s, small_sem.at[0])] + small_copies[2:]
    qw = wq_s.shape[2]
    wq_copies = [pltpu.make_async_copy(wq_hbm.at[:, pl.ds(i * qw, qw)], wq_s.at[i], wq_sem.at[i]) for i in range(n_hp)]
    wkv_copies = [pltpu.make_async_copy(wk_hbm, wk_s, wkv_sem.at[0]), pltpu.make_async_copy(wv_hbm, wv_s, wkv_sem.at[1])]
    for cp in small_copies + wq_copies + wkv_copies:
        cp.start()

    barrier = pltpu.get_barrier_semaphore()
    for d in range(1, n):
        pl.semaphore_signal(barrier, inc=1, device_id={'kv': lax.rem(me + d, n)}, device_id_type=mesh_id)

    quad = SUBL // 2
    n_quad = batch // quad

    def cache_copy(src, dst, sem, i):
        sl = pl.ds(i * quad, quad)
        return pltpu.make_async_copy(src.at[sl], dst.at[sl], sem.at[i])

    k_copies = [cache_copy(k_hbm, k_s, k_sem, i) for i in range(n_quad)]
    v_copies = [cache_copy(v_hbm, v_s, v_sem, i) for i in range(n_quad)]
    n_ec = wg_s.shape[0] // LANES

    def weight_start(src, dst, sem, parts=4):
        ec = src.shape[0] // parts
        for i in range(parts):
            pltpu.make_async_copy(src.at[pl.ds(i * ec, ec)], dst.at[pl.ds(i * ec, ec)], sem).start()

    def weight_wait(dst, sem):
        pltpu.make_async_copy(dst, dst, sem).wait()

    for cp in small_waits:
        cp.wait()
    for cp in (k_copies[0], k_copies[1], v_copies[0]):
        cp.start()

    g1, b1, bq, bo, g2, b2 = [vec_s[i].reshape(1, dm) for i in range(6)]
    x = x_s[...].reshape(rows, dm).astype(F32)
    h = norm_rows(x, g1, b1)

    lane1 = lax.broadcasted_iota(jnp.int32, (1, LANES), 1)
    half_dim = hd // 2
    jlane = lax.rem(lane1, half_dim)
    lfv = jnp.zeros((1, LANES), F32)
    for j in range(half_dim):
        lfv = jnp.where(jlane == j, lf_s[j], lfv)
    inv = 1.0 / (lfv * jnp.exp(jlane.astype(F32) * (2.0 * math.log(ROPE_BASE) / hd)))
    subb = lax.broadcasted_iota(jnp.int32, (batch, LANES), 0)
    pos = jnp.zeros((batch, LANES), jnp.int32)
    for b in range(batch):
        pos = jnp.where(subb == b, len_s[b], pos)
    ang = jnp.concatenate([(pos + s).astype(F32) * inv for s in range(steps)], axis=0)
    cos = jnp.cos(ang) * ROPE_MSCALE
    sin = jnp.sin(ang) * ROPE_MSCALE
    lane_r = lax.broadcasted_iota(jnp.int32, (rows, LANES), 1)
    sin = jnp.where(lax.rem(lane_r, hd) < half_dim, -sin, sin)
    low_half = lax.rem(lane_r, hd) < half_dim
    low_head = lane_r < hd

    def rope(t):
        t = t.astype(BF16).astype(F32)
        rot = jnp.where(low_half, pltpu.roll(t, LANES - half_dim, 1), pltpu.roll(t, half_dim, 1))
        return (t * cos + rot * sin).astype(BF16).astype(F32)

    def q_block(hp):
        t = jnp.dot(h, wq_s[hp], preferred_element_type=F32) + bq[:, hp * qw:(hp + 1) * qw]
        parts = [rope(t[:, c * LANES:(c + 1) * LANES]) for c in range(qw // LANES)]
        for g in range(group):
            first, second = g, group + g
            a, a_hi = parts[first // 2], first % 2
            c, c_hi = parts[second // 2], second % 2
            a = pltpu.roll(a, hd, 1) if a_hi else a
            c = c if c_hi else pltpu.roll(c, hd, 1)
            q_s[hp, g * steps:(g + 1) * steps] = jnp.where(low_head, a, c).reshape(steps, batch, LANES)

    for cp in wq_copies[:2]:
        cp.wait()
    for cp in (k_copies[2], v_copies[1]):
        cp.start()
    for hp in range(2):
        q_block(hp)
    for cp in wq_copies[2:] + wkv_copies:
        cp.wait()
    for cp in (k_copies[3], v_copies[2], v_copies[3]):
        cp.start()
    for hp in range(2, n_hp):
        q_block(hp)
    t = jnp.dot(h, wk_s[...], preferred_element_type=F32) + bk_s[...].reshape(1, hdk)
    for hp in range(n_hp):
        kt_s[hp] = rope(t[:, hp * LANES:(hp + 1) * LANES]).reshape(steps, batch, LANES)
    t = (jnp.dot(h, wv_s[...], preferred_element_type=F32) + bv_s[...].reshape(1, hdk)).astype(BF16).astype(F32)
    for hp in range(n_hp):
        vt_s[hp] = t[:, hp * LANES:(hp + 1) * LANES].reshape(steps, batch, LANES)

    tpos = me * shard + lax.broadcasted_iota(jnp.int32, (1, shard), 1)
    diag = lax.broadcasted_iota(jnp.int32, (heads_kv, hdk), 0) == lax.broadcasted_iota(jnp.int32, (heads_kv, hdk), 1) // hd
    ident = lax.broadcasted_iota(jnp.int32, (qrows, LANES), 0) == lax.broadcasted_iota(jnp.int32, (qrows, LANES), 1)
    o_rows = gs_n * quad
    m_rows = o_rows + quad
    last = o_rows // SUBL * SUBL
    n_tile = last // SUBL + 1
    lane8 = lax.broadcasted_iota(jnp.int32, (SUBL, LANES), 1)
    sub8 = lax.broadcasted_iota(jnp.int32, (SUBL, LANES), 0)
    low8 = lane8 < hd
    low4 = sub8 < quad

    tail_hp = 2 * core + lax.rem(chip, 2)
    tail_q = chip // 2 * 2
    brow = pl.ds(pl.multiple_of(tail_q * quad, SUBL), SUBL)

    def tail_slots():
        for q in range(n_quad):
            tail_s[q, :m_rows] = jnp.zeros((m_rows, LANES), F32)
            tail_s[q, m_rows:m_rows + SUBL] = jnp.full((SUBL, LANES), NEG_FILL, F32)
            tail_s[q, m_rows + SUBL:] = jnp.zeros((SUBL, LANES), F32)
            for hp in range(n_hp):
                msg_s[q, hp, o_rows:] = jnp.zeros((quad, LANES), F32)
        m_tail = jnp.full((SUBL, LANES), NEG_FILL, F32)
        l_tail = jnp.zeros((SUBL, LANES), F32)
        for gs in range(gs_n):
            s = gs % steps
            qt = q_s[tail_hp, gs, brow, :]
            cols = []
            for slot in range(s + 1):
                prod = qt * kt_s[tail_hp, slot, brow, :]
                lo = jnp.sum(jnp.where(low8, prod, 0.0), axis=1, keepdims=True)
                hi = jnp.sum(jnp.where(low8, 0.0, prod), axis=1, keepdims=True)
                cols.append(jnp.where(low8, lo, hi) * (hd ** -0.5))
            mx = functools.reduce(jnp.maximum, cols)
            ws = [jnp.exp(c - mx) for c in cols]
            lsum = functools.reduce(jnp.add, ws)
            acc = functools.reduce(jnp.add, [w.astype(BF16).astype(F32) * vt_s[tail_hp, slot, brow, :] for slot, w in enumerate(ws)])
            for i in range(2):
                tail_s[tail_q + i, gs * quad:(gs + 1) * quad] = acc[i * quad:(i + 1) * quad]
            for j in range(2):
                sel = lane8 == gs * heads_kv + j
                m_tail = jnp.where(sel, mx[:, j * hd:j * hd + 1], m_tail)
                l_tail = jnp.where(sel, lsum[:, j * hd:j * hd + 1], l_tail)
        m_tail = pltpu.roll(m_tail, 2 * tail_hp, 1)
        l_tail = pltpu.roll(l_tail, 2 * tail_hp, 1)
        for i in range(2):
            for k in range(2):
                rs = slice(m_rows + k * quad, m_rows + (k + 1) * quad)
                tail_s[tail_q + i, rs] = m_tail[i * quad:(i + 1) * quad]
                rs = slice(m_rows + SUBL + k * quad, m_rows + SUBL + (k + 1) * quad)
                tail_s[tail_q + i, rs] = l_tail[i * quad:(i + 1) * quad]

    def to_row(col):
        return jnp.sum(jnp.where(ident, col, 0.0), axis=0, keepdims=True)

    def scores(i):
        for j in range(quad):
            b = i * quad + j
            blocks = []
            for gs in range(gs_n):
                qrow = jnp.concatenate([q_s[hp, gs, b:b + 1, :] for hp in range(n_hp)], axis=1)
                blocks.append(jnp.where(diag, qrow, 0.0))
            blocks.append(jnp.zeros((heads_kv, hdk), F32))
            qbd = jnp.concatenate(blocks, axis=0).astype(BF16)
            keep = tpos < len_s[b]
            sc = jnp.dot(qbd, k_s[b], preferred_element_type=F32) * (hd ** -0.5)
            sc = jnp.where(keep, sc, NEG_FILL)
            m = jnp.max(sc, axis=1, keepdims=True)
            w = jnp.where(keep, jnp.exp(sc - m), 0.0)
            p_s[b] = w.astype(BF16)
            mrow, lrow = to_row(m), to_row(jnp.sum(w, axis=1, keepdims=True))
            for k in range(2):
                r = k * quad + j
                ml_s[i, 0, r:r + 1, :] = mrow
                ml_s[i, 1, r:r + 1, :] = lrow

    def outputs(i):
        for j in range(quad):
            b = i * quad + j
            o = lax.dot_general(p_s[b], v_s[b], NT, preferred_element_type=F32)
            for gs in range(gs_n):
                row = jnp.sum(jnp.where(diag, o[gs * heads_kv:(gs + 1) * heads_kv], 0.0), axis=0, keepdims=True)
                for hp in range(n_hp):
                    msg_s[i, hp, gs * quad + j:gs * quad + j + 1, :] = row[:, hp * LANES:(hp + 1) * LANES]

    def spread(t, lane):
        return jnp.where(low8, t[:, lane:lane + 1], t[:, lane + 1:lane + 2])

    def both_halves(t):
        return jnp.where(low4, t, pltpu.roll(t, LANES - heads_kv, 1))

    tiles = [pl.ds(t * SUBL, SUBL) for t in range(n_tile)]

    def ml_copy(q):
        return remote(ml_s.at[q], mlp_s.at[q], ml_send.at[0], ml_recv.at[q], partner)

    def pair_copy(q):
        return remote(msg_s.at[q, pl.ds(2 * other, 2)], pair_s.at[q], pair_send.at[0], pair_recv.at[q], partner)

    def pair_factors(q):
        ms = [ml_s[q, 0], mlp_s[q, 0], tail_s[q, pl.ds(m_rows, SUBL)]]
        ls = [ml_s[q, 1], mlp_s[q, 1], tail_s[q, pl.ds(m_rows + SUBL, SUBL)]]
        mm = functools.reduce(jnp.maximum, ms)
        es = [jnp.exp(m - mm) for m in ms]
        ll = functools.reduce(jnp.add, [e * l for e, l in zip(es, ls)])
        recv_s[q, chip, core, 0, o_rows:] = mm[quad:]
        recv_s[q, chip, core, 1, o_rows:] = ll[quad:]
        es = [both_halves(e) for e in es]
        es[2] = pltpu.roll(es[2], lax.rem(LANES - 2 * tail_hp, LANES), 1)
        for k in range(2):
            shift = lax.rem(LANES - 2 * (2 * core + k), LANES)
            fs = [pltpu.roll(es[0], shift, 1), pltpu.roll(es[1], shift, 1), jnp.where(lax.rem(chip, 2) == k, es[2], 0.0)]
            for i, f in enumerate(fs):
                for t in range(n_tile):
                    cf_s[q, k, i, tiles[t]] = spread(f, t * 2 * heads_kv)

    def pair_merge(q):
        pair_copy(q).wait_recv()
        dst = recv_s.at[q, chip, core]
        for k in range(2):
            rs = pl.ds(0, o_rows)
            dst[k, rs] = cf_s[q, k, 0, rs] * msg_s[q, 2 * core + k, rs] + cf_s[q, k, 1, rs] * pair_s[q, k, rs] + cf_s[q, k, 2, rs] * tail_s[q, rs]
        for dx in (2, 1, 3):
            remote(dst, dst, g_send.at[0], g_recv.at[q, chip, core], lax.rem(chip + dx, n_hp) * 2 + core).start()
        remote(dst, dst, g_send.at[1], g_recv.at[q, chip, core], partner).start()

    def part_arrived(q, cx, c):
        blk = recv_s.at[q, cx, c]
        remote(blk, blk, g_send.at[0], g_recv.at[q, cx, c], me).wait_recv()
        return blk

    def part_relay(q):
        for dx in (1, 3, 2):
            cx = lax.rem(chip + dx, n_hp)
            blk = part_arrived(q, cx, core)
            remote(blk, blk, g_send.at[1], g_recv.at[q, cx, core], partner).start()

    def final_merge(q):
        for dx in (0, 1, 3, 2):
            part_arrived(q, lax.rem(chip + dx, n_hp), other)
        for c in range(2):
            ms = [recv_s[q, cx, c, 0, tiles[-1]] for cx in range(n_hp)]
            mm = functools.reduce(jnp.maximum, ms)
            es = [jnp.exp(m - mm) for m in ms]
            inv_l = 1.0 / functools.reduce(jnp.add, [e * recv_s[q, cx, c, 1, tiles[-1]] for cx, e in enumerate(es)])
            es = [jnp.where(low4, pltpu.roll(e * inv_l, quad, 0), pltpu.roll(e * inv_l, LANES - heads_kv, 1)) for e in es]
            for k in range(2):
                hp = 2 * c + k
                for t in range(n_tile):
                    lane = t * 2 * heads_kv + 2 * hp
                    o = functools.reduce(jnp.add, [spread(e, lane) * recv_s[q, cx, c, k, tiles[t]] for cx, e in enumerate(es)])
                    for i in range(2):
                        gs = 2 * t + i
                        if gs < gs_n:
                            r = gs % steps * batch + q * quad
                            of_s[gs // steps, r:r + quad, hp * LANES:(hp + 1) * LANES] = o[i * quad:(i + 1) * quad]

    for i in range(n_quad + 1):
        if i < n_quad:
            k_copies[i].wait()
        if i:
            v_copies[i - 1].wait()
        if i == n_quad - 1:
            for g in range(group):
                pltpu.make_async_copy(wo_hbm.at[:, :, g], wo_s.at[:, g], wo_sem.at[0]).start()
            weight_start(wg_hbm, wg_s, exp_sem.at[0])
            weight_start(wu_hbm, wu_s, exp_sem.at[1])
            weight_start(wd_hbm, wd_s, wd_sem.at[0])
        if i > 1:
            ml_copy(i - 2).wait_recv()
        if i < n_quad:
            scores(i)
        if i == 1:
            tail_slots()
        if i:
            outputs(i - 1)
        if i > 1:
            pair_factors(i - 2)
        if i == 0:
            pl.semaphore_wait(barrier, n - 1)
        if i < n_quad:
            ml_copy(i).start()
        if i:
            pair_copy(i - 1).start()
        if i > 1:
            pair_merge(i - 2)
    ml_copy(n_quad - 1).wait_recv()
    pair_factors(n_quad - 1)
    pair_merge(n_quad - 1)

    part_relay(0)
    for q in range(n_quad):
        if q + 1 < n_quad:
            part_relay(q + 1)
        else:
            weight_wait(wo_s, wo_sem.at[0])
            weight_wait(wg_s, exp_sem.at[0])
            weight_wait(wu_s, exp_sem.at[1])
        final_merge(q)

    lhs = jnp.concatenate([of_s[g, :, hp * LANES:(hp + 1) * LANES] for hp in range(n_hp) for g in range(group)], axis=1).astype(BF16)
    acc = jnp.dot(lhs, wo_s[...].reshape(dm, dm), preferred_element_type=F32)
    x = x_s[...].reshape(rows, dm).astype(F32)
    xm = (x + acc + bo).astype(BF16).astype(F32)
    xm_s[...] = xm.reshape(2, rows // 2, dm)
    h2 = norm_rows(xm, g2, b2)

    logits = lax.dot_general(h2, wr_s[...], NT, preferred_element_type=F32)
    topk = mask_s.shape[1]
    e_iota = lax.broadcasted_iota(jnp.int32, (topk, n_exp), 1)
    grows = []
    for s in range(steps):
        ids = idx_s[s]
        for b in range(batch):
            r = s * batch + b
            lg = jnp.where(mask_s[r] == 1, logits[r:r + 1, :], NEG_FILL)
            ex = jnp.exp(lg - jnp.max(lg, axis=1, keepdims=True))
            pr = ex / jnp.sum(ex, axis=1, keepdims=True)
            grows.append(jnp.sum(jnp.where(ids[:, b:b + 1] == e_iota, pr, 0.0), axis=0, keepdims=True))
    gates = jnp.concatenate(grows, axis=0)
    per = LANES // ff

    def act(c):
        rs = pl.ds(c * LANES, LANES)
        ag = lax.dot_general(h2, wg_s[rs, :], NT, preferred_element_type=F32)
        au = lax.dot_general(h2, wu_s[rs, :], NT, preferred_element_type=F32)
        return ag * (1.0 / (1.0 + jnp.exp(-ag))), au

    for c in range(n_ec):
        gex_s[c] = jnp.where(low_head, gates[:, per * c:per * c + 1], gates[:, per * c + 1:per * c + 2])
    for c in range(n_ec):
        sg, au = act(c)
        u_s[c] = (gex_s[c] * sg * au).astype(BF16)

    cw = n_hp * LANES
    n_ch = dm // cw
    hr = rows // 2
    u = jnp.concatenate([u_s[c] for c in range(n_ec)], axis=1)

    def d_copy(k):
        return remote(pbuf_s.at[k, other], ppair_s.at[k], d_send.at[0], d_recv.at[k], partner)

    def add_pair(k):
        d_copy(k).wait_recv()
        psum_s[k] = pbuf_s[k, core] + ppair_s[k]
        for dx in (2, 1, 3):
            cx = lax.rem(chip + dx, n_hp)
            remote(psum_s.at[k, cx], rbuf_s.at[k, chip], p_send.at[0], p_recv.at[k, chip], cx * 2 + core).start()

    weight_wait(wd_s, wd_sem.at[0])
    for k in range(n_ch):
        part = jnp.dot(u, wd_s[:, k * cw:(k + 1) * cw], preferred_element_type=F32)
        part = part.astype(BF16).astype(F32)
        for half in range(2):
            for cx in range(n_hp):
                pbuf_s[k, half, cx] = part[half * hr:(half + 1) * hr, cx * LANES:(cx + 1) * LANES]
        d_copy(k).start()
        if k:
            add_pair(k - 1)
    add_pair(n_ch - 1)

    for src_s, dst in ((kt_s, tk_out), (vt_s, tv_out)):
        for hp in range(n_hp):
            t = src_s[hp].reshape(rows, LANES)
            hs_s[:, 2 * hp, :] = t[:, :hd]
            hs_s[:, 2 * hp + 1, :] = pltpu.roll(t, hd, 1)[:, :hd]
        for s in range(steps):
            dst[:, s] = hs_s[s * batch:(s + 1) * batch].astype(BF16)

    def y_arrived(k, cx, c):
        blk = ybuf_s.at[k, cx, c]
        remote(blk, blk, y_send.at[0], y_recv.at[k, cx, c], me).wait_recv()
        return blk

    for k in range(n_ch):
        y = xm_s[core, :, pl.ds(pl.multiple_of(k * cw + chip * LANES, LANES), LANES)] + psum_s[k, chip]
        for dx in (1, 3, 2):
            cx = lax.rem(chip + dx, n_hp)
            remote(rbuf_s.at[k, cx], rbuf_s.at[k, cx], p_send.at[0], p_recv.at[k, cx], me).wait_recv()
            y = y + rbuf_s[k, cx]
        ybuf_s[k, chip, core] = y.astype(BF16).astype(F32)
        blk = ybuf_s.at[k, chip, core]
        for dx in (2, 1, 3):
            remote(blk, blk, y_send.at[0], y_recv.at[k, chip, core], lax.rem(chip + dx, n_hp) * 2 + core).start()
        remote(blk, blk, y_send.at[1], y_recv.at[k, chip, core], partner).start()
    for k in range(n_ch):
        for dx in (1, 3, 2):
            cx = lax.rem(chip + dx, n_hp)
            blk = y_arrived(k, cx, core)
            remote(blk, blk, y_send.at[1], y_recv.at[k, cx, core], partner).start()
    for k in range(n_ch):
        for dx in (0, 1, 3, 2):
            y_arrived(k, lax.rem(chip + dx, n_hp), other)
        for cx in range(n_hp):
            blk = jnp.concatenate([ybuf_s[k, cx, 0], ybuf_s[k, cx, 1]], axis=0)
            hid_out[:, :, k * cw + cx * LANES:k * cw + (cx + 1) * LANES] = blk.astype(BF16).reshape(steps, batch, LANES)
    one = pl.ds(0, 1)
    part_blocks = pl.ds(0, n_hp - 1)
    for blks, sem in ((mlp_s, ml_send.at[0]), (pair_s, pair_send.at[0]), (recv_s.at[part_blocks, :, one], g_send.at[0]), (recv_s.at[:, :, one], g_send.at[1]),
                      (ppair_s, d_send.at[0]), (rbuf_s.at[:, part_blocks], p_send.at[0]), (ybuf_s.at[:, part_blocks, one], y_send.at[0]), (ybuf_s.at[:, :, one], y_send.at[1])):
        pltpu.make_async_copy(blks, blks, sem).wait()


def emit_kernel(*refs):
    k = len(refs) // 2
    stores = [pltpu.make_async_copy(refs[i], refs[k + i], refs[2 * k].at[i]) for i in range(k)]
    for cp in stores:
        cp.start()
    for cp in stores:
        cp.wait()


def solution(mesh):
    n = mesh.shape['kv']

    def layer_steps(x_first, next_emb, k_cache, v_cache, seq_len, ln1_gain, ln1_bias, w_q, b_q, w_k, b_k, w_v, b_v, w_o, b_o, ln2_gain, ln2_bias, w_router, w_gate, w_up, w_down, long_factor, expert_idx, route_mask):
        batch, shard, heads_kv, hd = k_cache.shape
        dm = x_first.shape[1]
        q_heads = w_q.shape[1] // hd
        group = q_heads // heads_kv
        steps = next_emb.shape[0] + 1
        n_exp, _, ff = w_gate.shape
        topk = expert_idx.shape[-1]
        rows = steps * batch
        hdk = heads_kv * hd
        n_hp = hdk // LANES
        gs_n = group * steps
        qrows = (gs_n + 1) * heads_kv
        fe = n_exp * ff
        dims = (n, steps, batch, heads_kv, hd, group, shard, n_exp, ff, dm)
        args = (
            x_first, next_emb,
            jnp.transpose(k_cache, (0, 2, 3, 1)).reshape(batch, hdk, shard),
            jnp.transpose(v_cache, (0, 2, 3, 1)).reshape(batch, hdk, shard),
            seq_len, ln1_gain, ln1_bias, w_q, b_q, w_k, b_k, w_v, b_v,
            w_o.reshape(n_hp, 2, group, hd, dm), b_o, ln2_gain, ln2_bias,
            jnp.transpose(w_router),
            jnp.transpose(w_gate, (0, 2, 1)).reshape(fe, dm),
            jnp.transpose(w_up, (0, 2, 1)).reshape(fe, dm),
            w_down.reshape(fe, dm), long_factor,
            jnp.transpose(expert_idx, (0, 2, 1)),
            route_mask.reshape(rows, topk, n_exp),
        )
        any_spec = pl.BlockSpec(memory_space=pl.ANY)
        dma = pltpu.SemaphoreType.DMA
        vm = pltpu.VMEM
        outs = (
            jax.ShapeDtypeStruct((steps, batch, dm), BF16),
            jax.ShapeDtypeStruct((batch, steps, heads_kv, hd), BF16),
            jax.ShapeDtypeStruct((batch, steps, heads_kv, hd), BF16),
        )
        n_quad = batch // (SUBL // 2)
        m_rows = (gs_n + 1) * (SUBL // 2)
        n_ch = dm // hdk
        qblk = vm((n_ch, n_hp, rows // 2, LANES), F32)
        scratch = [
            vm((steps, batch, dm), BF16), pltpu.SMEM((batch,), jnp.int32), pltpu.SMEM((hd // 2,), F32),
            vm((6, dm), F32), vm((hdk,), F32), vm((hdk,), F32), vm((n_exp, dm), BF16),
            vm((steps, topk, batch), jnp.int32), vm((rows, topk, n_exp), jnp.int32),
            vm((n_hp, dm, dm // n_hp), BF16), vm((dm, hdk), BF16), vm((dm, hdk), BF16),
            vm((n_hp, group, 2, hd, dm), BF16), vm((batch, hdk, shard), BF16), vm((batch, hdk, shard), BF16),
            vm((fe, dm), BF16), vm((fe, dm), BF16), vm((fe, dm), BF16),
            vm((n_hp, gs_n, batch, LANES), F32), vm((n_hp, steps, batch, LANES), F32), vm((n_hp, steps, batch, LANES), F32),
            vm((rows, heads_kv, hd), F32), vm((batch, qrows, shard), BF16),
            vm((n_quad, n_hp, m_rows, LANES), F32), vm((n_quad, 2, m_rows, LANES), F32),
            vm((n_quad, 2, SUBL, LANES), F32), vm((n_quad, 2, SUBL, LANES), F32), vm((n_quad, 2, 3, m_rows, LANES), F32), vm((n_quad, m_rows + 2 * SUBL, LANES), F32),
            vm((n_quad, n_hp, 2, 2, m_rows, LANES), F32), vm((group, rows, hdk), F32), vm((2, rows // 2, dm), F32),
            vm((fe // LANES, rows, LANES), F32), vm((fe // LANES, rows, LANES), BF16),
            vm((n_ch, 2, n_hp, rows // 2, LANES), F32), qblk, qblk, qblk, vm((n_ch, n_hp, 2, rows // 2, LANES), F32),
            dma((14,)), dma((n_hp,)), dma((2,)), dma((1,)), dma((4,)), dma((4,)), dma((2,)), dma((1,)),
            dma((1,)), dma((n_quad,)), dma((1,)), dma((n_quad,)), dma((2,)), dma((n_quad, n_hp, 2)),
            dma((1,)), dma((n_ch,)), dma((1,)), dma((n_ch, n_hp)), dma((2,)), dma((n_ch, n_hp, 2)),
        ]
        vmem_spec = pl.BlockSpec(memory_space=pltpu.VMEM)
        made = pl.pallas_call(
            functools.partial(layer_kernel, dims),
            out_shape=tuple(vm(o.shape, o.dtype) for o in outs),
            in_specs=[any_spec] * len(args),
            out_specs=(vmem_spec,) * 3,
            scratch_shapes=scratch,
            compiler_params=pltpu.CompilerParams(collective_id=0, has_side_effects=True, vmem_limit_bytes=VMEM_BYTES),
        )(*args)
        made = [pltpu.with_memory_space_constraint(m, pltpu.VMEM) for m in made]
        return pl.pallas_call(
            emit_kernel,
            out_shape=outs,
            in_specs=[any_spec] * 3,
            out_specs=(any_spec,) * 3,
            scratch_shapes=[dma((3,))],
        )(*made)

    replicated = P()
    in_specs = (P('dp'), P(None, 'dp'), P('dp', 'kv'), P('dp', 'kv'), P('dp')) + (replicated,) * 13 + (P(None, None, 'kv'), P(None, None, 'kv'), P(None, 'kv'), replicated, P(None, 'dp'), P(None, 'dp'))
    out_specs = (P(None, 'dp'), P('dp'), P('dp'))
    return jax.shard_map(layer_steps, mesh=mesh, in_specs=in_specs, out_specs=out_specs, check_vma=False)
```

```python
import functools
import math

import jax
import jax.numpy as jnp
from jax import lax
from jax.experimental import pallas as pl
from jax.experimental.pallas import tpu as pltpu
from jax.sharding import PartitionSpec as P

ROPE_BASE = 10000.0
ROPE_MSCALE = math.sqrt(1.0 + math.log(32.0) / math.log(4096.0))
NORM_EPS = 1e-5
NEG_FILL = -1e30
LANES = 128
SUBL = 8
F32 = jnp.float32
BF16 = jnp.bfloat16
NT = (((1,), (1,)), ((), ()))
VMEM_BYTES = 61 * 1024 * 1024


def norm_rows(x, gain, bias):
    mean = jnp.mean(x, axis=-1, keepdims=True)
    cent = x - mean
    var = jnp.mean(cent * cent, axis=-1, keepdims=True)
    return (cent * lax.rsqrt(var + NORM_EPS) * gain + bias).astype(BF16)


def layer_kernel(dims, x_first, next_emb, k_hbm, v_hbm, len_hbm, g1_hbm, b1_hbm, wq_hbm, bq_hbm, wk_hbm, bk_hbm, wv_hbm, bv_hbm, wo_hbm, bo_hbm, g2_hbm, b2_hbm, wr_hbm, wg_hbm, wu_hbm, wd_hbm, lf_hbm, idx_hbm, mask_hbm,
                 hid_out, tk_out, tv_out,
                 x_s, len_s, lf_s, vec_s, bk_s, bv_s, wr_s, idx_s, mask_s,
                 wq_s, wk_s, wv_s, wo_s, k_s, v_s, wg_s, wu_s, wd_s,
                 q_s, kt_s, vt_s, hs_s, p_s, msg_s, pair_s, ml_s, mlp_s, cf_s, tail_s, recv_s, of_s, xm_s, gex_s, u_s, pbuf_s, ppair_s, psum_s, rbuf_s, ybuf_s,
                 small_sem, wq_sem, wkv_sem, wo_sem, k_sem, v_sem, exp_sem, wd_sem,
                 ml_send, ml_recv, pair_send, pair_recv, g_send, g_recv, d_send, d_recv, p_send, p_recv, y_send):
    n, steps, batch, heads_kv, hd, group, shard, n_exp, ff, dm = dims
    rows = steps * batch
    gs_n = group * steps
    qrows = (gs_n + 1) * heads_kv
    hdk = heads_kv * hd
    n_hp = hdk // LANES
    me = lax.axis_index('kv')
    chip = me // 2
    core = lax.rem(me, 2)
    other = 1 - core
    partner = chip * 2 + other
    mesh_id = pl.DeviceIdType.MESH

    def remote(src, dst, send, recv, dev):
        return pltpu.make_async_remote_copy(src_ref=src, dst_ref=dst, send_sem=send, recv_sem=recv, device_id={'kv': dev}, device_id_type=mesh_id)

    vecs = (g1_hbm, b1_hbm, bq_hbm, bo_hbm, g2_hbm, b2_hbm)
    smalls = [(x_first, x_s.at[0], 0), (next_emb, x_s.at[pl.ds(1, steps - 1)], 0)]
    smalls += [(len_hbm, len_s, 1), (lf_hbm, lf_s, 2), (bk_hbm, bk_s, 3), (bv_hbm, bv_s, 4), (wr_hbm, wr_s, 5), (idx_hbm, idx_s, 6), (mask_hbm, mask_s, 7)]
    smalls += [(src, vec_s.at[i], 8 + i) for i, src in enumerate(vecs)]
    small_copies = [pltpu.make_async_copy(src, dst, small_sem.at[i]) for src, dst, i in smalls]
    small_waits = [pltpu.make_async_copy(x_s, x_s, small_sem.at[0])] + small_copies[2:]
    qw = wq_s.shape[2]
    wq_copies = [pltpu.make_async_copy(wq_hbm.at[:, pl.ds(i * qw, qw)], wq_s.at[i], wq_sem.at[i]) for i in range(n_hp)]
    wkv_copies = [pltpu.make_async_copy(wk_hbm, wk_s, wkv_sem.at[0]), pltpu.make_async_copy(wv_hbm, wv_s, wkv_sem.at[1])]
    for cp in small_copies:
        cp.start()
    cut = dm // 2
    for j in range(2):
        for i in range(n_hp):
            pltpu.make_async_copy(wq_hbm.at[pl.ds(j * cut, cut), pl.ds(i * qw, qw)], wq_s.at[i, pl.ds(j * cut, cut)], wq_sem.at[i]).start()
    for j in range(2):
        for i, (src, dst) in enumerate(((wk_hbm, wk_s), (wv_hbm, wv_s))):
            pltpu.make_async_copy(src.at[pl.ds(j * cut, cut)], dst.at[pl.ds(j * cut, cut)], wkv_sem.at[i]).start()

    barrier = pltpu.get_barrier_semaphore()
    for d in range(1, n):
        pl.semaphore_signal(barrier, inc=1, device_id={'kv': lax.rem(me + d, n)}, device_id_type=mesh_id)

    quad = SUBL // 2
    n_quad = batch // quad

    def cache_copy(src, dst, sem, i):
        sl = pl.ds(i * quad, quad)
        return pltpu.make_async_copy(src.at[sl], dst.at[sl], sem.at[i])

    def cache_start(src, dst, sem, i):
        for b in range(i * quad, (i + 1) * quad):
            pltpu.make_async_copy(src.at[b], dst.at[b], sem.at[i]).start()

    k_start = functools.partial(cache_start, k_hbm, k_s, k_sem)
    v_start = functools.partial(cache_start, v_hbm, v_s, v_sem)
    k_copies = [cache_copy(k_hbm, k_s, k_sem, i) for i in range(n_quad)]
    v_copies = [cache_copy(v_hbm, v_s, v_sem, i) for i in range(n_quad)]
    n_ec = wg_s.shape[0] // LANES

    def weight_start(src, dst, sem, parts=4):
        ec = src.shape[0] // parts
        for i in range(parts):
            pltpu.make_async_copy(src.at[pl.ds(i * ec, ec)], dst.at[pl.ds(i * ec, ec)], sem).start()

    def weight_wait(dst, sem):
        pltpu.make_async_copy(dst, dst, sem).wait()

    for cp in small_waits:
        cp.wait()
    k_start(0)
    v_start(0)
    k_start(1)

    g1, b1, bq, bo, g2, b2 = [vec_s[i].reshape(1, dm) for i in range(6)]
    x = x_s[...].reshape(rows, dm).astype(F32)
    h = norm_rows(x, g1, b1)

    lane1 = lax.broadcasted_iota(jnp.int32, (1, LANES), 1)
    half_dim = hd // 2
    jlane = lax.rem(lane1, half_dim)
    lfv = jnp.zeros((1, LANES), F32)
    for j in range(half_dim):
        lfv = jnp.where(jlane == j, lf_s[j], lfv)
    inv = 1.0 / (lfv * jnp.exp(jlane.astype(F32) * (2.0 * math.log(ROPE_BASE) / hd)))
    subb = lax.broadcasted_iota(jnp.int32, (batch, LANES), 0)
    pos = jnp.zeros((batch, LANES), jnp.int32)
    for b in range(batch):
        pos = jnp.where(subb == b, len_s[b], pos)
    ang = jnp.concatenate([(pos + s).astype(F32) * inv for s in range(steps)], axis=0)
    cos = jnp.cos(ang) * ROPE_MSCALE
    sin = jnp.sin(ang) * ROPE_MSCALE
    lane_r = lax.broadcasted_iota(jnp.int32, (rows, LANES), 1)
    sin = jnp.where(lax.rem(lane_r, hd) < half_dim, -sin, sin)
    low_half = lax.rem(lane_r, hd) < half_dim
    low_head = lane_r < hd

    def rope(t):
        t = t.astype(BF16).astype(F32)
        rot = jnp.where(low_half, pltpu.roll(t, LANES - half_dim, 1), pltpu.roll(t, half_dim, 1))
        return (t * cos + rot * sin).astype(BF16).astype(F32)

    def q_block(hp):
        t = jnp.dot(h, wq_s[hp], preferred_element_type=F32) + bq[:, hp * qw:(hp + 1) * qw]
        parts = [rope(t[:, c * LANES:(c + 1) * LANES]) for c in range(qw // LANES)]
        for g in range(group):
            first, second = g, group + g
            a, a_hi = parts[first // 2], first % 2
            c, c_hi = parts[second // 2], second % 2
            a = pltpu.roll(a, hd, 1) if a_hi else a
            c = c if c_hi else pltpu.roll(c, hd, 1)
            q_s[hp, g * steps:(g + 1) * steps] = jnp.where(low_head, a, c).reshape(steps, batch, LANES)

    for cp in wq_copies[:2]:
        cp.wait()
    k_start(2)
    v_start(1)
    for hp in range(2):
        q_block(hp)
    for cp in wq_copies[2:] + wkv_copies:
        cp.wait()
    k_start(3)
    v_start(2)
    v_start(3)
    for hp in range(2, n_hp):
        q_block(hp)
    t = jnp.dot(h, wk_s[...], preferred_element_type=F32) + bk_s[...].reshape(1, hdk)
    for hp in range(n_hp):
        kt_s[hp] = rope(t[:, hp * LANES:(hp + 1) * LANES]).reshape(steps, batch, LANES)
    t = (jnp.dot(h, wv_s[...], preferred_element_type=F32) + bv_s[...].reshape(1, hdk)).astype(BF16).astype(F32)
    for hp in range(n_hp):
        vt_s[hp] = t[:, hp * LANES:(hp + 1) * LANES].reshape(steps, batch, LANES)

    tpos = me * shard + lax.broadcasted_iota(jnp.int32, (1, shard), 1)
    diag = lax.broadcasted_iota(jnp.int32, (heads_kv, hdk), 0) == lax.broadcasted_iota(jnp.int32, (heads_kv, hdk), 1) // hd
    ident = lax.broadcasted_iota(jnp.int32, (qrows, LANES), 0) == lax.broadcasted_iota(jnp.int32, (qrows, LANES), 1)
    o_rows = gs_n * quad
    m_rows = o_rows + quad
    last = o_rows // SUBL * SUBL
    n_tile = last // SUBL + 1
    lane8 = lax.broadcasted_iota(jnp.int32, (SUBL, LANES), 1)
    sub8 = lax.broadcasted_iota(jnp.int32, (SUBL, LANES), 0)
    low8 = lane8 < hd
    low4 = sub8 < quad

    tail_hp = 2 * core + lax.rem(chip, 2)
    tail_q = chip // 2 * 2
    brow = pl.ds(pl.multiple_of(tail_q * quad, SUBL), SUBL)

    def tail_slots():
        for q in range(n_quad):
            tail_s[q, :m_rows] = jnp.zeros((m_rows, LANES), F32)
            tail_s[q, m_rows:m_rows + SUBL] = jnp.full((SUBL, LANES), NEG_FILL, F32)
            tail_s[q, m_rows + SUBL:] = jnp.zeros((SUBL, LANES), F32)
            for hp in range(n_hp):
                msg_s[q, hp, o_rows:] = jnp.zeros((quad, LANES), F32)
        m_tail = jnp.full((SUBL, LANES), NEG_FILL, F32)
        l_tail = jnp.zeros((SUBL, LANES), F32)
        for gs in range(gs_n):
            s = gs % steps
            qt = q_s[tail_hp, gs, brow, :]
            cols = []
            for slot in range(s + 1):
                prod = qt * kt_s[tail_hp, slot, brow, :]
                lo = jnp.sum(jnp.where(low8, prod, 0.0), axis=1, keepdims=True)
                hi = jnp.sum(jnp.where(low8, 0.0, prod), axis=1, keepdims=True)
                cols.append(jnp.where(low8, lo, hi) * (hd ** -0.5))
            mx = functools.reduce(jnp.maximum, cols)
            ws = [jnp.exp(c - mx) for c in cols]
            lsum = functools.reduce(jnp.add, ws)
            acc = functools.reduce(jnp.add, [w.astype(BF16).astype(F32) * vt_s[tail_hp, slot, brow, :] for slot, w in enumerate(ws)])
            for i in range(2):
                tail_s[tail_q + i, gs * quad:(gs + 1) * quad] = acc[i * quad:(i + 1) * quad]
            for j in range(2):
                sel = lane8 == gs * heads_kv + j
                m_tail = jnp.where(sel, mx[:, j * hd:j * hd + 1], m_tail)
                l_tail = jnp.where(sel, lsum[:, j * hd:j * hd + 1], l_tail)
        m_tail = pltpu.roll(m_tail, 2 * tail_hp, 1)
        l_tail = pltpu.roll(l_tail, 2 * tail_hp, 1)
        for i in range(2):
            for k in range(2):
                rs = slice(m_rows + k * quad, m_rows + (k + 1) * quad)
                tail_s[tail_q + i, rs] = m_tail[i * quad:(i + 1) * quad]
                rs = slice(m_rows + SUBL + k * quad, m_rows + SUBL + (k + 1) * quad)
                tail_s[tail_q + i, rs] = l_tail[i * quad:(i + 1) * quad]

    def to_row(col):
        return jnp.sum(jnp.where(ident, col, 0.0), axis=0, keepdims=True)

    def scores(i):
        for j in range(quad):
            b = i * quad + j
            blocks = []
            for gs in range(gs_n):
                qrow = jnp.concatenate([q_s[hp, gs, b:b + 1, :] for hp in range(n_hp)], axis=1)
                blocks.append(jnp.where(diag, qrow, 0.0))
            blocks.append(jnp.zeros((heads_kv, hdk), F32))
            qbd = jnp.concatenate(blocks, axis=0).astype(BF16)
            keep = tpos < len_s[b]
            sc = jnp.dot(qbd, k_s[b], preferred_element_type=F32) * (hd ** -0.5)
            sc = jnp.where(keep, sc, NEG_FILL)
            m = jnp.max(sc, axis=1, keepdims=True)
            w = jnp.where(keep, jnp.exp(sc - m), 0.0)
            p_s[b] = w.astype(BF16)
            mrow, lrow = to_row(m), to_row(jnp.sum(w, axis=1, keepdims=True))
            for k in range(2):
                r = k * quad + j
                ml_s[i, 0, r:r + 1, :] = mrow
                ml_s[i, 1, r:r + 1, :] = lrow

    def outputs(i):
        for j in range(quad):
            b = i * quad + j
            o = lax.dot_general(p_s[b], v_s[b], NT, preferred_element_type=F32)
            for gs in range(gs_n):
                row = jnp.sum(jnp.where(diag, o[gs * heads_kv:(gs + 1) * heads_kv], 0.0), axis=0, keepdims=True)
                for hp in range(n_hp):
                    msg_s[i, hp, gs * quad + j:gs * quad + j + 1, :] = row[:, hp * LANES:(hp + 1) * LANES]

    def spread(t, lane):
        return jnp.where(low8, t[:, lane:lane + 1], t[:, lane + 1:lane + 2])

    def both_halves(t):
        return jnp.where(low4, t, pltpu.roll(t, LANES - heads_kv, 1))

    tiles = [pl.ds(t * SUBL, SUBL) for t in range(n_tile)]

    def ml_copy(q):
        return remote(ml_s.at[q], mlp_s.at[q], ml_send.at[0], ml_recv.at[q], partner)

    def pair_copy(q):
        return remote(msg_s.at[q, pl.ds(2 * other, 2)], pair_s.at[q], pair_send.at[0], pair_recv.at[q], partner)

    def pair_factors(q):
        ms = [ml_s[q, 0], mlp_s[q, 0], tail_s[q, pl.ds(m_rows, SUBL)]]
        ls = [ml_s[q, 1], mlp_s[q, 1], tail_s[q, pl.ds(m_rows + SUBL, SUBL)]]
        mm = functools.reduce(jnp.maximum, ms)
        es = [jnp.exp(m - mm) for m in ms]
        ll = functools.reduce(jnp.add, [e * l for e, l in zip(es, ls)])
        recv_s[q, chip, core, 0, o_rows:] = mm[quad:]
        recv_s[q, chip, core, 1, o_rows:] = ll[quad:]
        es = [both_halves(e) for e in es]
        es[2] = pltpu.roll(es[2], lax.rem(LANES - 2 * tail_hp, LANES), 1)
        for k in range(2):
            shift = lax.rem(LANES - 2 * (2 * core + k), LANES)
            fs = [pltpu.roll(es[0], shift, 1), pltpu.roll(es[1], shift, 1), jnp.where(lax.rem(chip, 2) == k, es[2], 0.0)]
            for i, f in enumerate(fs):
                for t in range(n_tile):
                    cf_s[q, k, i, tiles[t]] = spread(f, t * 2 * heads_kv)

    def pair_merge(q):
        pair_copy(q).wait_recv()
        dst = recv_s.at[q, chip, core]
        for k in range(2):
            rs = pl.ds(0, o_rows)
            dst[k, rs] = cf_s[q, k, 0, rs] * msg_s[q, 2 * core + k, rs] + cf_s[q, k, 1, rs] * pair_s[q, k, rs] + cf_s[q, k, 2, rs] * tail_s[q, rs]
        for dx in (2, 1, 3):
            remote(dst, dst, g_send.at[0], g_recv.at[q, chip, core], lax.rem(chip + dx, n_hp) * 2 + core).start()
        remote(dst, dst, g_send.at[1], g_recv.at[q, chip, core], partner).start()

    def part_arrived(q, cx, c):
        blk = recv_s.at[q, cx, c]
        remote(blk, blk, g_send.at[0], g_recv.at[q, cx, c], me).wait_recv()
        return blk

    def part_relay(q):
        for dx in (1, 3, 2):
            cx = lax.rem(chip + dx, n_hp)
            blk = part_arrived(q, cx, core)
            remote(blk, blk, g_send.at[1], g_recv.at[q, cx, core], partner).start()

    def final_merge(q):
        for dx in (0, 1, 3, 2):
            part_arrived(q, lax.rem(chip + dx, n_hp), other)
        for c in range(2):
            ms = [recv_s[q, cx, c, 0, tiles[-1]] for cx in range(n_hp)]
            mm = functools.reduce(jnp.maximum, ms)
            es = [jnp.exp(m - mm) for m in ms]
            inv_l = 1.0 / functools.reduce(jnp.add, [e * recv_s[q, cx, c, 1, tiles[-1]] for cx, e in enumerate(es)])
            es = [jnp.where(low4, pltpu.roll(e * inv_l, quad, 0), pltpu.roll(e * inv_l, LANES - heads_kv, 1)) for e in es]
            for k in range(2):
                hp = 2 * c + k
                for t in range(n_tile):
                    lane = t * 2 * heads_kv + 2 * hp
                    o = functools.reduce(jnp.add, [spread(e, lane) * recv_s[q, cx, c, k, tiles[t]] for cx, e in enumerate(es)])
                    for i in range(2):
                        gs = 2 * t + i
                        if gs < gs_n:
                            r = gs % steps * batch + q * quad
                            of_s[gs // steps, r:r + quad, hp * LANES:(hp + 1) * LANES] = o[i * quad:(i + 1) * quad]

    stages = [(0, None, None), (None, 0, None), (1, None, 0)]
    stages += [(i + 1 if i + 1 < n_quad else None, i, i - 1 if i > 1 else None) for i in range(1, n_quad)]
    for sc, out, mg in stages:
        if sc is not None:
            k_copies[sc].wait()
        if out is not None:
            v_copies[out].wait()
        if sc == n_quad - 1:
            for g in range(group):
                pltpu.make_async_copy(wo_hbm.at[:, :, g], wo_s.at[:, g], wo_sem.at[0]).start()
            weight_start(wg_hbm, wg_s, exp_sem.at[0])
            weight_start(wu_hbm, wu_s, exp_sem.at[1])
            weight_start(wd_hbm, wd_s, wd_sem.at[0])
        if mg is not None:
            ml_copy(mg).wait_recv()
        if sc is not None:
            scores(sc)
        if out == 0:
            tail_slots()
        if out is not None:
            outputs(out)
        if mg is not None:
            pair_factors(mg)
        if sc == 0:
            pl.semaphore_wait(barrier, n - 1)
        if sc is not None:
            ml_copy(sc).start()
        if out is not None:
            pair_copy(out).start()
        if mg is not None:
            pair_merge(mg)
    ml_copy(n_quad - 1).wait_recv()
    pair_factors(n_quad - 1)
    pair_merge(n_quad - 1)

    part_relay(0)
    for q in range(n_quad):
        if q + 1 < n_quad:
            part_relay(q + 1)
        else:
            weight_wait(wo_s, wo_sem.at[0])
            weight_wait(wg_s, exp_sem.at[0])
            weight_wait(wu_s, exp_sem.at[1])
        final_merge(q)

    lhs = jnp.concatenate([of_s[g, :, hp * LANES:(hp + 1) * LANES] for hp in range(n_hp) for g in range(group)], axis=1).astype(BF16)
    acc = jnp.dot(lhs, wo_s[...].reshape(dm, dm), preferred_element_type=F32)
    x = x_s[...].reshape(rows, dm).astype(F32)
    xm = (x + acc + bo).astype(BF16).astype(F32)
    xm_s[...] = xm.reshape(2, rows // 2, dm)
    h2 = norm_rows(xm, g2, b2)

    logits = lax.dot_general(h2, wr_s[...], NT, preferred_element_type=F32)
    topk = mask_s.shape[1]
    e_iota = lax.broadcasted_iota(jnp.int32, (topk, n_exp), 1)
    grows = []
    for s in range(steps):
        ids = idx_s[s]
        for b in range(batch):
            r = s * batch + b
            lg = jnp.where(mask_s[r] == 1, logits[r:r + 1, :], NEG_FILL)
            ex = jnp.exp(lg - jnp.max(lg, axis=1, keepdims=True))
            pr = ex / jnp.sum(ex, axis=1, keepdims=True)
            grows.append(jnp.sum(jnp.where(ids[:, b:b + 1] == e_iota, pr, 0.0), axis=0, keepdims=True))
    gates = jnp.concatenate(grows, axis=0)
    per = LANES // ff

    def act(c):
        rs = pl.ds(c * LANES, LANES)
        ag = lax.dot_general(h2, wg_s[rs, :], NT, preferred_element_type=F32)
        au = lax.dot_general(h2, wu_s[rs, :], NT, preferred_element_type=F32)
        return ag * (1.0 / (1.0 + jnp.exp(-ag))), au

    for c in range(n_ec):
        gex_s[c] = jnp.where(low_head, gates[:, per * c:per * c + 1], gates[:, per * c + 1:per * c + 2])
    for c in range(n_ec):
        sg, au = act(c)
        u_s[c] = (gex_s[c] * sg * au).astype(BF16)

    cw = n_hp * LANES
    n_ch = dm // cw
    hr = rows // 2
    u = jnp.concatenate([u_s[c] for c in range(n_ec)], axis=1)

    def d_copy(k):
        return remote(pbuf_s.at[k, other], ppair_s.at[k], d_send.at[0], d_recv.at[k], partner)

    def add_pair(k):
        d_copy(k).wait_recv()
        psum_s[k] = pbuf_s[k, core] + ppair_s[k]
        for dx in (2, 1, 3):
            cx = lax.rem(chip + dx, n_hp)
            remote(psum_s.at[k, cx], rbuf_s.at[k, chip], p_send.at[0], p_recv.at[k, chip], cx * 2 + core).start()

    weight_wait(wd_s, wd_sem.at[0])
    for k in range(n_ch):
        part = jnp.dot(u, wd_s[:, k * cw:(k + 1) * cw], preferred_element_type=F32)
        part = part.astype(BF16).astype(F32)
        for half in range(2):
            for cx in range(n_hp):
                pbuf_s[k, half, cx] = part[half * hr:(half + 1) * hr, cx * LANES:(cx + 1) * LANES]
        d_copy(k).start()
        if k:
            add_pair(k - 1)
    add_pair(n_ch - 1)

    for src_s, dst in ((kt_s, tk_out), (vt_s, tv_out)):
        for hp in range(n_hp):
            t = src_s[hp].reshape(rows, LANES)
            hs_s[:, 2 * hp, :] = t[:, :hd]
            hs_s[:, 2 * hp + 1, :] = pltpu.roll(t, hd, 1)[:, :hd]
        for s in range(steps):
            dst[:, s] = hs_s[s * batch:(s + 1) * batch].astype(BF16)

    def y_arrived(k, cx, c):
        blk = ybuf_s.at[k, cx, c]
        remote(blk, blk, y_send.at[0], g_recv.at[k, cx, c], me).wait_recv()
        return blk

    for k in range(n_ch):
        y = xm_s[core, :, pl.ds(pl.multiple_of(k * cw + chip * LANES, LANES), LANES)] + psum_s[k, chip]
        for dx in (1, 3, 2):
            cx = lax.rem(chip + dx, n_hp)
            remote(rbuf_s.at[k, cx], rbuf_s.at[k, cx], p_send.at[0], p_recv.at[k, cx], me).wait_recv()
            y = y + rbuf_s[k, cx]
        ybuf_s[k, chip, core] = y.astype(BF16).astype(F32)
        blk = ybuf_s.at[k, chip, core]
        for dx in (2, 1, 3):
            remote(blk, blk, y_send.at[0], g_recv.at[k, chip, core], lax.rem(chip + dx, n_hp) * 2 + core).start()
        remote(blk, blk, y_send.at[1], g_recv.at[k, chip, core], partner).start()
    for k in range(n_ch):
        for dx in (1, 3, 2):
            cx = lax.rem(chip + dx, n_hp)
            blk = y_arrived(k, cx, core)
            remote(blk, blk, y_send.at[1], g_recv.at[k, cx, core], partner).start()
    for k in range(n_ch):
        for dx in (0, 1, 3, 2):
            y_arrived(k, lax.rem(chip + dx, n_hp), other)
        for cx in range(n_hp):
            blk = jnp.concatenate([ybuf_s[k, cx, 0], ybuf_s[k, cx, 1]], axis=0)
            hid_out[:, :, k * cw + cx * LANES:k * cw + (cx + 1) * LANES] = blk.astype(BF16).reshape(steps, batch, LANES)
    one = pl.ds(0, 1)
    part_blocks = pl.ds(0, n_hp - 1)
    for blks, sem in ((mlp_s, ml_send.at[0]), (pair_s, pair_send.at[0]), (recv_s.at[part_blocks, :, one], g_send.at[0]), (recv_s.at[:, :, one], g_send.at[1]),
                      (ppair_s, d_send.at[0]), (rbuf_s.at[:, part_blocks], p_send.at[0]), (ybuf_s.at[:, part_blocks, one], y_send.at[0]), (ybuf_s.at[:, :, one], y_send.at[1])):
        pltpu.make_async_copy(blks, blks, sem).wait()


def emit_kernel(*refs):
    k = len(refs) // 2
    stores = [pltpu.make_async_copy(refs[i], refs[k + i], refs[2 * k].at[i]) for i in range(k)]
    for cp in stores:
        cp.start()
    for cp in stores:
        cp.wait()


def solution(mesh):
    n = mesh.shape['kv']

    def layer_steps(x_first, next_emb, k_cache, v_cache, seq_len, ln1_gain, ln1_bias, w_q, b_q, w_k, b_k, w_v, b_v, w_o, b_o, ln2_gain, ln2_bias, w_router, w_gate, w_up, w_down, long_factor, expert_idx, route_mask):
        batch, shard, heads_kv, hd = k_cache.shape
        dm = x_first.shape[1]
        q_heads = w_q.shape[1] // hd
        group = q_heads // heads_kv
        steps = next_emb.shape[0] + 1
        n_exp, _, ff = w_gate.shape
        topk = expert_idx.shape[-1]
        rows = steps * batch
        hdk = heads_kv * hd
        n_hp = hdk // LANES
        gs_n = group * steps
        qrows = (gs_n + 1) * heads_kv
        fe = n_exp * ff
        dims = (n, steps, batch, heads_kv, hd, group, shard, n_exp, ff, dm)
        args = (
            x_first, next_emb,
            jnp.transpose(k_cache, (0, 2, 3, 1)).reshape(batch, hdk, shard),
            jnp.transpose(v_cache, (0, 2, 3, 1)).reshape(batch, hdk, shard),
            seq_len, ln1_gain, ln1_bias, w_q, b_q, w_k, b_k, w_v, b_v,
            w_o.reshape(n_hp, 2, group, hd, dm), b_o, ln2_gain, ln2_bias,
            jnp.transpose(w_router),
            jnp.transpose(w_gate, (0, 2, 1)).reshape(fe, dm),
            jnp.transpose(w_up, (0, 2, 1)).reshape(fe, dm),
            w_down.reshape(fe, dm), long_factor,
            jnp.transpose(expert_idx, (0, 2, 1)),
            route_mask.reshape(rows, topk, n_exp),
        )
        any_spec = pl.BlockSpec(memory_space=pl.ANY)
        dma = pltpu.SemaphoreType.DMA
        vm = pltpu.VMEM
        outs = (
            jax.ShapeDtypeStruct((steps, batch, dm), BF16),
            jax.ShapeDtypeStruct((batch, steps, heads_kv, hd), BF16),
            jax.ShapeDtypeStruct((batch, steps, heads_kv, hd), BF16),
        )
        n_quad = batch // (SUBL // 2)
        m_rows = (gs_n + 1) * (SUBL // 2)
        n_ch = dm // hdk
        qblk = vm((n_ch, n_hp, rows // 2, LANES), F32)
        scratch = [
            vm((steps, batch, dm), BF16), pltpu.SMEM((batch,), jnp.int32), pltpu.SMEM((hd // 2,), F32),
            vm((6, dm), F32), vm((hdk,), F32), vm((hdk,), F32), vm((n_exp, dm), BF16),
            vm((steps, topk, batch), jnp.int32), vm((rows, topk, n_exp), jnp.int32),
            vm((n_hp, dm, dm // n_hp), BF16), vm((dm, hdk), BF16), vm((dm, hdk), BF16),
            vm((n_hp, group, 2, hd, dm), BF16), vm((batch, hdk, shard), BF16), vm((batch, hdk, shard), BF16),
            vm((fe, dm), BF16), vm((fe, dm), BF16), vm((fe, dm), BF16),
            vm((n_hp, gs_n, batch, LANES), F32), vm((n_hp, steps, batch, LANES), F32), vm((n_hp, steps, batch, LANES), F32),
            vm((rows, heads_kv, hd), F32), vm((batch, qrows, shard), BF16),
            vm((n_quad, n_hp, m_rows, LANES), F32), vm((n_quad, 2, m_rows, LANES), F32),
            vm((n_quad, 2, SUBL, LANES), F32), vm((n_quad, 2, SUBL, LANES), F32), vm((n_quad, 2, 3, m_rows, LANES), F32), vm((n_quad, m_rows + 2 * SUBL, LANES), F32),
            vm((n_quad, n_hp, 2, 2, m_rows, LANES), F32), vm((group, rows, hdk), F32), vm((2, rows // 2, dm), F32),
            vm((fe // LANES, rows, LANES), F32), vm((fe // LANES, rows, LANES), BF16),
            vm((n_ch, 2, n_hp, rows // 2, LANES), F32), qblk, qblk, qblk, vm((n_ch, n_hp, 2, rows // 2, LANES), F32),
            dma((14,)), dma((n_hp,)), dma((2,)), dma((1,)), dma((4,)), dma((4,)), dma((2,)), dma((1,)),
            dma((1,)), dma((n_quad,)), dma((1,)), dma((n_quad,)), dma((2,)), dma((n_quad, n_hp, 2)),
            dma((1,)), dma((n_ch,)), dma((1,)), dma((n_ch, n_hp)), dma((2,)),
        ]
        vmem_spec = pl.BlockSpec(memory_space=pltpu.VMEM)
        made = pl.pallas_call(
            functools.partial(layer_kernel, dims),
            out_shape=tuple(vm(o.shape, o.dtype) for o in outs),
            in_specs=[any_spec] * len(args),
            out_specs=(vmem_spec,) * 3,
            scratch_shapes=scratch,
            compiler_params=pltpu.CompilerParams(collective_id=0, has_side_effects=True, vmem_limit_bytes=VMEM_BYTES),
        )(*args)
        made = [pltpu.with_memory_space_constraint(m, pltpu.VMEM) for m in made]
        return pl.pallas_call(
            emit_kernel,
            out_shape=outs,
            in_specs=[any_spec] * 3,
            out_specs=(any_spec,) * 3,
            scratch_shapes=[dma((3,))],
        )(*made)

    replicated = P()
    in_specs = (P('dp'), P(None, 'dp'), P('dp', 'kv'), P('dp', 'kv'), P('dp')) + (replicated,) * 13 + (P(None, None, 'kv'), P(None, None, 'kv'), P(None, 'kv'), replicated, P(None, 'dp'), P(None, 'dp'))
    out_specs = (P(None, 'dp'), P('dp'), P('dp'))
    return jax.shard_map(layer_steps, mesh=mesh, in_specs=in_specs, out_specs=out_specs, check_vma=False)
```

```python
import functools
import math

import jax
import jax.numpy as jnp
from jax import lax
from jax.experimental import pallas as pl
from jax.experimental.pallas import tpu as pltpu
from jax.sharding import PartitionSpec as P

ROPE_BASE = 10000.0
ROPE_MSCALE = math.sqrt(1.0 + math.log(32.0) / math.log(4096.0))
NORM_EPS = 1e-5
NEG_FILL = -1e30
LANES = 128
SUBL = 8
F32 = jnp.float32
BF16 = jnp.bfloat16
NT = (((1,), (1,)), ((), ()))
VMEM_BYTES = 61 * 1024 * 1024


def norm_rows(x, gain, bias):
    mean = jnp.mean(x, axis=-1, keepdims=True)
    cent = x - mean
    var = jnp.mean(cent * cent, axis=-1, keepdims=True)
    return (cent * lax.rsqrt(var + NORM_EPS) * gain + bias).astype(BF16)


def layer_kernel(dims, x_first, next_emb, k_hbm, v_hbm, len_hbm, g1_hbm, b1_hbm, wq_hbm, bq_hbm, wk_hbm, bk_hbm, wv_hbm, bv_hbm, wo_hbm, bo_hbm, g2_hbm, b2_hbm, wr_hbm, wg_hbm, wu_hbm, wd_hbm, lf_hbm, idx_hbm, mask_hbm,
                 hid_out, tk_out, tv_out,
                 x_s, len_s, lf_s, vec_s, bk_s, bv_s, wr_s, idx_s, mask_s,
                 wq_s, wk_s, wv_s, wo_s, k_s, v_s, wg_s, wu_s, wd_s,
                 q_s, kt_s, vt_s, hs_s, p_s, msg_s, pair_s, ml_s, mlp_s, cf_s, tail_s, recv_s, of_s, xm_s, gex_s, u_s, pbuf_s, ppair_s, psum_s, rbuf_s, ybuf_s,
                 small_sem, wq_sem, wkv_sem, wo_sem, k_sem, v_sem, exp_sem, wd_sem,
                 ml_send, ml_recv, pair_send, pair_recv, g_send, g_recv, d_send, d_recv, p_send, p_recv, y_send):
    n, steps, batch, heads_kv, hd, group, shard, n_exp, ff, dm = dims
    rows = steps * batch
    gs_n = group * steps
    qrows = (gs_n + 1) * heads_kv
    hdk = heads_kv * hd
    n_hp = hdk // LANES
    me = lax.axis_index('kv')
    chip = me // 2
    core = lax.rem(me, 2)
    other = 1 - core
    partner = chip * 2 + other
    mesh_id = pl.DeviceIdType.MESH

    def remote(src, dst, send, recv, dev):
        return pltpu.make_async_remote_copy(src_ref=src, dst_ref=dst, send_sem=send, recv_sem=recv, device_id={'kv': dev}, device_id_type=mesh_id)

    vecs = (g1_hbm, b1_hbm, bq_hbm, bo_hbm, g2_hbm, b2_hbm)
    smalls = [(x_first, x_s.at[0], 0), (next_emb, x_s.at[pl.ds(1, steps - 1)], 0)]
    smalls += [(len_hbm, len_s, 1), (lf_hbm, lf_s, 2), (bk_hbm, bk_s, 3), (bv_hbm, bv_s, 4), (wr_hbm, wr_s, 5), (idx_hbm, idx_s, 6), (mask_hbm, mask_s, 7)]
    smalls += [(src, vec_s.at[i], 8 + i) for i, src in enumerate(vecs)]
    small_copies = [pltpu.make_async_copy(src, dst, small_sem.at[i]) for src, dst, i in smalls]
    small_waits = [pltpu.make_async_copy(x_s, x_s, small_sem.at[0])] + small_copies[2:]
    qw = wq_s.shape[2]
    wq_copies = [pltpu.make_async_copy(wq_hbm.at[:, pl.ds(i * qw, qw)], wq_s.at[i], wq_sem.at[i]) for i in range(n_hp)]
    wkv_copies = [pltpu.make_async_copy(wk_hbm, wk_s, wkv_sem.at[0]), pltpu.make_async_copy(wv_hbm, wv_s, wkv_sem.at[1])]
    for cp in small_copies + wq_copies + wkv_copies:
        cp.start()

    barrier = pltpu.get_barrier_semaphore()
    for d in range(1, n):
        pl.semaphore_signal(barrier, inc=1, device_id={'kv': lax.rem(me + d, n)}, device_id_type=mesh_id)

    quad = SUBL // 2
    n_quad = batch // quad

    def cache_copy(src, dst, sem, i):
        sl = pl.ds(i * quad, quad)
        return pltpu.make_async_copy(src.at[sl], dst.at[sl], sem.at[i])

    k_copies = [cache_copy(k_hbm, k_s, k_sem, i) for i in range(n_quad)]
    v_copies = [cache_copy(v_hbm, v_s, v_sem, i) for i in range(n_quad)]
    n_ec = wg_s.shape[0] // LANES

    def weight_start(src, dst, sem, parts=4):
        ec = src.shape[0] // parts
        for i in range(parts):
            pltpu.make_async_copy(src.at[pl.ds(i * ec, ec)], dst.at[pl.ds(i * ec, ec)], sem).start()

    def weight_wait(dst, sem):
        pltpu.make_async_copy(dst, dst, sem).wait()

    for cp in small_waits:
        cp.wait()
    for cp in (k_copies[0], k_copies[1], v_copies[0]):
        cp.start()

    g1, b1, bq, bo, g2, b2 = [vec_s[i].reshape(1, dm) for i in range(6)]
    x = x_s[...].reshape(rows, dm).astype(F32)
    h = norm_rows(x, g1, b1)

    lane1 = lax.broadcasted_iota(jnp.int32, (1, LANES), 1)
    half_dim = hd // 2
    jlane = lax.rem(lane1, half_dim)
    lfv = jnp.zeros((1, LANES), F32)
    for j in range(half_dim):
        lfv = jnp.where(jlane == j, lf_s[j], lfv)
    inv = 1.0 / (lfv * jnp.exp(jlane.astype(F32) * (2.0 * math.log(ROPE_BASE) / hd)))
    subb = lax.broadcasted_iota(jnp.int32, (batch, LANES), 0)
    pos = jnp.zeros((batch, LANES), jnp.int32)
    for b in range(batch):
        pos = jnp.where(subb == b, len_s[b], pos)
    ang = jnp.concatenate([(pos + s).astype(F32) * inv for s in range(steps)], axis=0)
    cos = jnp.cos(ang) * ROPE_MSCALE
    sin = jnp.sin(ang) * ROPE_MSCALE
    lane_r = lax.broadcasted_iota(jnp.int32, (rows, LANES), 1)
    sin = jnp.where(lax.rem(lane_r, hd) < half_dim, -sin, sin)
    low_half = lax.rem(lane_r, hd) < half_dim
    low_head = lane_r < hd

    def rope(t):
        t = t.astype(BF16).astype(F32)
        rot = jnp.where(low_half, pltpu.roll(t, LANES - half_dim, 1), pltpu.roll(t, half_dim, 1))
        return (t * cos + rot * sin).astype(BF16).astype(F32)

    def q_block(hp):
        t = jnp.dot(h, wq_s[hp], preferred_element_type=F32) + bq[:, hp * qw:(hp + 1) * qw]
        parts = [rope(t[:, c * LANES:(c + 1) * LANES]) for c in range(qw // LANES)]
        for g in range(group):
            first, second = g, group + g
            a, a_hi = parts[first // 2], first % 2
            c, c_hi = parts[second // 2], second % 2
            a = pltpu.roll(a, hd, 1) if a_hi else a
            c = c if c_hi else pltpu.roll(c, hd, 1)
            q_s[hp, g * steps:(g + 1) * steps] = jnp.where(low_head, a, c).reshape(steps, batch, LANES)

    for cp in wq_copies[:2]:
        cp.wait()
    for cp in (k_copies[2], v_copies[1]):
        cp.start()
    for hp in range(2):
        q_block(hp)
    for cp in wq_copies[2:] + wkv_copies:
        cp.wait()
    for cp in (k_copies[3], v_copies[2], v_copies[3]):
        cp.start()
    for hp in range(2, n_hp):
        q_block(hp)
    t = jnp.dot(h, wk_s[...], preferred_element_type=F32) + bk_s[...].reshape(1, hdk)
    for hp in range(n_hp):
        kt_s[hp] = rope(t[:, hp * LANES:(hp + 1) * LANES]).reshape(steps, batch, LANES)
    t = (jnp.dot(h, wv_s[...], preferred_element_type=F32) + bv_s[...].reshape(1, hdk)).astype(BF16).astype(F32)
    for hp in range(n_hp):
        vt_s[hp] = t[:, hp * LANES:(hp + 1) * LANES].reshape(steps, batch, LANES)

    tpos = me * shard + lax.broadcasted_iota(jnp.int32, (1, shard), 1)
    diag = lax.broadcasted_iota(jnp.int32, (heads_kv, hdk), 0) == lax.broadcasted_iota(jnp.int32, (heads_kv, hdk), 1) // hd
    ident = lax.broadcasted_iota(jnp.int32, (qrows, LANES), 0) == lax.broadcasted_iota(jnp.int32, (qrows, LANES), 1)
    o_rows = gs_n * quad
    m_rows = o_rows + quad
    last = o_rows // SUBL * SUBL
    n_tile = last // SUBL + 1
    lane8 = lax.broadcasted_iota(jnp.int32, (SUBL, LANES), 1)
    sub8 = lax.broadcasted_iota(jnp.int32, (SUBL, LANES), 0)
    low8 = lane8 < hd
    low4 = sub8 < quad

    tail_hp = 2 * core + lax.rem(chip, 2)
    tail_q = chip // 2 * 2
    brow = pl.ds(pl.multiple_of(tail_q * quad, SUBL), SUBL)

    def tail_slots():
        for q in range(n_quad):
            tail_s[q, :m_rows] = jnp.zeros((m_rows, LANES), F32)
            tail_s[q, m_rows:m_rows + SUBL] = jnp.full((SUBL, LANES), NEG_FILL, F32)
            tail_s[q, m_rows + SUBL:] = jnp.zeros((SUBL, LANES), F32)
            for hp in range(n_hp):
                msg_s[q, hp, o_rows:] = jnp.zeros((quad, LANES), F32)
        m_tail = jnp.full((SUBL, LANES), NEG_FILL, F32)
        l_tail = jnp.zeros((SUBL, LANES), F32)
        for gs in range(gs_n):
            s = gs % steps
            qt = q_s[tail_hp, gs, brow, :]
            cols = []
            for slot in range(s + 1):
                prod = qt * kt_s[tail_hp, slot, brow, :]
                lo = jnp.sum(jnp.where(low8, prod, 0.0), axis=1, keepdims=True)
                hi = jnp.sum(jnp.where(low8, 0.0, prod), axis=1, keepdims=True)
                cols.append(jnp.where(low8, lo, hi) * (hd ** -0.5))
            mx = functools.reduce(jnp.maximum, cols)
            ws = [jnp.exp(c - mx) for c in cols]
            lsum = functools.reduce(jnp.add, ws)
            acc = functools.reduce(jnp.add, [w.astype(BF16).astype(F32) * vt_s[tail_hp, slot, brow, :] for slot, w in enumerate(ws)])
            for i in range(2):
                tail_s[tail_q + i, gs * quad:(gs + 1) * quad] = acc[i * quad:(i + 1) * quad]
            for j in range(2):
                sel = lane8 == gs * heads_kv + j
                m_tail = jnp.where(sel, mx[:, j * hd:j * hd + 1], m_tail)
                l_tail = jnp.where(sel, lsum[:, j * hd:j * hd + 1], l_tail)
        m_tail = pltpu.roll(m_tail, 2 * tail_hp, 1)
        l_tail = pltpu.roll(l_tail, 2 * tail_hp, 1)
        for i in range(2):
            for k in range(2):
                rs = slice(m_rows + k * quad, m_rows + (k + 1) * quad)
                tail_s[tail_q + i, rs] = m_tail[i * quad:(i + 1) * quad]
                rs = slice(m_rows + SUBL + k * quad, m_rows + SUBL + (k + 1) * quad)
                tail_s[tail_q + i, rs] = l_tail[i * quad:(i + 1) * quad]

    def to_row(col):
        return jnp.sum(jnp.where(ident, col, 0.0), axis=0, keepdims=True)

    def scores(i):
        for j in range(quad):
            b = i * quad + j
            blocks = []
            for gs in range(gs_n):
                qrow = jnp.concatenate([q_s[hp, gs, b:b + 1, :] for hp in range(n_hp)], axis=1)
                blocks.append(jnp.where(diag, qrow, 0.0))
            blocks.append(jnp.zeros((heads_kv, hdk), F32))
            qbd = jnp.concatenate(blocks, axis=0).astype(BF16)
            keep = tpos < len_s[b]
            sc = jnp.dot(qbd, k_s[b], preferred_element_type=F32) * (hd ** -0.5)
            sc = jnp.where(keep, sc, NEG_FILL)
            m = jnp.max(sc, axis=1, keepdims=True)
            w = jnp.where(keep, jnp.exp(sc - m), 0.0)
            p_s[b] = w.astype(BF16)
            mrow, lrow = to_row(m), to_row(jnp.sum(w, axis=1, keepdims=True))
            for k in range(2):
                r = k * quad + j
                ml_s[i, 0, r:r + 1, :] = mrow
                ml_s[i, 1, r:r + 1, :] = lrow

    def outputs(i):
        for j in range(quad):
            b = i * quad + j
            o = lax.dot_general(p_s[b], v_s[b], NT, preferred_element_type=F32)
            for gs in range(gs_n):
                row = jnp.sum(jnp.where(diag, o[gs * heads_kv:(gs + 1) * heads_kv], 0.0), axis=0, keepdims=True)
                for hp in range(n_hp):
                    msg_s[i, hp, gs * quad + j:gs * quad + j + 1, :] = row[:, hp * LANES:(hp + 1) * LANES]

    def spread(t, lane):
        return jnp.where(low8, t[:, lane:lane + 1], t[:, lane + 1:lane + 2])

    def both_halves(t):
        return jnp.where(low4, t, pltpu.roll(t, LANES - heads_kv, 1))

    tiles = [pl.ds(t * SUBL, SUBL) for t in range(n_tile)]

    def ml_copy(q):
        return remote(ml_s.at[q], mlp_s.at[q], ml_send.at[0], ml_recv.at[q], partner)

    def pair_copy(q):
        return remote(msg_s.at[q, pl.ds(2 * other, 2)], pair_s.at[q], pair_send.at[0], pair_recv.at[q], partner)

    def pair_factors(q):
        ms = [ml_s[q, 0], mlp_s[q, 0], tail_s[q, pl.ds(m_rows, SUBL)]]
        ls = [ml_s[q, 1], mlp_s[q, 1], tail_s[q, pl.ds(m_rows + SUBL, SUBL)]]
        mm = functools.reduce(jnp.maximum, ms)
        es = [jnp.exp(m - mm) for m in ms]
        ll = functools.reduce(jnp.add, [e * l for e, l in zip(es, ls)])
        recv_s[q, chip, core, 0, o_rows:] = mm[quad:]
        recv_s[q, chip, core, 1, o_rows:] = ll[quad:]
        es = [both_halves(e) for e in es]
        es[2] = pltpu.roll(es[2], lax.rem(LANES - 2 * tail_hp, LANES), 1)
        for k in range(2):
            shift = lax.rem(LANES - 2 * (2 * core + k), LANES)
            fs = [pltpu.roll(es[0], shift, 1), pltpu.roll(es[1], shift, 1), jnp.where(lax.rem(chip, 2) == k, es[2], 0.0)]
            for i, f in enumerate(fs):
                for t in range(n_tile):
                    cf_s[q, k, i, tiles[t]] = spread(f, t * 2 * heads_kv)

    def pair_merge(q):
        pair_copy(q).wait_recv()
        dst = recv_s.at[q, chip, core]
        for k in range(2):
            rs = pl.ds(0, o_rows)
            dst[k, rs] = cf_s[q, k, 0, rs] * msg_s[q, 2 * core + k, rs] + cf_s[q, k, 1, rs] * pair_s[q, k, rs] + cf_s[q, k, 2, rs] * tail_s[q, rs]
        for dx in (2, 1, 3):
            remote(dst, dst, g_send.at[0], g_recv.at[q, chip, core], lax.rem(chip + dx, n_hp) * 2 + core).start()
        remote(dst, dst, g_send.at[1], g_recv.at[q, chip, core], partner).start()

    def part_arrived(q, cx, c):
        blk = recv_s.at[q, cx, c]
        remote(blk, blk, g_send.at[0], g_recv.at[q, cx, c], me).wait_recv()
        return blk

    def part_relay(q):
        for dx in (1, 3, 2):
            cx = lax.rem(chip + dx, n_hp)
            blk = part_arrived(q, cx, core)
            remote(blk, blk, g_send.at[1], g_recv.at[q, cx, core], partner).start()

    def final_merge(q):
        for dx in (0, 1, 3, 2):
            part_arrived(q, lax.rem(chip + dx, n_hp), other)
        for c in range(2):
            ms = [recv_s[q, cx, c, 0, tiles[-1]] for cx in range(n_hp)]
            mm = functools.reduce(jnp.maximum, ms)
            es = [jnp.exp(m - mm) for m in ms]
            inv_l = 1.0 / functools.reduce(jnp.add, [e * recv_s[q, cx, c, 1, tiles[-1]] for cx, e in enumerate(es)])
            es = [jnp.where(low4, pltpu.roll(e * inv_l, quad, 0), pltpu.roll(e * inv_l, LANES - heads_kv, 1)) for e in es]
            for k in range(2):
                hp = 2 * c + k
                for t in range(n_tile):
                    lane = t * 2 * heads_kv + 2 * hp
                    o = functools.reduce(jnp.add, [spread(e, lane) * recv_s[q, cx, c, k, tiles[t]] for cx, e in enumerate(es)])
                    for i in range(2):
                        gs = 2 * t + i
                        if gs < gs_n:
                            r = gs % steps * batch + q * quad
                            of_s[gs // steps, r:r + quad, hp * LANES:(hp + 1) * LANES] = o[i * quad:(i + 1) * quad]

    for i in range(n_quad + 1):
        if i < n_quad:
            k_copies[i].wait()
        if i:
            v_copies[i - 1].wait()
        if i == n_quad - 1:
            for g in range(group):
                pltpu.make_async_copy(wo_hbm.at[:, :, g], wo_s.at[:, g], wo_sem.at[0]).start()
            weight_start(wg_hbm, wg_s, exp_sem.at[0])
            weight_start(wu_hbm, wu_s, exp_sem.at[1])
            weight_start(wd_hbm, wd_s, wd_sem.at[0])
        if i > 1:
            ml_copy(i - 2).wait_recv()
        if i < n_quad:
            scores(i)
        if i == 1:
            tail_slots()
        if i:
            outputs(i - 1)
        if i > 1:
            pair_factors(i - 2)
        if i == 0:
            pl.semaphore_wait(barrier, n - 1)
        if i < n_quad:
            ml_copy(i).start()
        if i:
            pair_copy(i - 1).start()
        if i > 1:
            pair_merge(i - 2)
    ml_copy(n_quad - 1).wait_recv()
    pair_factors(n_quad - 1)
    pair_merge(n_quad - 1)

    part_relay(0)
    for q in range(n_quad):
        if q + 1 < n_quad:
            part_relay(q + 1)
        else:
            weight_wait(wo_s, wo_sem.at[0])
            weight_wait(wg_s, exp_sem.at[0])
            weight_wait(wu_s, exp_sem.at[1])
        final_merge(q)

    lhs = jnp.concatenate([of_s[g, :, hp * LANES:(hp + 1) * LANES] for hp in range(n_hp) for g in range(group)], axis=1).astype(BF16)
    acc = jnp.dot(lhs, wo_s[...].reshape(dm, dm), preferred_element_type=F32)
    x = x_s[...].reshape(rows, dm).astype(F32)
    xm = (x + acc + bo).astype(BF16).astype(F32)
    xm_s[...] = xm.reshape(2, rows // 2, dm)
    h2 = norm_rows(xm, g2, b2)

    logits = lax.dot_general(h2, wr_s[...], NT, preferred_element_type=F32)
    topk = mask_s.shape[1]
    e_iota = lax.broadcasted_iota(jnp.int32, (topk, n_exp), 1)
    grows = []
    for s in range(steps):
        ids = idx_s[s]
        for b in range(batch):
            r = s * batch + b
            lg = jnp.where(mask_s[r] == 1, logits[r:r + 1, :], NEG_FILL)
            ex = jnp.exp(lg - jnp.max(lg, axis=1, keepdims=True))
            pr = ex / jnp.sum(ex, axis=1, keepdims=True)
            grows.append(jnp.sum(jnp.where(ids[:, b:b + 1] == e_iota, pr, 0.0), axis=0, keepdims=True))
    gates = jnp.concatenate(grows, axis=0)
    per = LANES // ff

    def act(c):
        rs = pl.ds(c * LANES, LANES)
        ag = lax.dot_general(h2, wg_s[rs, :], NT, preferred_element_type=F32)
        au = lax.dot_general(h2, wu_s[rs, :], NT, preferred_element_type=F32)
        return ag * (1.0 / (1.0 + jnp.exp(-ag))), au

    for c in range(n_ec):
        gex_s[c] = jnp.where(low_head, gates[:, per * c:per * c + 1], gates[:, per * c + 1:per * c + 2])
    for c in range(n_ec):
        sg, au = act(c)
        u_s[c] = (gex_s[c] * sg * au).astype(BF16)

    cw = n_hp * LANES
    n_ch = dm // cw
    hr = rows // 2
    u = jnp.concatenate([u_s[c] for c in range(n_ec)], axis=1)

    def d_copy(k):
        return remote(pbuf_s.at[k, other], ppair_s.at[k], d_send.at[0], d_recv.at[k], partner)

    def add_pair(k):
        d_copy(k).wait_recv()
        psum_s[k] = pbuf_s[k, core] + ppair_s[k]
        for dx in (2, 1, 3):
            cx = lax.rem(chip + dx, n_hp)
            remote(psum_s.at[k, cx], rbuf_s.at[k, chip], p_send.at[0], p_recv.at[k, chip], cx * 2 + core).start()

    weight_wait(wd_s, wd_sem.at[0])
    for k in range(n_ch):
        part = jnp.dot(u, wd_s[:, k * cw:(k + 1) * cw], preferred_element_type=F32)
        part = part.astype(BF16).astype(F32)
        for half in range(2):
            for cx in range(n_hp):
                pbuf_s[k, half, cx] = part[half * hr:(half + 1) * hr, cx * LANES:(cx + 1) * LANES]
        d_copy(k).start()
        if k:
            add_pair(k - 1)
    add_pair(n_ch - 1)

    for src_s, dst in ((kt_s, tk_out), (vt_s, tv_out)):
        for hp in range(n_hp):
            t = src_s[hp].reshape(rows, LANES)
            hs_s[:, 2 * hp, :] = t[:, :hd]
            hs_s[:, 2 * hp + 1, :] = pltpu.roll(t, hd, 1)[:, :hd]
        for s in range(steps):
            dst[:, s] = hs_s[s * batch:(s + 1) * batch].astype(BF16)

    def y_arrived(k, cx, c):
        blk = ybuf_s.at[k, cx, c]
        remote(blk, blk, y_send.at[0], g_recv.at[k, cx, c], me).wait_recv()
        return blk

    for k in range(n_ch):
        y = xm_s[core, :, pl.ds(pl.multiple_of(k * cw + chip * LANES, LANES), LANES)] + psum_s[k, chip]
        for dx in (1, 3, 2):
            cx = lax.rem(chip + dx, n_hp)
            remote(rbuf_s.at[k, cx], rbuf_s.at[k, cx], p_send.at[0], p_recv.at[k, cx], me).wait_recv()
            y = y + rbuf_s[k, cx]
        ybuf_s[k, chip, core] = y.astype(BF16).astype(F32)
        blk = ybuf_s.at[k, chip, core]
        for dx in (2, 1, 3):
            remote(blk, blk, y_send.at[0], g_recv.at[k, chip, core], lax.rem(chip + dx, n_hp) * 2 + core).start()
        remote(blk, blk, y_send.at[1], g_recv.at[k, chip, core], partner).start()
    for k in range(n_ch):
        for dx in (1, 3, 2):
            cx = lax.rem(chip + dx, n_hp)
            blk = y_arrived(k, cx, core)
            remote(blk, blk, y_send.at[1], g_recv.at[k, cx, core], partner).start()
    for k in range(n_ch):
        for dx in (0, 1, 3, 2):
            y_arrived(k, lax.rem(chip + dx, n_hp), other)
        for cx in range(n_hp):
            blk = jnp.concatenate([ybuf_s[k, cx, 0], ybuf_s[k, cx, 1]], axis=0)
            hid_out[:, :, k * cw + cx * LANES:k * cw + (cx + 1) * LANES] = blk.astype(BF16).reshape(steps, batch, LANES)
    one = pl.ds(0, 1)
    part_blocks = pl.ds(0, n_hp - 1)
    for blks, sem in ((mlp_s, ml_send.at[0]), (pair_s, pair_send.at[0]), (recv_s.at[part_blocks, :, one], g_send.at[0]), (recv_s.at[:, :, one], g_send.at[1]),
                      (ppair_s, d_send.at[0]), (rbuf_s.at[:, part_blocks], p_send.at[0]), (ybuf_s.at[:, part_blocks, one], y_send.at[0]), (ybuf_s.at[:, :, one], y_send.at[1])):
        pltpu.make_async_copy(blks, blks, sem).wait()


def emit_kernel(*refs):
    k = len(refs) // 2
    stores = [pltpu.make_async_copy(refs[i], refs[k + i], refs[2 * k].at[i]) for i in range(k)]
    for cp in stores:
        cp.start()
    for cp in stores:
        cp.wait()


def solution(mesh):
    n = mesh.shape['kv']

    def layer_steps(x_first, next_emb, k_cache, v_cache, seq_len, ln1_gain, ln1_bias, w_q, b_q, w_k, b_k, w_v, b_v, w_o, b_o, ln2_gain, ln2_bias, w_router, w_gate, w_up, w_down, long_factor, expert_idx, route_mask):
        batch, shard, heads_kv, hd = k_cache.shape
        dm = x_first.shape[1]
        q_heads = w_q.shape[1] // hd
        group = q_heads // heads_kv
        steps = next_emb.shape[0] + 1
        n_exp, _, ff = w_gate.shape
        topk = expert_idx.shape[-1]
        rows = steps * batch
        hdk = heads_kv * hd
        n_hp = hdk // LANES
        gs_n = group * steps
        qrows = (gs_n + 1) * heads_kv
        fe = n_exp * ff
        dims = (n, steps, batch, heads_kv, hd, group, shard, n_exp, ff, dm)
        args = (
            x_first, next_emb,
            jnp.transpose(k_cache, (0, 2, 3, 1)).reshape(batch, hdk, shard),
            jnp.transpose(v_cache, (0, 2, 3, 1)).reshape(batch, hdk, shard),
            seq_len, ln1_gain, ln1_bias, w_q, b_q, w_k, b_k, w_v, b_v,
            w_o.reshape(n_hp, 2, group, hd, dm), b_o, ln2_gain, ln2_bias,
            jnp.transpose(w_router),
            jnp.transpose(w_gate, (0, 2, 1)).reshape(fe, dm),
            jnp.transpose(w_up, (0, 2, 1)).reshape(fe, dm),
            w_down.reshape(fe, dm), long_factor,
            jnp.transpose(expert_idx, (0, 2, 1)),
            route_mask.reshape(rows, topk, n_exp),
        )
        any_spec = pl.BlockSpec(memory_space=pl.ANY)
        dma = pltpu.SemaphoreType.DMA
        vm = pltpu.VMEM
        outs = (
            jax.ShapeDtypeStruct((steps, batch, dm), BF16),
            jax.ShapeDtypeStruct((batch, steps, heads_kv, hd), BF16),
            jax.ShapeDtypeStruct((batch, steps, heads_kv, hd), BF16),
        )
        n_quad = batch // (SUBL // 2)
        m_rows = (gs_n + 1) * (SUBL // 2)
        n_ch = dm // hdk
        qblk = vm((n_ch, n_hp, rows // 2, LANES), F32)
        scratch = [
            vm((steps, batch, dm), BF16), pltpu.SMEM((batch,), jnp.int32), pltpu.SMEM((hd // 2,), F32),
            vm((6, dm), F32), vm((hdk,), F32), vm((hdk,), F32), vm((n_exp, dm), BF16),
            vm((steps, topk, batch), jnp.int32), vm((rows, topk, n_exp), jnp.int32),
            vm((n_hp, dm, dm // n_hp), BF16), vm((dm, hdk), BF16), vm((dm, hdk), BF16),
            vm((n_hp, group, 2, hd, dm), BF16), vm((batch, hdk, shard), BF16), vm((batch, hdk, shard), BF16),
            vm((fe, dm), BF16), vm((fe, dm), BF16), vm((fe, dm), BF16),
            vm((n_hp, gs_n, batch, LANES), F32), vm((n_hp, steps, batch, LANES), F32), vm((n_hp, steps, batch, LANES), F32),
            vm((rows, heads_kv, hd), F32), vm((batch, qrows, shard), BF16),
            vm((n_quad, n_hp, m_rows, LANES), F32), vm((n_quad, 2, m_rows, LANES), F32),
            vm((n_quad, 2, SUBL, LANES), F32), vm((n_quad, 2, SUBL, LANES), F32), vm((n_quad, 2, 3, m_rows, LANES), F32), vm((n_quad, m_rows + 2 * SUBL, LANES), F32),
            vm((n_quad, n_hp, 2, 2, m_rows, LANES), F32), vm((group, rows, hdk), F32), vm((2, rows // 2, dm), F32),
            vm((fe // LANES, rows, LANES), F32), vm((fe // LANES, rows, LANES), BF16),
            vm((n_ch, 2, n_hp, rows // 2, LANES), F32), qblk, qblk, qblk, vm((n_ch, n_hp, 2, rows // 2, LANES), F32),
            dma((14,)), dma((n_hp,)), dma((2,)), dma((1,)), dma((4,)), dma((4,)), dma((2,)), dma((1,)),
            dma((1,)), dma((n_quad,)), dma((1,)), dma((n_quad,)), dma((2,)), dma((n_quad, n_hp, 2)),
            dma((1,)), dma((n_ch,)), dma((1,)), dma((n_ch, n_hp)), dma((2,)),
        ]
        vmem_spec = pl.BlockSpec(memory_space=pltpu.VMEM)
        made = pl.pallas_call(
            functools.partial(layer_kernel, dims),
            out_shape=tuple(vm(o.shape, o.dtype) for o in outs),
            in_specs=[any_spec] * len(args),
            out_specs=(vmem_spec,) * 3,
            scratch_shapes=scratch,
            compiler_params=pltpu.CompilerParams(collective_id=0, has_side_effects=True, vmem_limit_bytes=VMEM_BYTES),
        )(*args)
        made = [pltpu.with_memory_space_constraint(m, pltpu.VMEM) for m in made]
        return pl.pallas_call(
            emit_kernel,
            out_shape=outs,
            in_specs=[any_spec] * 3,
            out_specs=(any_spec,) * 3,
            scratch_shapes=[dma((3,))],
        )(*made)

    replicated = P()
    in_specs = (P('dp'), P(None, 'dp'), P('dp', 'kv'), P('dp', 'kv'), P('dp')) + (replicated,) * 13 + (P(None, None, 'kv'), P(None, None, 'kv'), P(None, 'kv'), replicated, P(None, 'dp'), P(None, 'dp'))
    out_specs = (P(None, 'dp'), P('dp'), P('dp'))
    return jax.shard_map(layer_steps, mesh=mesh, in_specs=in_specs, out_specs=out_specs, check_vma=False)
```
